32 devices in a mesh: gx: 4 (over z), gy: 2 (over y), gz: 4 (over x, core).
Axes of the slice: x: 2, y: 2, z: 4, core: 2. Of those that a mesh axis runs over, the one named last changes fastest.
Arguments:
- displ: float32 [3, 4, 2, 4, 9945], P(None, 'gx', 'gy', 'gz'), may hold values from -6 to 6
- veloc: float32 [3, 4, 2, 4, 9945], P(None, 'gx', 'gy', 'gz'), may hold values from -6 to 6
- accel: float32 [3, 4, 2, 4, 9945], P(None, 'gx', 'gy', 'gz'), may hold values from -12 to 12
- node_index: int32 [4, 2, 4, 125, 128], P('gx', 'gy', 'gz'), may hold values from 0 to 9944, as said below
- inv_map: float32 [4, 2, 4, 9, 125, 128], P('gx', 'gy', 'gz'), may hold values from -1 to 2, as said below
- jac_weight: float32 [4, 2, 4, 125, 128], P('gx', 'gy', 'gz'), may hold values from 0.05 to 0.5
- lame_first: float32 [4, 2, 4, 125, 128], P('gx', 'gy', 'gz'), may hold values from 0.02 to 0.1
- shear_mod: float32 [4, 2, 4, 125, 128], P('gx', 'gy', 'gz'), may hold values from 0.02 to 0.1
- density: float32 [4, 2, 4, 125, 128], P('gx', 'gy', 'gz'), may hold values from 1 to 3
Outputs:
- displ_out: float32 [3, 4, 2, 4, 9945], P(None, 'gx', 'gy', 'gz')
- veloc_out: float32 [3, 4, 2, 4, 9945], P(None, 'gx', 'gy', 'gz')
- accel_out: float32 [3, 4, 2, 4, 9945], P(None, 'gx', 'gy', 'gz')
The draws below stay inside these ranges and needn't reach their ends.
Inputs may be any that keep to these rules, and one draw needn't show every extreme that they name: `node_index`: on each device the element slots hold the elements of a brick of 4 x 16 x 2 elements in a drawn order, each once; element (ex, ey, ez) has its point (a, b, c) at node ((4 ex + a) * 65 + 4 ey + b) * 9 + 4 ez + c. `inv_map`: the entries with l equal to j are positive.
All inputs are finite; a program needn't handle non-finite values.
Results may differ from the reference program's by a relative error of at most 0.00024.
Values sent between devices are 32-bit elements; how exact they have to be, the bound alone decides.
A program may use at most 64 MiB of HBM per device.

```python
import math
import jax
import jax.numpy as jnp
import numpy as np
from jax import lax

NGLL = 5
EX = 4
EY = 16
EZ = 2
STEPS = 1
E_DEV = 128
NODES_DEV = 9945
N_GX = 4
N_GY = 2
N_GZ = 4


def draw_node_index(key, part):
    devices = N_GX * N_GY * N_GZ
    elements = EX * EY * EZ
    keys = jax.random.split(key, devices)
    orders = jax.vmap(lambda subkey: jax.random.permutation(subkey, elements))(keys).astype(jnp.int32)
    elem_x = orders // (EY * EZ)
    elem_y = orders // EZ % EY
    elem_z = orders % EZ
    points = jnp.arange(125, dtype=jnp.int32)
    offset_a = points // 25
    offset_b = points // 5 % 5
    offset_c = points % 5
    node_y = 4 * EY + 1
    node_z = 4 * EZ + 1
    along_x = 4 * elem_x[:, None, :] + offset_a[None, :, None]
    along_y = 4 * elem_y[:, None, :] + offset_b[None, :, None]
    along_z = 4 * elem_z[:, None, :] + offset_c[None, :, None]
    flat = (along_x * node_y + along_y) * node_z + along_z
    return flat.reshape(N_GX, N_GY, N_GZ, 125, elements).astype(jnp.int32)


def draw_inv_map(key, part):
    elements = EX * EY * EZ
    shape = (N_GX, N_GY, N_GZ, 3, 3, 125, elements)
    diag_key, other_key = jax.random.split(key)
    diagonal = jax.random.uniform(diag_key, shape, jnp.float32, 0.7, 1.4)
    offdiag = jnp.clip(0.25 * jax.random.normal(other_key, shape, jnp.float32), -1.0, 1.0)
    identity = jnp.eye(3, dtype=jnp.float32)[:, :, None, None]
    full = identity * diagonal + (1.0 - identity) * offdiag
    return full.reshape(N_GX, N_GY, N_GZ, 9, 125, elements).astype(jnp.float32)


def block_levels(stream_key, dims, pieces, low, largest):
    loudness, own = 1.0, jax.random.fold_in(stream_key, 6)
    for axis_at, blocks in pieces:
        draws = jnp.exp(jax.random.uniform(jax.random.fold_in(own, axis_at), (blocks,), jnp.float32, low / len(pieces), largest / len(pieces)))
        loudness = loudness * jnp.repeat(draws, dims[axis_at] // blocks).reshape([-1 if axis == axis_at else 1 for axis in range(len(dims))])
    return loudness


def normal_values(key, extent, width, limit, shards=(), kind=jnp.bfloat16):
    values = width * jax.random.normal(key, extent, jnp.float32)
    if shards:
        values = values * block_levels(key, extent, shards, -0.22, 0.18)
    return jnp.clip(values, -limit, limit).astype(kind)


def setup_inputs(seed: int = 0) -> dict:
    seeds = jax.random.split(jax.random.key(seed), 10)
    return {
        "displ": normal_values(seeds[0], (3, N_GX, N_GY, N_GZ, NODES_DEV), 1.0, 6.0, ((1, 4), (2, 2), (3, 4)), jnp.float32),
        "veloc": normal_values(seeds[1], (3, N_GX, N_GY, N_GZ, NODES_DEV), 1.0, 6.0, ((1, 4), (2, 2), (3, 4)), jnp.float32),
        "accel": normal_values(seeds[2], (3, N_GX, N_GY, N_GZ, NODES_DEV), 2.0, 12.0, ((1, 4), (2, 2), (3, 4)), jnp.float32),
        "node_index": draw_node_index(jax.random.fold_in(seeds[9], 71), 0),
        "inv_map": draw_inv_map(jax.random.fold_in(seeds[9], 71), 0),
        "jac_weight": jnp.clip(jnp.exp(math.log(0.5) - 2.3025851 * jax.random.uniform(seeds[5], (N_GX, N_GY, N_GZ, NGLL * NGLL * NGLL, E_DEV), jnp.float32) ** block_levels(seeds[5], (N_GX, N_GY, N_GZ, NGLL * NGLL * NGLL, E_DEV), ((0, 4), (1, 2), (2, 4)), -0.2, 0.2)), 0.05, 0.5),
        "lame_first": jnp.clip(jnp.exp(math.log(0.1) - 1.609438 * jax.random.uniform(seeds[6], (N_GX, N_GY, N_GZ, NGLL * NGLL * NGLL, E_DEV), jnp.float32) ** block_levels(seeds[6], (N_GX, N_GY, N_GZ, NGLL * NGLL * NGLL, E_DEV), ((0, 4), (1, 2), (2, 4)), -0.2, 0.2)), 0.02, 0.1),
        "shear_mod": jnp.clip(jnp.exp(math.log(0.1) - 1.609438 * jax.random.uniform(seeds[7], (N_GX, N_GY, N_GZ, NGLL * NGLL * NGLL, E_DEV), jnp.float32) ** block_levels(seeds[7], (N_GX, N_GY, N_GZ, NGLL * NGLL * NGLL, E_DEV), ((0, 4), (1, 2), (2, 4)), -0.2, 0.2)), 0.02, 0.1),
        "density": jnp.clip(jnp.exp(math.log(3.0) - 1.0986123 * jax.random.uniform(seeds[8], (N_GX, N_GY, N_GZ, NGLL * NGLL * NGLL, E_DEV), jnp.float32) ** block_levels(seeds[8], (N_GX, N_GY, N_GZ, NGLL * NGLL * NGLL, E_DEV), ((0, 4), (1, 2), (2, 4)), -0.2, 0.2)), 1.0, 3.0),
    }


time_step = 0.1

def derivative_table():
    points = np.array([-1.0, -np.sqrt(3.0 / 7.0), 0.0, np.sqrt(3.0 / 7.0), 1.0])
    points_count = points.shape[0]
    weights = np.array([1.0 / np.prod([points[source] - points[other] for other in range(points_count) if other != source]) for source in range(points_count)])
    deriv_table = np.zeros((points_count, points_count))
    for target in range(points_count):
        for source in range(points_count):
            if target != source:
                deriv_table[target, source] = weights[source] / weights[target] / (points[target] - points[source])
        deriv_table[target, target] = -np.sum(deriv_table[target])
    return deriv_table

def element_force(position, node_index, inv_map, jac_weight, lame_first, shear_mod, deriv):
    highest = lax.Precision.HIGHEST
    elements = node_index.shape[1]
    nodes = position.shape[1]
    local = position[:, node_index].reshape(3, 5, 5, 5, elements)
    grad_a = jnp.einsum('ap,cpbke->cabke', deriv, local, precision=highest).reshape(3, 125, elements)
    grad_b = jnp.einsum('bp,capke->cabke', deriv, local, precision=highest).reshape(3, 125, elements)
    grad_c = jnp.einsum('kp,cabpe->cabke', deriv, local, precision=highest).reshape(3, 125, elements)
    mapping = inv_map.reshape(3, 3, 125, elements)
    strain_grad = grad_a[:, None] * mapping[0][None] + grad_b[:, None] * mapping[1][None] + grad_c[:, None] * mapping[2][None]
    divergence = strain_grad[0, 0] + strain_grad[1, 1] + strain_grad[2, 2]
    identity = jnp.eye(3, dtype=jnp.float32)[:, :, None, None]
    stress = shear_mod * (strain_grad + jnp.swapaxes(strain_grad, 0, 1)) + lame_first * divergence * identity
    flux = stress[:, 0][:, None] * mapping[:, 0][None] + stress[:, 1][:, None] * mapping[:, 1][None] + stress[:, 2][:, None] * mapping[:, 2][None]
    flux = (jac_weight * flux).reshape(3, 3, 5, 5, 5, elements)
    terms = jnp.einsum('pa,cpbke->cabke', deriv, flux[:, 0], precision=highest)
    terms = terms + jnp.einsum('pb,capke->cabke', deriv, flux[:, 1], precision=highest)
    terms = terms + jnp.einsum('pk,cabpe->cabke', deriv, flux[:, 2], precision=highest)
    return jnp.zeros((3, nodes), jnp.float32).at[:, node_index].add(-terms.reshape(3, 125, elements))

def fold_planes(field, dev_axis, node_axis):
    length = field.shape[node_axis]
    devices = field.shape[dev_axis]
    first = lax.slice_in_dim(field, 0, 1, axis=node_axis)
    last = lax.slice_in_dim(field, length - 1, length, axis=node_axis)
    middle = lax.slice_in_dim(field, 1, length - 1, axis=node_axis)
    zero_plane = jnp.zeros_like(lax.slice_in_dim(first, 0, 1, axis=dev_axis))
    from_lower = jnp.concatenate([zero_plane, lax.slice_in_dim(last, 0, devices - 1, axis=dev_axis)], axis=dev_axis)
    from_upper = jnp.concatenate([lax.slice_in_dim(first, 1, devices, axis=dev_axis), zero_plane], axis=dev_axis)
    return jnp.concatenate([first + from_lower, middle, last + from_upper], axis=node_axis)

def assemble_all(field):
    for dev_axis, node_axis in ((1, 4), (2, 5), (3, 6)):
        field = fold_planes(field, dev_axis, node_axis)
    return field

def reference(displ, veloc, accel, node_index, inv_map, jac_weight, lame_first, shear_mod, density):
    devices = N_GX * N_GY * N_GZ
    node_x = 4 * EX + 1
    node_y = 4 * EY + 1
    node_z = 4 * EZ + 1
    nodes = node_x * node_y * node_z
    elements = EX * EY * EZ
    deriv = jnp.asarray(derivative_table(), jnp.float32)
    index_all = node_index.reshape(devices, 125, elements)
    map_all = inv_map.reshape(devices, 9, 125, elements)
    weight_all = jac_weight.reshape(devices, 125, elements)
    lame_all = lame_first.reshape(devices, 125, elements)
    shear_all = shear_mod.reshape(devices, 125, elements)
    dens_all = density.reshape(devices, 125, elements)

    def mass_one(items):
        index, weight, dens = items
        return jnp.zeros((nodes,), jnp.float32).at[index].add(dens * weight)
    mass_local = lax.map(mass_one, (index_all, weight_all, dens_all))
    mass = assemble_all(mass_local.reshape(1, N_GX, N_GY, N_GZ, node_x, node_y, node_z))
    mass = mass.reshape(N_GX, N_GY, N_GZ, nodes)

    def force_one(items):
        position, index, mapping, weight, lame, shear = items
        return element_force(position, index, mapping, weight, lame, shear, deriv)
    half_step = 0.5 * time_step
    half_square = 0.5 * time_step * time_step
    for step in range(STEPS):
        displ = displ + time_step * veloc + half_square * accel
        veloc = veloc + half_step * accel
        moved = jnp.moveaxis(displ.reshape(3, devices, nodes), 1, 0)
        forces = lax.map(force_one, (moved, index_all, map_all, weight_all, lame_all, shear_all))
        forces = jnp.moveaxis(forces, 0, 1).reshape(3, N_GX, N_GY, N_GZ, node_x, node_y, node_z)
        forces = assemble_all(forces).reshape(3, N_GX, N_GY, N_GZ, nodes)
        accel = forces / mass[None]
        veloc = veloc + half_step * accel
    return (displ, veloc, accel)
```

```python
import jax
import jax.numpy as jnp
import numpy as np
from jax import lax
from jax.experimental import pallas as pl
from jax.experimental.pallas import tpu as pltpu
from jax.sharding import PartitionSpec as P

EX = 4
EY = 16
EZ = 2
NX = 4 * EX + 1
NY = 4 * EY + 1
NZ = 4 * EZ + 1
PLANE = NY * NZ
GROUP = 4
GROUPS = EY // GROUP
STEP = 4 * GROUP * NZ
SPAN = 256
WIDE = 640
GROW = 64
SROW = 72
SUB = EZ * GROUP

LIMIT = 24 * 1024 * 1024

time_step = 0.1
MESH = pl.DeviceIdType.MESH


def derivative_table():
    points = np.array([-1.0, -np.sqrt(3.0 / 7.0), 0.0, np.sqrt(3.0 / 7.0), 1.0])
    count = points.shape[0]
    weights = np.array(
        [
            1.0 / np.prod([points[s] - points[o] for o in range(count) if o != s])
            for s in range(count)
        ]
    )
    table = np.zeros((count, count))
    for t in range(count):
        for s in range(count):
            if t != s:
                table[t, s] = weights[s] / weights[t] / (points[t] - points[s])
        table[t, t] = -np.sum(table[t])
    return table


def constants():
    table = derivative_table()
    select = np.zeros((25 * SUB, SPAN), np.float32)
    for b in range(5):
        for c in range(5):
            for ez in range(EZ):
                for ey in range(GROUP):
                    row = (b * 5 + c) * SUB + ez * GROUP + ey
                    select[row, (4 * ey + b) * NZ + 4 * ez + c] = 1.0
    eye = np.eye(5)
    parts = [
        np.kron(table, np.kron(eye, eye)),
        np.kron(eye, np.kron(table, eye)),
        np.kron(eye, np.kron(eye, table)),
    ]
    pad = np.zeros((125, 160))
    for a in range(5):
        for q in range(25):
            pad[a * 25 + q, a * 32 + q] = 1.0
    deriv = np.zeros((384, 160), np.float32)
    for l in range(3):
        deriv[l * 128 : l * 128 + 125] = parts[l] @ pad
    spread = np.zeros((160, 128), np.float32)
    spread[:, :125] = pad.T
    return select, deriv, -deriv.T.copy(), spread


def split2(x):
    hi = x.astype(jnp.bfloat16)
    low = (x - hi.astype(jnp.float32)).astype(jnp.bfloat16)
    return (hi, low)


def halves(x):
    hi = np.asarray(x, jnp.bfloat16)
    low = np.asarray(x - hi.astype(np.float32), jnp.bfloat16)
    return np.stack([hi, low])


def product(pair, y):
    hi, low = split2(y)
    dot = lambda a, b: jnp.dot(a, b, preferred_element_type=jnp.float32)
    return dot(pair[0], hi) + dot(pair[0], low) + dot(pair[1], hi)


def dots(x, y, dims, split_left):
    total = None
    for piece in split2(x if split_left else y):
        left, right = (piece, y) if split_left else (x, piece)
        out = lax.dot_general(
            left, right, (dims, ((), ())), preferred_element_type=jnp.float32
        )
        total = out if total is None else total + out
    return total


def squeezed(ref):
    return ref.at[:, 0] if len(ref.shape) == 3 else ref.at[:, :, 0]


def kernel(
    displ, veloc, accel, node, inv, jac, lame, shear, dens,
    select_ref, deriv_ref, back_ref, spread_ref,
    pos_out, vel_out, acc_out,
    select_s, deriv_s, back_s, spread_s,
    d_s, v_s, a_s, node_s, inv_s, jac_s, lame_s, shear_s, dens_s,
    nf, u_s, fl_s, md_s, zp_s, grid_s,
    z_send, z_recv, y_send, y_recv, x_send, x_recv,
    in_sem, send_sem, recv_sem,
):
    names = ("gz", "gy", "gx")
    spots = [lax.axis_index(n) for n in names]
    sizes = [lax.axis_size(n) for n in names]
    has_low = [s > 0 for s in spots]
    has_high = [s < n - 1 for s, n in zip(spots, sizes)]
    barrier = pltpu.get_barrier_semaphore()
    for n, s, lo, hi in zip(names, spots, has_low, has_high):

        @pl.when(lo)
        def _():
            pl.semaphore_signal(barrier, inc=1, device_id={n: s - 1}, device_id_type=MESH)

        @pl.when(hi)
        def _():
            pl.semaphore_signal(barrier, inc=1, device_id={n: s + 1}, device_id_type=MESH)

    copies = []
    for k, (src, dst) in enumerate(((displ, d_s), (veloc, v_s), (accel, a_s))):
        for c in range(3):
            copies.append(
                pltpu.make_async_copy(
                    src.at[c], dst.at[pl.ds(c, 1)], in_sem.at[3 * k + c]
                )
            )
    elems = ((node, node_s), (inv, inv_s), (jac, jac_s), (lame, lame_s), (shear, shear_s), (dens, dens_s))
    for k, (src, dst) in enumerate(elems):
        copies.append(pltpu.make_async_copy(squeezed(src), dst, in_sem.at[9 + k]))
    consts = ((select_ref, select_s), (deriv_ref, deriv_s), (back_ref, back_s), (spread_ref, spread_s))
    for k, (src, dst) in enumerate(consts):
        copies.append(pltpu.make_async_copy(src, dst, in_sem.at[15 + k]))
    for cp in copies:
        cp.start()
    nf[...] = jnp.zeros_like(nf)
    u_s[...] = jnp.zeros_like(u_s)
    fl_s[...] = jnp.zeros_like(fl_s)
    md_s[...] = jnp.zeros_like(md_s)
    for cp in copies[:10] + copies[15:16]:
        cp.wait()

    half = 0.5 * time_step
    pos = d_s[...] + time_step * v_s[...] + (half * time_step) * a_s[...]
    d_s[...] = pos
    vel_out[...] = v_s[...] + half * a_s[...]
    pos_out[...] = pos
    for x in range(NX):
        nf[3 * x : 3 * x + 3, 0:PLANE] = d_s[:, PLANE * x : PLANE * (x + 1)]
    planes = nf[...]
    blocks = [planes[:, :SPAN]] + [
        pltpu.roll(planes, WIDE - STEP * g, 1)[:, :SPAN] for g in range(1, GROUPS)
    ]
    rows = jnp.concatenate(blocks, axis=0)
    select = select_s[...]
    lifted = dots(select, rows, ((1,), (1,)), False)

    corner = node_s[0:1, :].astype(jnp.float32)
    x0 = jnp.floor((corner + 0.5) * (1.0 / PLANE))
    rem = corner - PLANE * x0
    y0 = jnp.floor((rem + 0.5) * (1.0 / NZ))
    z0 = rem - NZ * y0
    grp = jnp.floor((y0 + 0.5) * (1.0 / (4 * GROUP)))
    low = (y0 - 4 * GROUP * grp) * 0.25 + GROUP * (z0 * 0.25)
    sub = lax.broadcasted_iota(jnp.int32, (SUB, 128), 0).astype(jnp.float32)
    mask = jnp.where(sub == low, 1.0, 0.0)[None]

    iota = lax.broadcasted_iota(jnp.int32, (GROUPS * GROW, 128), 0).astype(jnp.float32)
    goal = grp * GROW + 3.0 * x0
    picks = jnp.concatenate(
        [
            jnp.where(iota == goal + (3.0 * a + c), 1.0, 0.0).astype(jnp.bfloat16)
            for c in range(3)
            for a in range(5)
        ],
        axis=1,
    )
    gathered = dots(lifted, picks, ((1,), (0,)), True)
    for c in range(3):
        for a in range(5):
            j = (c * 5 + a) * 128
            part = gathered[:, j : j + 128].reshape(25, SUB, 128) * mask
            u_s[a * 32 : a * 32 + 25, c * 128 : (c + 1) * 128] = jnp.sum(part, axis=1)

    for cp in copies[16:]:
        cp.wait()
    local = product(deriv_s, u_s[...])
    for cp in copies[10:15]:
        cp.wait()
    grads = [
        [local[l * 128 : l * 128 + 125, c * 128 : (c + 1) * 128] for c in range(3)]
        for l in range(3)
    ]
    maps = [[inv_s[3 * l + j] for j in range(3)] for l in range(3)]
    weight = jac_s[...]
    lam = lame_s[...]
    mu = shear_s[...]
    h = [
        [sum(grads[l][c] * maps[l][j] for l in range(3)) for j in range(3)] for c in range(3)
    ]
    div = lam * (h[0][0] + h[1][1] + h[2][2])
    stress = [[None] * 3 for _ in range(3)]
    for c in range(3):
        for j in range(c, 3):
            s = mu * (h[c][j] + h[j][c])
            if c == j:
                s = s + div
            s = s * weight
            stress[c][j] = s
            stress[j][c] = s
    for l in range(3):
        for c in range(3):
            fl_s[l * 128 : l * 128 + 125, c * 128 : (c + 1) * 128] = sum(
                stress[c][j] * maps[l][j] for j in range(3)
            )
    md_s[0:125, :] = dens_s[...] * weight
    terms = product(back_s, fl_s[...])
    heavy = sum(
        jnp.dot(spread_s[...], part, preferred_element_type=jnp.float32)
        for part in split2(md_s[...])
    )

    spread_out = []
    puts = []
    iota2 = lax.broadcasted_iota(jnp.int32, (GROUPS * SROW, 128), 0).astype(jnp.float32)
    goal2 = grp * SROW + 4.0 * x0
    for k in range(4):
        for a in range(5):
            part = terms[a * 32 : a * 32 + 25, k * 128 : (k + 1) * 128] if k < 3 else heavy[a * 32 : a * 32 + 25]
            spread_out.append((part[:, None, :] * mask).reshape(25 * SUB, 128))
            puts.append(
                jnp.where(iota2 == goal2 + (4.0 * a + k), 1.0, 0.0).astype(jnp.bfloat16)
            )
    zp_s[...] = dots(
        jnp.concatenate(spread_out, axis=1),
        jnp.concatenate(puts, axis=1),
        ((1,), (1,)),
        True,
    )

    peers = sum(flag.astype(jnp.int32) for flag in has_low + has_high)
    pl.semaphore_wait(barrier, peers)

    def exchange(axis, send, recv):
        name, spot = names[axis], spots[axis]

        def copy(side, peer):
            return pltpu.make_async_remote_copy(
                src_ref=send.at[side],
                dst_ref=recv.at[1 - side],
                send_sem=send_sem.at[2 * axis + side],
                recv_sem=recv_sem.at[2 * axis + 1 - side],
                device_id={name: peer},
                device_id_type=MESH,
            )

        @pl.when(has_low[axis])
        def _():
            copy(0, spot - 1).start()

        @pl.when(has_high[axis])
        def _():
            copy(1, spot + 1).start()

        def finish(side):
            copy(1 - side, spot).wait_recv()

        def drain():
            for side, ok in ((0, has_low[axis]), (1, has_high[axis])):

                @pl.when(ok)
                def _():
                    copy(side, spot).wait_send()

        return finish, drain

    drains = []
    for b in range(5):
        z_send[0, b * 4 : b * 4 + 4] = zp_s[b * 5 * SUB : b * 5 * SUB + GROUP]
        top = (b * 5 + 4) * SUB + (EZ - 1) * GROUP
        z_send[1, b * 4 : b * 4 + 4] = zp_s[top : top + GROUP]
    finish, drain = exchange(0, z_send, z_recv)
    drains.append(drain)

    @pl.when(has_low[0])
    def _():
        finish(0)
        for b in range(5):
            at = b * 5 * SUB
            zp_s[at : at + GROUP] += z_recv[0, b * 4 : b * 4 + 4]

    @pl.when(has_high[0])
    def _():
        finish(1)
        for b in range(5):
            at = (b * 5 + 4) * SUB + (EZ - 1) * GROUP
            zp_s[at : at + GROUP] += z_recv[1, b * 4 : b * 4 + 4]

    flat = dots(zp_s[...], select, ((0,), (0,)), True)
    total = None
    blank = jnp.zeros((SROW, WIDE - SPAN), jnp.float32)
    for g in range(GROUPS):
        piece = jnp.concatenate([flat[g * SROW : (g + 1) * SROW], blank], axis=1)
        if g:
            piece = pltpu.roll(piece, STEP * g, 1)
        total = piece if total is None else total + piece
    grid_s[...] = total

    edge = WIDE - 128
    shift = PLANE - NZ - edge
    lanes = lax.broadcasted_iota(jnp.int32, (SROW, 128), 1)
    y_send[0] = grid_s[:, 0:128]
    y_send[1] = grid_s[:, edge:WIDE]
    finish, drain = exchange(1, y_send, y_recv)
    drains.append(drain)

    @pl.when(has_low[1])
    def _():
        finish(0)
        got = pltpu.roll(y_recv[0], 128 - shift, 1)
        grid_s[:, 0:128] += jnp.where(lanes < NZ, got, 0.0)

    @pl.when(has_high[1])
    def _():
        finish(1)
        got = jnp.where(lanes < NZ, y_recv[1], 0.0)
        grid_s[:, edge:WIDE] += pltpu.roll(got, shift, 1)

    x_send[0] = grid_s[0:8]
    x_send[1] = grid_s[SROW - 8 : SROW]
    finish, drain = exchange(2, x_send, x_recv)
    drains.append(drain)

    @pl.when(has_low[2])
    def _():
        finish(0)
        grid_s[0:4] += x_recv[0, 0:4]

    @pl.when(has_high[2])
    def _():
        finish(1)
        grid_s[SROW - 8 : SROW - 4] += x_recv[1, 0:4]

    for x in range(NX):
        force = grid_s[4 * x : 4 * x + 3, 0:PLANE]
        mass = grid_s[4 * x + 3 : 4 * x + 4, 0:PLANE]
        acc_out[:, PLANE * x : PLANE * (x + 1)] = force / mass
    for drain in drains:
        drain()


def finish(pos, vel, acc, pos_out, vel_out, acc_out, v_s, sem):
    def put(src, dst, k):
        copies = [
            pltpu.make_async_copy(src.at[pl.ds(c, 1)], dst.at[c], sem.at[k + c]) for c in range(3)
        ]
        for cp in copies:
            cp.start()
        return copies

    copies = put(pos, pos_out, 0) + put(acc, acc_out, 3)
    v_s[...] = vel[...] + (0.5 * time_step) * acc[...]
    for cp in copies + put(v_s, vel_out, 6):
        cp.wait()


def body(displ, veloc, accel, node_index, inv_map, jac_weight, lame_first, shear_mod, density):
    nodes = displ.shape[4]
    elements = node_index.shape[4]
    select, deriv, back, spread = constants()
    deriv, back = halves(deriv), halves(back)
    fields = [x.reshape(3, 1, nodes) for x in (displ, veloc, accel)]
    elems = [
        x.reshape(125, 1, elements) for x in (jac_weight, lame_first, shear_mod, density)
    ]
    vmem = pl.BlockSpec(memory_space=pltpu.VMEM)
    hbm = pl.BlockSpec(memory_space=pltpu.HBM)
    f32 = jnp.float32
    out = jax.ShapeDtypeStruct((3, 1, nodes), f32)
    elem = pltpu.VMEM((125, elements), f32)
    width = GROUPS * SROW
    result = pl.pallas_call(
        kernel,
        out_shape=[pltpu.VMEM((3, nodes), f32)] * 3,
        in_specs=[hbm] * 13,
        out_specs=[vmem] * 3,
        scratch_shapes=[
            pltpu.VMEM(select.shape, jnp.bfloat16),
            pltpu.VMEM(deriv.shape, jnp.bfloat16),
            pltpu.VMEM(back.shape, jnp.bfloat16),
            pltpu.VMEM(spread.shape, jnp.bfloat16),
            pltpu.VMEM((3, nodes), f32),
            pltpu.VMEM((3, nodes), f32),
            pltpu.VMEM((3, nodes), f32),
            pltpu.VMEM((125, elements), jnp.int32),
            pltpu.VMEM((9, 125, elements), f32),
            elem, elem, elem, elem,
            pltpu.VMEM((GROW, WIDE), f32),
            pltpu.VMEM((160, 384), f32),
            pltpu.VMEM((384, 384), f32),
            pltpu.VMEM((128, 128), f32),
            pltpu.VMEM((25 * SUB, width), f32),
            pltpu.VMEM((SROW, WIDE), f32),
            pltpu.VMEM((2, 24, width), f32),
            pltpu.VMEM((2, 24, width), f32),
            pltpu.VMEM((2, SROW, 128), f32),
            pltpu.VMEM((2, SROW, 128), f32),
            pltpu.VMEM((2, 8, WIDE), f32),
            pltpu.VMEM((2, 8, WIDE), f32),
            pltpu.SemaphoreType.DMA((19,)),
            pltpu.SemaphoreType.DMA((6,)),
            pltpu.SemaphoreType.DMA((6,)),
        ],
        compiler_params=pltpu.CompilerParams(
            collective_id=0, has_side_effects=True, vmem_limit_bytes=LIMIT
        ),
    )(
        *fields,
        node_index.reshape(125, 1, elements),
        inv_map.reshape(9, 125, 1, elements),
        *elems,
        jnp.asarray(select, jnp.bfloat16),
        jnp.asarray(deriv),
        jnp.asarray(back),
        jnp.asarray(spread, jnp.bfloat16),
    )
    final = pl.pallas_call(
        finish,
        out_shape=[out] * 3,
        in_specs=[vmem] * 3,
        out_specs=[hbm] * 3,
        scratch_shapes=[pltpu.VMEM((3, nodes), f32), pltpu.SemaphoreType.DMA((9,))],
        compiler_params=pltpu.CompilerParams(vmem_limit_bytes=LIMIT),
    )(*[pltpu.with_memory_space_constraint(x, pltpu.VMEM) for x in result])
    return tuple(x.reshape(displ.shape) for x in final)


def solution(mesh):
    field = P(None, "gx", "gy", "gz", None)
    elem = P("gx", "gy", "gz", None, None)
    placed = (field,) * 3 + (elem, P("gx", "gy", "gz", None, None, None)) + (elem,) * 4
    return jax.shard_map(
        body, mesh=mesh, in_specs=placed, out_specs=(field,) * 3, check_vma=False
    )
```

```python
import jax
import jax.numpy as jnp
import numpy as np
from jax import lax
from jax.experimental import pallas as pl
from jax.experimental.pallas import tpu as pltpu
from jax.sharding import PartitionSpec as P

EX = 4
EY = 16
EZ = 2
NX = 4 * EX + 1
NY = 4 * EY + 1
NZ = 4 * EZ + 1
PLANE = NY * NZ
GROUP = 4
GROUPS = EY // GROUP
STEP = 4 * GROUP * NZ
SPAN = 256
WIDE = 640
GROW = 64
SROW = 72
SUB = EZ * GROUP

LIMIT = 65 * 1000 * 1000

time_step = 0.1
MESH = pl.DeviceIdType.MESH


def derivative_table():
    points = np.array([-1.0, -np.sqrt(3.0 / 7.0), 0.0, np.sqrt(3.0 / 7.0), 1.0])
    count = points.shape[0]
    weights = np.array(
        [
            1.0 / np.prod([points[s] - points[o] for o in range(count) if o != s])
            for s in range(count)
        ]
    )
    table = np.zeros((count, count))
    for t in range(count):
        for s in range(count):
            if t != s:
                table[t, s] = weights[s] / weights[t] / (points[t] - points[s])
        table[t, t] = -np.sum(table[t])
    return table


def constants():
    table = derivative_table()
    select = np.zeros((25 * SUB, SPAN), np.float32)
    for b in range(5):
        for c in range(5):
            for ez in range(EZ):
                for ey in range(GROUP):
                    row = (b * 5 + c) * SUB + ez * GROUP + ey
                    select[row, (4 * ey + b) * NZ + 4 * ez + c] = 1.0
    eye = np.eye(5)
    parts = [
        np.kron(table, np.kron(eye, eye)),
        np.kron(eye, np.kron(table, eye)),
        np.kron(eye, np.kron(eye, table)),
    ]
    pad = np.zeros((125, 160))
    for a in range(5):
        for q in range(25):
            pad[a * 25 + q, a * 32 + q] = 1.0
    deriv = np.zeros((384, 160), np.float32)
    for l in range(3):
        deriv[l * 128 : l * 128 + 125] = parts[l] @ pad
    spread = np.zeros((160, 128), np.float32)
    spread[:, :125] = pad.T
    return select, deriv, -deriv.T.copy(), spread


def split2(x):
    hi = x.astype(jnp.bfloat16)
    low = (x - hi.astype(jnp.float32)).astype(jnp.bfloat16)
    return (hi, low)


def halves(x):
    hi = np.asarray(x, jnp.bfloat16)
    low = np.asarray(x - hi.astype(np.float32), jnp.bfloat16)
    return np.stack([hi, low])


def product(pair, y):
    hi, low = split2(y)
    dot = lambda a, b: jnp.dot(a, b, preferred_element_type=jnp.float32)
    return dot(pair[0], hi) + dot(pair[0], low) + dot(pair[1], hi)


def dots(x, y, dims, split_left):
    total = None
    for piece in split2(x if split_left else y):
        left, right = (piece, y) if split_left else (x, piece)
        out = lax.dot_general(
            left, right, (dims, ((), ())), preferred_element_type=jnp.float32
        )
        total = out if total is None else total + out
    return total


def squeezed(ref):
    return ref.at[:, 0] if len(ref.shape) == 3 else ref.at[:, :, 0]


def kernel(
    displ, veloc, accel, node, inv, jac, lame, shear, dens,
    select_ref, deriv_ref, back_ref, spread_ref,
    pos_out, vel_out, acc_out,
    select_s, deriv_s, back_s, spread_s,
    d_s, v_s, a_s, node_s, inv_s, jac_s, lame_s, shear_s, dens_s,
    nf, u_s, fl_s, md_s, zp_s, grid_s,
    z_send, z_recv, y_send, y_recv, x_send, x_recv,
    in_sem, send_sem, recv_sem,
):
    names = ("gz", "gy", "gx")
    spots = [lax.axis_index(n) for n in names]
    sizes = [lax.axis_size(n) for n in names]
    has_low = [s > 0 for s in spots]
    has_high = [s < n - 1 for s, n in zip(spots, sizes)]
    barrier = pltpu.get_barrier_semaphore()
    for n, s, lo, hi in zip(names, spots, has_low, has_high):

        @pl.when(lo)
        def _():
            pl.semaphore_signal(barrier, inc=1, device_id={n: s - 1}, device_id_type=MESH)

        @pl.when(hi)
        def _():
            pl.semaphore_signal(barrier, inc=1, device_id={n: s + 1}, device_id_type=MESH)

    copies = []
    for k, (src, dst) in enumerate(((displ, d_s), (veloc, v_s), (accel, a_s))):
        for c in range(3):
            copies.append(
                pltpu.make_async_copy(
                    src.at[c], dst.at[pl.ds(c, 1)], in_sem.at[3 * k + c]
                )
            )
    elems = ((node, node_s), (inv, inv_s), (jac, jac_s), (lame, lame_s), (shear, shear_s), (dens, dens_s))
    for k, (src, dst) in enumerate(elems):
        copies.append(pltpu.make_async_copy(squeezed(src), dst, in_sem.at[9 + k]))
    consts = ((select_ref, select_s), (deriv_ref, deriv_s), (back_ref, back_s), (spread_ref, spread_s))
    for k, (src, dst) in enumerate(consts):
        copies.append(pltpu.make_async_copy(src, dst, in_sem.at[15 + k]))
    for cp in copies:
        cp.start()
    nf[...] = jnp.zeros_like(nf)
    u_s[...] = jnp.zeros_like(u_s)
    fl_s[...] = jnp.zeros_like(fl_s)
    md_s[...] = jnp.zeros_like(md_s)
    for cp in copies[:10] + copies[15:16]:
        cp.wait()

    half = 0.5 * time_step
    pos = d_s[...] + time_step * v_s[...] + (half * time_step) * a_s[...]
    d_s[...] = pos
    vel_out[...] = v_s[...] + half * a_s[...]
    pos_out[...] = pos
    for x in range(NX):
        nf[3 * x : 3 * x + 3, 0:PLANE] = d_s[:, PLANE * x : PLANE * (x + 1)]
    planes = nf[...]
    blocks = [planes[:, :SPAN]] + [
        pltpu.roll(planes, WIDE - STEP * g, 1)[:, :SPAN] for g in range(1, GROUPS)
    ]
    rows = jnp.concatenate(blocks, axis=0)
    select = select_s[...]
    lifted = dots(select, rows, ((1,), (1,)), False)

    corner = node_s[0:1, :].astype(jnp.float32)
    x0 = jnp.floor((corner + 0.5) * (1.0 / PLANE))
    rem = corner - PLANE * x0
    y0 = jnp.floor((rem + 0.5) * (1.0 / NZ))
    z0 = rem - NZ * y0
    grp = jnp.floor((y0 + 0.5) * (1.0 / (4 * GROUP)))
    low = (y0 - 4 * GROUP * grp) * 0.25 + GROUP * (z0 * 0.25)
    sub = lax.broadcasted_iota(jnp.int32, (SUB, 128), 0).astype(jnp.float32)
    mask = jnp.where(sub == low, 1.0, 0.0)[None]

    iota = lax.broadcasted_iota(jnp.int32, (GROUPS * GROW, 128), 0).astype(jnp.float32)
    goal = grp * GROW + 3.0 * x0
    picks = jnp.concatenate(
        [
            jnp.where(iota == goal + (3.0 * a + c), 1.0, 0.0).astype(jnp.bfloat16)
            for c in range(3)
            for a in range(5)
        ],
        axis=1,
    )
    gathered = dots(lifted, picks, ((1,), (0,)), True)
    for c in range(3):
        for a in range(5):
            j = (c * 5 + a) * 128
            part = gathered[:, j : j + 128].reshape(25, SUB, 128) * mask
            u_s[a * 32 : a * 32 + 25, c * 128 : (c + 1) * 128] = jnp.sum(part, axis=1)

    for cp in copies[16:]:
        cp.wait()
    local = product(deriv_s, u_s[...])
    for cp in copies[10:15]:
        cp.wait()
    grads = [
        [local[l * 128 : l * 128 + 125, c * 128 : (c + 1) * 128] for c in range(3)]
        for l in range(3)
    ]
    maps = [[inv_s[3 * l + j] for j in range(3)] for l in range(3)]
    weight = jac_s[...]
    lam = lame_s[...]
    mu = shear_s[...]
    h = [
        [sum(grads[l][c] * maps[l][j] for l in range(3)) for j in range(3)] for c in range(3)
    ]
    div = lam * (h[0][0] + h[1][1] + h[2][2])
    stress = [[None] * 3 for _ in range(3)]
    for c in range(3):
        for j in range(c, 3):
            s = mu * (h[c][j] + h[j][c])
            if c == j:
                s = s + div
            s = s * weight
            stress[c][j] = s
            stress[j][c] = s
    for l in range(3):
        for c in range(3):
            fl_s[l * 128 : l * 128 + 125, c * 128 : (c + 1) * 128] = sum(
                stress[c][j] * maps[l][j] for j in range(3)
            )
    md_s[0:125, :] = dens_s[...] * weight
    terms = product(back_s, fl_s[...])
    heavy = sum(
        jnp.dot(spread_s[...], part, preferred_element_type=jnp.float32)
        for part in split2(md_s[...])
    )

    spread_out = []
    puts = []
    iota2 = lax.broadcasted_iota(jnp.int32, (GROUPS * SROW, 128), 0).astype(jnp.float32)
    goal2 = grp * SROW + 4.0 * x0
    for k in range(4):
        for a in range(5):
            part = terms[a * 32 : a * 32 + 25, k * 128 : (k + 1) * 128] if k < 3 else heavy[a * 32 : a * 32 + 25]
            spread_out.append((part[:, None, :] * mask).reshape(25 * SUB, 128))
            puts.append(
                jnp.where(iota2 == goal2 + (4.0 * a + k), 1.0, 0.0).astype(jnp.bfloat16)
            )
    zp_s[...] = dots(
        jnp.concatenate(spread_out, axis=1),
        jnp.concatenate(puts, axis=1),
        ((1,), (1,)),
        True,
    )

    peers = sum(flag.astype(jnp.int32) for flag in has_low + has_high)
    pl.semaphore_wait(barrier, peers)

    def exchange(axis, send, recv):
        name, spot = names[axis], spots[axis]

        def copy(side, peer):
            return pltpu.make_async_remote_copy(
                src_ref=send.at[side],
                dst_ref=recv.at[1 - side],
                send_sem=send_sem.at[2 * axis + side],
                recv_sem=recv_sem.at[2 * axis + 1 - side],
                device_id={name: peer},
                device_id_type=MESH,
            )

        @pl.when(has_low[axis])
        def _():
            copy(0, spot - 1).start()

        @pl.when(has_high[axis])
        def _():
            copy(1, spot + 1).start()

        def finish(side):
            copy(1 - side, spot).wait_recv()

        def drain():
            for side, ok in ((0, has_low[axis]), (1, has_high[axis])):

                @pl.when(ok)
                def _():
                    copy(side, spot).wait_send()

        return finish, drain

    drains = []
    for b in range(5):
        z_send[0, b * 4 : b * 4 + 4] = zp_s[b * 5 * SUB : b * 5 * SUB + GROUP]
        top = (b * 5 + 4) * SUB + (EZ - 1) * GROUP
        z_send[1, b * 4 : b * 4 + 4] = zp_s[top : top + GROUP]
    finish, drain = exchange(0, z_send, z_recv)
    drains.append(drain)

    @pl.when(has_low[0])
    def _():
        finish(0)
        for b in range(5):
            at = b * 5 * SUB
            zp_s[at : at + GROUP] += z_recv[0, b * 4 : b * 4 + 4]

    @pl.when(has_high[0])
    def _():
        finish(1)
        for b in range(5):
            at = (b * 5 + 4) * SUB + (EZ - 1) * GROUP
            zp_s[at : at + GROUP] += z_recv[1, b * 4 : b * 4 + 4]

    flat = dots(zp_s[...], select, ((0,), (0,)), True)
    total = None
    blank = jnp.zeros((SROW, WIDE - SPAN), jnp.float32)
    for g in range(GROUPS):
        piece = jnp.concatenate([flat[g * SROW : (g + 1) * SROW], blank], axis=1)
        if g:
            piece = pltpu.roll(piece, STEP * g, 1)
        total = piece if total is None else total + piece
    grid_s[...] = total

    edge = WIDE - 128
    shift = PLANE - NZ - edge
    lanes = lax.broadcasted_iota(jnp.int32, (SROW, 128), 1)
    y_send[0] = grid_s[:, 0:128]
    y_send[1] = grid_s[:, edge:WIDE]
    finish, drain = exchange(1, y_send, y_recv)
    drains.append(drain)

    @pl.when(has_low[1])
    def _():
        finish(0)
        got = pltpu.roll(y_recv[0], 128 - shift, 1)
        grid_s[:, 0:128] += jnp.where(lanes < NZ, got, 0.0)

    @pl.when(has_high[1])
    def _():
        finish(1)
        got = jnp.where(lanes < NZ, y_recv[1], 0.0)
        grid_s[:, edge:WIDE] += pltpu.roll(got, shift, 1)

    x_send[0] = grid_s[0:8]
    x_send[1] = grid_s[SROW - 8 : SROW]
    finish, drain = exchange(2, x_send, x_recv)
    drains.append(drain)

    @pl.when(has_low[2])
    def _():
        finish(0)
        grid_s[0:4] += x_recv[0, 0:4]

    @pl.when(has_high[2])
    def _():
        finish(1)
        grid_s[SROW - 8 : SROW - 4] += x_recv[1, 0:4]

    for x in range(NX):
        force = grid_s[4 * x : 4 * x + 3, 0:PLANE]
        mass = grid_s[4 * x + 3 : 4 * x + 4, 0:PLANE]
        acc_out[:, PLANE * x : PLANE * (x + 1)] = force / mass
    for drain in drains:
        drain()


def finish(pos, vel, acc, pos_out, vel_out, acc_out, v_s, sem):
    def put(src, dst, k):
        copies = [
            pltpu.make_async_copy(src.at[pl.ds(c, 1)], dst.at[c], sem.at[k + c]) for c in range(3)
        ]
        for cp in copies:
            cp.start()
        return copies

    copies = put(pos, pos_out, 0) + put(acc, acc_out, 3)
    v_s[...] = vel[...] + (0.5 * time_step) * acc[...]
    for cp in copies + put(v_s, vel_out, 6):
        cp.wait()


def body(displ, veloc, accel, node_index, inv_map, jac_weight, lame_first, shear_mod, density):
    nodes = displ.shape[4]
    elements = node_index.shape[4]
    select, deriv, back, spread = constants()
    deriv, back = halves(deriv), halves(back)
    fields = [x.reshape(3, 1, nodes) for x in (displ, veloc, accel)]
    elems = [
        x.reshape(125, 1, elements) for x in (jac_weight, lame_first, shear_mod, density)
    ]
    vmem = pl.BlockSpec(memory_space=pltpu.VMEM)
    hbm = pl.BlockSpec(memory_space=pltpu.HBM)
    f32 = jnp.float32
    out = jax.ShapeDtypeStruct((3, 1, nodes), f32)
    elem = pltpu.VMEM((125, elements), f32)
    width = GROUPS * SROW
    result = pl.pallas_call(
        kernel,
        out_shape=[pltpu.VMEM((3, nodes), f32)] * 3,
        in_specs=[hbm] * 13,
        out_specs=[vmem] * 3,
        scratch_shapes=[
            pltpu.VMEM(select.shape, jnp.bfloat16),
            pltpu.VMEM(deriv.shape, jnp.bfloat16),
            pltpu.VMEM(back.shape, jnp.bfloat16),
            pltpu.VMEM(spread.shape, jnp.bfloat16),
            pltpu.VMEM((3, nodes), f32),
            pltpu.VMEM((3, nodes), f32),
            pltpu.VMEM((3, nodes), f32),
            pltpu.VMEM((125, elements), jnp.int32),
            pltpu.VMEM((9, 125, elements), f32),
            elem, elem, elem, elem,
            pltpu.VMEM((GROW, WIDE), f32),
            pltpu.VMEM((160, 384), f32),
            pltpu.VMEM((384, 384), f32),
            pltpu.VMEM((128, 128), f32),
            pltpu.VMEM((25 * SUB, width), f32),
            pltpu.VMEM((SROW, WIDE), f32),
            pltpu.VMEM((2, 24, width), f32),
            pltpu.VMEM((2, 24, width), f32),
            pltpu.VMEM((2, SROW, 128), f32),
            pltpu.VMEM((2, SROW, 128), f32),
            pltpu.VMEM((2, 8, WIDE), f32),
            pltpu.VMEM((2, 8, WIDE), f32),
            pltpu.SemaphoreType.DMA((19,)),
            pltpu.SemaphoreType.DMA((6,)),
            pltpu.SemaphoreType.DMA((6,)),
        ],
        compiler_params=pltpu.CompilerParams(
            collective_id=0, has_side_effects=True, vmem_limit_bytes=LIMIT
        ),
    )(
        *fields,
        node_index.reshape(125, 1, elements),
        inv_map.reshape(9, 125, 1, elements),
        *elems,
        jnp.asarray(select, jnp.bfloat16),
        jnp.asarray(deriv),
        jnp.asarray(back),
        jnp.asarray(spread, jnp.bfloat16),
    )
    final = pl.pallas_call(
        finish,
        out_shape=[out] * 3,
        in_specs=[vmem] * 3,
        out_specs=[hbm] * 3,
        scratch_shapes=[pltpu.VMEM((3, nodes), f32), pltpu.SemaphoreType.DMA((9,))],
        compiler_params=pltpu.CompilerParams(vmem_limit_bytes=LIMIT),
    )(*[pltpu.with_memory_space_constraint(x, pltpu.VMEM) for x in result])
    return tuple(x.reshape(displ.shape) for x in final)


def solution(mesh):
    field = P(None, "gx", "gy", "gz", None)
    elem = P("gx", "gy", "gz", None, None)
    placed = (field,) * 3 + (elem, P("gx", "gy", "gz", None, None, None)) + (elem,) * 4
    return jax.shard_map(
        body, mesh=mesh, in_specs=placed, out_specs=(field,) * 3, check_vma=False
    )
```

```python
import jax
import jax.numpy as jnp
import numpy as np
from jax import lax
from jax.experimental import pallas as pl
from jax.experimental.pallas import tpu as pltpu
from jax.sharding import PartitionSpec as P

EX = 4
EY = 16
EZ = 2
NX = 4 * EX + 1
NY = 4 * EY + 1
NZ = 4 * EZ + 1
PLANE = NY * NZ
GROUP = 4
GROUPS = EY // GROUP
STEP = 4 * GROUP * NZ
SPAN = 256
WIDE = 640
GROW = 64
SROW = 72
SUB = EZ * GROUP
REACH = (4 * GROUP + 1) * NZ
FACE = 160
EDGE = 512
TAIL = PLANE - NZ - EDGE
PITCH = 14

LIMIT = 65 * 1000 * 1000

time_step = 0.1
MESH = pl.DeviceIdType.MESH


def derivative_table():
    points = np.array([-1.0, -np.sqrt(3.0 / 7.0), 0.0, np.sqrt(3.0 / 7.0), 1.0])
    count = points.shape[0]
    weights = np.array(
        [
            1.0 / np.prod([points[s] - points[o] for o in range(count) if o != s])
            for s in range(count)
        ]
    )
    table = np.zeros((count, count))
    for t in range(count):
        for s in range(count):
            if t != s:
                table[t, s] = weights[s] / weights[t] / (points[t] - points[s])
        table[t, t] = -np.sum(table[t])
    return table


def constants():
    table = derivative_table()
    select = np.zeros((25 * SUB, SPAN), np.float32)
    for b in range(5):
        for c in range(5):
            for ez in range(EZ):
                for ey in range(GROUP):
                    row = (b * 5 + c) * SUB + ez * GROUP + ey
                    select[row, (4 * ey + b) * NZ + 4 * ez + c] = 1.0
                    if ez == 0 and c == 0:
                        select[row, FACE + 4 * ey + b] = 1.0
                    if ez == EZ - 1 and c == 4:
                        select[row, FACE + 32 + 4 * ey + b] = 1.0
    eye = np.eye(5)
    parts = [
        np.kron(table, np.kron(eye, eye)),
        np.kron(eye, np.kron(table, eye)),
        np.kron(eye, np.kron(eye, table)),
    ]
    pad = np.zeros((125, 160))
    for a in range(5):
        for q in range(25):
            pad[a * 25 + q, a * 32 + q] = 1.0
    deriv = np.zeros((384, 160), np.float32)
    for l in range(3):
        deriv[l * 128 : l * 128 + 125] = parts[l] @ pad
    spread = np.zeros((160, 128), np.float32)
    spread[:, :125] = pad.T
    return select, deriv, -deriv.T.copy(), spread


def split2(x):
    hi = x.astype(jnp.bfloat16)
    low = (x - hi.astype(jnp.float32)).astype(jnp.bfloat16)
    return (hi, low)


def halves(x):
    hi = np.asarray(x, jnp.bfloat16)
    low = np.asarray(x - hi.astype(np.float32), jnp.bfloat16)
    return np.stack([hi, low])


def product(pair, y):
    hi, low = split2(y)
    dot = lambda a, b: jnp.dot(a, b, preferred_element_type=jnp.float32)
    return dot(pair[0], hi) + dot(pair[0], low) + dot(pair[1], hi)


def dots(x, y, dims, split_left):
    total = None
    for piece in split2(x if split_left else y):
        left, right = (piece, y) if split_left else (x, piece)
        out = lax.dot_general(
            left, right, (dims, ((), ())), preferred_element_type=jnp.float32
        )
        total = out if total is None else total + out
    return total


def ways():
    steps = (0, -1, 1)
    found = [(x, y, z) for z in steps for y in steps for x in steps][1:]
    half = [w for w in found if w > (0, 0, 0)]
    half.sort(key=lambda w: (sum(map(abs, w)), -abs(w[2])))
    other = [tuple(-v for v in w) for w in half]
    return half + other[::-1]


WAYS = ways()


def neighbours():
    names = ("gx", "gy", "gz")
    spots = [lax.axis_index(n) for n in names]
    sizes = [lax.axis_size(n) for n in names]
    links = []
    for way in WAYS:
        there = None
        peer = {}
        for n, s, z, w in zip(names, spots, sizes, way):
            if w:
                ok = s > 0 if w < 0 else s < z - 1
                there = ok if there is None else there & ok
                peer[n] = s + w
        links.append((way, there, peer))
    return links


def squeezed(ref):
    return ref.at[:, 0] if len(ref.shape) == 3 else ref.at[:, :, 0]


def kernel(
    displ, veloc, accel, node, inv, jac, lame, shear, dens,
    select_ref, deriv_ref, back_ref, spread_ref,
    pos_out, vel_out, acc_out,
    select_s, deriv_s, back_s, spread_s,
    d_s, v_s, a_s, node_s, inv_s, jac_s, lame_s, shear_s, dens_s,
    nf, u_s, fl_s, md_s, grid_s,
    m_send, p_send, x_send, e_send,
    m_recv, p_recv, q_recv, x_recv, e_recv, f_recv, c_recv,
    in_sem, send_sem, recv_sem,
):
    links = neighbours()
    copies = []
    for k, (src, dst) in enumerate(((displ, d_s), (veloc, v_s), (accel, a_s))):
        for c in range(3):
            copies.append(
                pltpu.make_async_copy(
                    src.at[c], dst.at[pl.ds(c, 1)], in_sem.at[3 * k + c]
                )
            )
    elems = ((node, node_s), (inv, inv_s), (jac, jac_s), (lame, lame_s), (shear, shear_s), (dens, dens_s))
    for k, (src, dst) in enumerate(elems):
        copies.append(pltpu.make_async_copy(squeezed(src), dst, in_sem.at[9 + k]))
    consts = ((select_ref, select_s), (deriv_ref, deriv_s), (back_ref, back_s), (spread_ref, spread_s))
    for k, (src, dst) in enumerate(consts):
        copies.append(pltpu.make_async_copy(src, dst, in_sem.at[15 + k]))
    for cp in copies:
        cp.start()
    nf[...] = jnp.zeros_like(nf)
    u_s[...] = jnp.zeros_like(u_s)
    fl_s[...] = jnp.zeros_like(fl_s)
    md_s[...] = jnp.zeros_like(md_s)
    for ref in (m_recv, p_recv, q_recv, x_recv, e_recv, f_recv, c_recv):
        ref[...] = jnp.zeros_like(ref)
    barrier = pltpu.get_barrier_semaphore()
    for way, there, peer in links:

        @pl.when(there)
        def _():
            pl.semaphore_signal(barrier, inc=1, device_id=peer, device_id_type=MESH)

    for cp in copies[:10] + copies[15:16]:
        cp.wait()

    half = 0.5 * time_step
    pos = d_s[...] + time_step * v_s[...] + (half * time_step) * a_s[...]
    d_s[...] = pos
    vel_out[...] = v_s[...] + half * a_s[...]
    pos_out[...] = pos
    for x in range(NX):
        nf[3 * x : 3 * x + 3, 0:PLANE] = d_s[:, PLANE * x : PLANE * (x + 1)]
    planes = nf[...]
    blocks = [planes[:, :SPAN]] + [
        pltpu.roll(planes, WIDE - STEP * g, 1)[:, :SPAN] for g in range(1, GROUPS)
    ]
    rows = jnp.concatenate(blocks, axis=0)
    inside = lax.broadcasted_iota(jnp.int32, (1, SPAN), 1) < REACH
    rows = jnp.where(inside, rows, 0.0)
    select = select_s[...]
    lifted = dots(select, rows, ((1,), (1,)), False)

    corner = node_s[0:1, :].astype(jnp.float32)
    x0 = jnp.floor((corner + 0.5) * (1.0 / PLANE))
    rem = corner - PLANE * x0
    y0 = jnp.floor((rem + 0.5) * (1.0 / NZ))
    z0 = rem - NZ * y0
    grp = jnp.floor((y0 + 0.5) * (1.0 / (4 * GROUP)))
    low = (y0 - 4 * GROUP * grp) * 0.25 + GROUP * (z0 * 0.25)
    sub = lax.broadcasted_iota(jnp.int32, (SUB, 128), 0).astype(jnp.float32)
    mask = jnp.where(sub == low, 1.0, 0.0)[None]

    iota = lax.broadcasted_iota(jnp.int32, (GROUPS * GROW, 128), 0).astype(jnp.float32)
    goal = grp * GROW + 3.0 * x0
    picks = jnp.concatenate(
        [
            jnp.where(iota == goal + (3.0 * a + c), 1.0, 0.0).astype(jnp.bfloat16)
            for c in range(3)
            for a in range(5)
        ],
        axis=1,
    )
    gathered = dots(lifted, picks, ((1,), (0,)), True)
    for c in range(3):
        for a in range(5):
            j = (c * 5 + a) * 128
            part = gathered[:, j : j + 128].reshape(25, SUB, 128) * mask
            u_s[a * 32 : a * 32 + 25, c * 128 : (c + 1) * 128] = jnp.sum(part, axis=1)

    for cp in copies[16:]:
        cp.wait()
    local = product(deriv_s, u_s[...])
    for cp in copies[10:15]:
        cp.wait()
    grads = [
        [local[l * 128 : l * 128 + 125, c * 128 : (c + 1) * 128] for c in range(3)]
        for l in range(3)
    ]
    maps = [[inv_s[3 * l + j] for j in range(3)] for l in range(3)]
    weight = jac_s[...]
    lam = lame_s[...]
    mu = shear_s[...]
    h = [
        [sum(grads[l][c] * maps[l][j] for l in range(3)) for j in range(3)] for c in range(3)
    ]
    div = lam * (h[0][0] + h[1][1] + h[2][2])
    stress = [[None] * 3 for _ in range(3)]
    for c in range(3):
        for j in range(c, 3):
            s = mu * (h[c][j] + h[j][c])
            if c == j:
                s = s + div
            s = s * weight
            stress[c][j] = s
            stress[j][c] = s
    for l in range(3):
        for c in range(3):
            fl_s[l * 128 : l * 128 + 125, c * 128 : (c + 1) * 128] = sum(
                stress[c][j] * maps[l][j] for j in range(3)
            )
    md_s[0:125, :] = dens_s[...] * weight
    terms = product(back_s, fl_s[...])
    heavy = sum(
        jnp.dot(spread_s[...], part, preferred_element_type=jnp.float32)
        for part in split2(md_s[...])
    )

    spread_out = []
    puts = []
    iota2 = lax.broadcasted_iota(jnp.int32, (GROUPS * SROW, 128), 0).astype(jnp.float32)
    goal2 = grp * SROW + 4.0 * x0
    for k in range(4):
        for a in range(5):
            part = terms[a * 32 : a * 32 + 25, k * 128 : (k + 1) * 128] if k < 3 else heavy[a * 32 : a * 32 + 25]
            spread_out.append((part[:, None, :] * mask).reshape(25 * SUB, 128))
            puts.append(
                jnp.where(iota2 == goal2 + (4.0 * a + k), 1.0, 0.0).astype(jnp.bfloat16)
            )
    puts_all = jnp.concatenate(puts, axis=1)
    zp = dots(jnp.concatenate(spread_out, axis=1), puts_all, ((1,), (1,)), True)

    flat = dots(zp, select, ((0,), (0,)), True)
    lanes = lax.broadcasted_iota(jnp.int32, (SROW, 128), 1)
    wide = lax.broadcasted_iota(jnp.int32, (1, SPAN), 1)
    total = None
    faces = [None, None]
    blank = jnp.zeros((SROW, WIDE - SPAN), jnp.float32)
    for g in range(GROUPS):
        piece = flat[g * SROW : (g + 1) * SROW]
        for side in range(2):
            at = FACE - 128 + 32 * side
            face = pltpu.roll(piece[:, 128:], (4 * GROUP * g - at) % 128, 1)
            first = 4 * GROUP * g
            face = jnp.where((lanes >= first) & (lanes <= first + 4 * GROUP), face, 0.0)
            faces[side] = face if g == 0 else faces[side] + face
        piece = jnp.concatenate([jnp.where(wide < REACH, piece, 0.0), blank], axis=1)
        if g:
            piece = pltpu.roll(piece, STEP * g, 1)
        total = piece if total is None else total + piece

    grid_s[...] = total
    ends = (total[:, 0:128], pltpu.roll(total[:, EDGE:WIDE], 128 - TAIL, 1))
    rows8 = [slice(8 * i, 8 * i + 8) for i in range(SROW // 8)]
    lane8 = lax.broadcasted_iota(jnp.int32, (8, 128), 1)
    for side in range(2):
        m_send[side] = faces[side]
        top = 4 * (NX - 1) * side
        x_send[side] = total[top : top + 4]
        for dz in range(2):
            e_send[side, dz] = faces[dz][top : top + 4]
        packed = None
        for i, part in enumerate(rows8):
            got = jnp.where(lane8 < NZ, ends[side][part], 0.0)
            got = pltpu.roll(got, PITCH * i, 1) if i else got
            packed = got if packed is None else packed + got
        p_send[side] = packed

    def copy(k, way, peer, arriving):
        ref_from, ref_to = route(way, arriving)
        return pltpu.make_async_remote_copy(
            src_ref=ref_from,
            dst_ref=ref_to,
            send_sem=send_sem.at[k],
            recv_sem=recv_sem.at[len(WAYS) - 1 - k if not arriving else k],
            device_id=peer,
            device_id_type=MESH,
        )

    def route(way, arriving):
        low = tuple((w + 1) // 2 for w in way)
        sx, sy, sz = low
        if arriving:
            ox, oy, oz = low
            sx, sy, sz = 1 - sx, 1 - sy, 1 - sz
        else:
            ox, oy, oz = 1 - sx, 1 - sy, 1 - sz
        dx, dy, dz = (w != 0 for w in way)
        end = pl.ds(EDGE * sy, 128)
        if dx and dy and dz:
            return x_send.at[sx, :, end], c_recv.at[ox, oy, oz]
        if dx and dy:
            return x_send.at[sx, :, end], f_recv.at[ox, oy]
        if dx and dz:
            return e_send.at[sx, sz], e_recv.at[ox, oz]
        if dy and dz:
            return p_send.at[sy], q_recv.at[oy, oz]
        if dx:
            return x_send.at[sx], x_recv.at[ox]
        if dy:
            return p_send.at[sy], p_recv.at[oy]
        return m_send.at[sz], m_recv.at[oz]

    peers = sum(there.astype(jnp.int32) for way, there, peer in links)
    pl.semaphore_wait(barrier, peers)
    farthest = sorted(range(len(WAYS)), key=lambda k: -sum(map(abs, WAYS[k])))
    for k in farthest:
        way, there, peer = links[k]

        @pl.when(there)
        def _():
            copy(k, way, peer, False).start()

    for k, (way, there, peer) in enumerate(links):

        @pl.when(there)
        def _():
            copy(k, way, peer, True).wait_recv()

    full = []
    pad = jnp.zeros((SROW - 4 * NX, 128), jnp.float32)
    gap = jnp.zeros((4 * NX - 8, 128), jnp.float32)
    for dz in range(2):
        rim = jnp.concatenate([e_recv[0, dz], gap, e_recv[1, dz], pad], axis=0)
        full.append(m_recv[dz] + rim)
    strips = []
    for sy in range(2):
        sums = p_recv[sy]
        for dz in range(2):
            got = pltpu.roll(q_recv[sy, dz], 128 - 8 if dz == 0 else 8, 1)
            here = lax.rem(lane8, PITCH) == (NZ - 1) * dz
            sums = sums + jnp.where(here & (lane8 < PITCH * 9), got, 0.0)
        parts = []
        for i in range(SROW // 8):
            got = pltpu.roll(sums, 128 - PITCH * i, 1) if i else sums
            parts.append(jnp.where(lane8 < NZ, got, 0.0))
        strip = jnp.concatenate(parts, axis=0)
        corners = []
        for sx in range(2):
            shift = 128 - TAIL if sy == 0 else 0
            got = f_recv[sx, sy]
            got = pltpu.roll(got, shift, 1) if shift else got
            lane4 = lax.broadcasted_iota(jnp.int32, (4, 128), 1)
            got = jnp.where(lane4 < NZ, got, 0.0)
            for dz in range(2):
                far = c_recv[sx, sy, dz]
                far = pltpu.roll(far, (shift + (128 - 8 if dz == 0 else 8)) % 128, 1)
                got = got + jnp.where(lane4 == (NZ - 1) * dz, far, 0.0)
            corners.append(got)
        strip = strip + jnp.concatenate([corners[0], gap, corners[1], pad], axis=0)
        strips.append(strip if sy == 0 else pltpu.roll(strip, TAIL, 1))
    for j in range(WIDE // 128):
        at = slice(128 * j, 128 * j + 128)
        node = lanes + 128 * j
        along = lax.div(node, NZ)
        depth = node - NZ * along
        sums = grid_s[:, at]
        for dz in range(2):
            got = jnp.take_along_axis(full[dz], jnp.minimum(along, 127), axis=1)
            sums = sums + jnp.where((depth == (NZ - 1) * dz) & (along < NY), got, 0.0)
        if j == 0:
            sums = sums + strips[0]
        if j == WIDE // 128 - 1:
            sums = sums + strips[1]
        grid_s[:, at] = sums
        for sx in range(2):
            top = 4 * (NX - 1) * sx
            grid_s[top : top + 4, at] += x_recv[sx, :, at]

    for x in range(NX):
        force = grid_s[4 * x : 4 * x + 3, 0:PLANE]
        mass = grid_s[4 * x + 3 : 4 * x + 4, 0:PLANE]
        acc_out[:, PLANE * x : PLANE * (x + 1)] = force / mass
    for k, (way, there, peer) in enumerate(links):

        @pl.when(there)
        def _():
            copy(k, way, peer, False).wait_send()


def finish(pos, vel, acc, pos_out, vel_out, acc_out, v_s, sem):
    def put(src, dst, k):
        copies = [
            pltpu.make_async_copy(src.at[pl.ds(c, 1)], dst.at[c], sem.at[k + c]) for c in range(3)
        ]
        for cp in copies:
            cp.start()
        return copies

    copies = put(pos, pos_out, 0) + put(acc, acc_out, 3)
    v_s[...] = vel[...] + (0.5 * time_step) * acc[...]
    for cp in copies + put(v_s, vel_out, 6):
        cp.wait()


def body(displ, veloc, accel, node_index, inv_map, jac_weight, lame_first, shear_mod, density):
    nodes = displ.shape[4]
    elements = node_index.shape[4]
    select, deriv, back, spread = constants()
    deriv, back = halves(deriv), halves(back)
    fields = [x.reshape(3, 1, nodes) for x in (displ, veloc, accel)]
    elems = [
        x.reshape(125, 1, elements) for x in (jac_weight, lame_first, shear_mod, density)
    ]
    vmem = pl.BlockSpec(memory_space=pltpu.VMEM)
    hbm = pl.BlockSpec(memory_space=pltpu.HBM)
    f32 = jnp.float32
    out = jax.ShapeDtypeStruct((3, 1, nodes), f32)
    elem = pltpu.VMEM((125, elements), f32)
    result = pl.pallas_call(
        kernel,
        out_shape=[pltpu.VMEM((3, nodes), f32)] * 3,
        in_specs=[hbm] * 13,
        out_specs=[vmem] * 3,
        scratch_shapes=[
            pltpu.VMEM(select.shape, jnp.bfloat16),
            pltpu.VMEM(deriv.shape, jnp.bfloat16),
            pltpu.VMEM(back.shape, jnp.bfloat16),
            pltpu.VMEM(spread.shape, jnp.bfloat16),
            pltpu.VMEM((3, nodes), f32),
            pltpu.VMEM((3, nodes), f32),
            pltpu.VMEM((3, nodes), f32),
            pltpu.VMEM((125, elements), jnp.int32),
            pltpu.VMEM((9, 125, elements), f32),
            elem, elem, elem, elem,
            pltpu.VMEM((GROW, WIDE), f32),
            pltpu.VMEM((160, 384), f32),
            pltpu.VMEM((384, 384), f32),
            pltpu.VMEM((128, 128), f32),
            pltpu.VMEM((SROW, WIDE), f32),
            pltpu.VMEM((2, SROW, 128), f32),
            pltpu.VMEM((2, 8, 128), f32),
            pltpu.VMEM((2, 4, WIDE), f32),
            pltpu.VMEM((2, 2, 4, 128), f32),
            pltpu.VMEM((2, SROW, 128), f32),
            pltpu.VMEM((2, 8, 128), f32),
            pltpu.VMEM((2, 2, 8, 128), f32),
            pltpu.VMEM((2, 4, WIDE), f32),
            pltpu.VMEM((2, 2, 4, 128), f32),
            pltpu.VMEM((2, 2, 4, 128), f32),
            pltpu.VMEM((2, 2, 2, 4, 128), f32),
            pltpu.SemaphoreType.DMA((19,)),
            pltpu.SemaphoreType.DMA((26,)),
            pltpu.SemaphoreType.DMA((26,)),
        ],
        compiler_params=pltpu.CompilerParams(
            collective_id=0, has_side_effects=True, vmem_limit_bytes=LIMIT
        ),
    )(
        *fields,
        node_index.reshape(125, 1, elements),
        inv_map.reshape(9, 125, 1, elements),
        *elems,
        jnp.asarray(select, jnp.bfloat16),
        jnp.asarray(deriv),
        jnp.asarray(back),
        jnp.asarray(spread, jnp.bfloat16),
    )
    final = pl.pallas_call(
        finish,
        out_shape=[out] * 3,
        in_specs=[vmem] * 3,
        out_specs=[hbm] * 3,
        scratch_shapes=[pltpu.VMEM((3, nodes), f32), pltpu.SemaphoreType.DMA((9,))],
        compiler_params=pltpu.CompilerParams(vmem_limit_bytes=LIMIT),
    )(*[pltpu.with_memory_space_constraint(x, pltpu.VMEM) for x in result])
    return tuple(x.reshape(displ.shape) for x in final)


def solution(mesh):
    field = P(None, "gx", "gy", "gz", None)
    elem = P("gx", "gy", "gz", None, None)
    placed = (field,) * 3 + (elem, P("gx", "gy", "gz", None, None, None)) + (elem,) * 4
    return jax.shard_map(
        body, mesh=mesh, in_specs=placed, out_specs=(field,) * 3, check_vma=False
    )
```

```python
import jax
import jax.numpy as jnp
import numpy as np
from jax import lax
from jax.experimental import pallas as pl
from jax.experimental.pallas import tpu as pltpu
from jax.sharding import PartitionSpec as P

EX = 4
EY = 16
EZ = 2
NX = 4 * EX + 1
NY = 4 * EY + 1
NZ = 4 * EZ + 1
PLANE = NY * NZ
CHUNKS = -(-PLANE // 128)
STRIDE = 4 * NZ
SPAN = 5 * NZ
SLOT = 48
GROWS = 56
SROW = 72
TAIL = PLANE - NZ - 128 * (CHUNKS - 1)
PITCH = 14

LIMIT = 65 * 1000 * 1000

time_step = 0.1
MESH = pl.DeviceIdType.MESH


def derivative_table():
    points = np.array([-1.0, -np.sqrt(3.0 / 7.0), 0.0, np.sqrt(3.0 / 7.0), 1.0])
    count = points.shape[0]
    weights = np.array(
        [
            1.0 / np.prod([points[s] - points[o] for o in range(count) if o != s])
            for s in range(count)
        ]
    )
    table = np.zeros((count, count))
    for t in range(count):
        for s in range(count):
            if t != s:
                table[t, s] = weights[s] / weights[t] / (points[t] - points[s])
        table[t, t] = -np.sum(table[t])
    return table


def constants():
    table = derivative_table()
    eye = np.eye(5)
    parts = [
        np.kron(table, np.kron(eye, eye)),
        np.kron(eye, np.kron(table, eye)),
        np.kron(eye, np.kron(eye, table)),
    ]
    pad = np.zeros((125, 5 * SLOT))
    for a in range(5):
        for b in range(5):
            for c in range(5):
                pad[a * 25 + 5 * b + c, a * SLOT + NZ * b + c] = 1.0
    deriv = np.zeros((384, 5 * SLOT), np.float32)
    for l in range(3):
        deriv[l * 128 : l * 128 + 125] = parts[l] @ pad
    spread = np.zeros((5 * SLOT, 128), np.float32)
    spread[:, :125] = pad.T
    return deriv, -deriv.T.copy(), spread


def split2(x):
    hi = x.astype(jnp.bfloat16)
    low = (x - hi.astype(jnp.float32)).astype(jnp.bfloat16)
    return (hi, low)


def halves(x):
    hi = np.asarray(x, jnp.bfloat16)
    low = np.asarray(x - hi.astype(np.float32), jnp.bfloat16)
    return np.stack([hi, low])


def product(pair, y):
    hi, low = split2(y)
    dot = lambda a, b: jnp.dot(a, b, preferred_element_type=jnp.float32)
    return dot(pair[0], hi) + dot(pair[0], low) + dot(pair[1], hi)


def stacked(x, y, dims):
    rows = x.shape[0]
    out = lax.dot_general(
        jnp.concatenate(split2(x), axis=0),
        y,
        (dims, ((), ())),
        preferred_element_type=jnp.float32,
    )
    return out[:rows] + out[rows:]


def ways():
    steps = (0, -1, 1)
    found = [(x, y, z) for z in steps for y in steps for x in steps][1:]
    half = [w for w in found if w > (0, 0, 0)]
    half.sort(key=lambda w: (sum(map(abs, w)), -abs(w[2])))
    other = [tuple(-v for v in w) for w in half]
    return half + other[::-1]


WAYS = ways()


def neighbours():
    names = ("gx", "gy", "gz")
    spots = [lax.axis_index(n) for n in names]
    sizes = [lax.axis_size(n) for n in names]
    links = []
    for way in WAYS:
        there = None
        peer = {}
        for n, s, z, w in zip(names, spots, sizes, way):
            if w:
                ok = s > 0 if w < 0 else s < z - 1
                there = ok if there is None else there & ok
                peer[n] = s + w
        links.append((way, there, peer))
    return links


def squeezed(ref):
    return ref.at[:, 0] if len(ref.shape) == 3 else ref.at[:, :, 0]


def kernel(
    displ, veloc, accel, node, inv, jac, lame, shear, dens,
    deriv_ref, back_ref, spread_ref,
    pos_out, vel_out, acc_out,
    deriv_s, back_s, spread_s,
    d_s, v_s, a_s, node_s, inv_s, jac_s, lame_s, shear_s, dens_s,
    nf, u_s, fl_s, md_s, grid_s,
    m_send, p_send, x_send, e_send,
    m_recv, p_recv, q_recv, x_recv, e_recv, f_recv, c_recv,
    in_sem, send_sem, recv_sem,
):
    links = neighbours()
    copies = []
    for k, (src, dst) in enumerate(((displ, d_s), (veloc, v_s), (accel, a_s))):
        for c in range(3):
            copies.append(
                pltpu.make_async_copy(
                    src.at[c], dst.at[pl.ds(c, 1)], in_sem.at[3 * k + c]
                )
            )
    elems = ((node, node_s), (inv, inv_s), (jac, jac_s), (lame, lame_s), (shear, shear_s), (dens, dens_s))
    for k, (src, dst) in enumerate(elems):
        copies.append(pltpu.make_async_copy(squeezed(src), dst, in_sem.at[9 + k]))
    consts = ((deriv_ref, deriv_s), (back_ref, back_s), (spread_ref, spread_s))
    for k, (src, dst) in enumerate(consts):
        copies.append(pltpu.make_async_copy(src, dst, in_sem.at[15 + k]))
    for cp in copies:
        cp.start()
    nf[...] = jnp.zeros_like(nf)
    u_s[...] = jnp.zeros_like(u_s)
    fl_s[...] = jnp.zeros_like(fl_s)
    md_s[...] = jnp.zeros_like(md_s)
    for ref in (m_recv, p_recv, q_recv, x_recv, e_recv, f_recv, c_recv):
        ref[...] = jnp.zeros_like(ref)
    barrier = pltpu.get_barrier_semaphore()
    for way, there, peer in links:

        @pl.when(there)
        def _():
            pl.semaphore_signal(barrier, inc=1, device_id=peer, device_id_type=MESH)

    for cp in copies[:10]:
        cp.wait()

    half = 0.5 * time_step
    pos = d_s[...] + time_step * v_s[...] + (half * time_step) * a_s[...]
    d_s[...] = pos
    vel_out[...] = v_s[...] + half * a_s[...]
    pos_out[...] = pos
    for x in range(NX):
        rows = pl.ds(x, 3, stride=16) if x < NX - 1 else pl.ds(48, 3)
        for j in range(CHUNKS):
            lanes = min(128, PLANE - 128 * j)
            at = PLANE * x + 128 * j
            nf[j, rows, 0:lanes] = d_s[:, at : at + lanes]

    corner = node_s[0:1, :].astype(jnp.float32)
    x0 = jnp.floor((corner + 0.5) * (1.0 / PLANE))
    rem = corner - PLANE * x0
    y0 = jnp.floor((rem + 0.5) * (1.0 / NZ))
    z0 = rem - NZ * y0
    upper = z0 > 1.0
    last = x0 > NX - 6.0
    iota = lax.broadcasted_iota(jnp.int32, (256, 128), 0).astype(jnp.float32)
    goal = 4.0 * y0 + x0
    picks = []
    for a in range(5):
        aim = goal + a if a < 4 else jnp.where(last, -1.0, goal + a)
        picks.append(jnp.where(iota == aim, 1.0, 0.0).astype(jnp.bfloat16))
    picks = jnp.concatenate(picks, axis=1)
    goal = 2.0 * y0
    ends = []
    for c in range(4):
        aim = jnp.where(last, goal + c, -1.0)
        ends.append(jnp.where(iota[0:128] == aim, 1.0, 0.0).astype(jnp.bfloat16))
    ends = jnp.concatenate(ends, axis=1)

    lane = lax.broadcasted_iota(jnp.int32, (1, 128), 1)
    windows = []
    for ey in range(EY):
        j, at = divmod(STRIDE * ey, 128)
        part = nf[j]
        if at + SLOT > 128:
            part = jnp.where(lane >= at, part, nf[j + 1])
        windows.append(pltpu.roll(part, 128 - at, 1) if at else part)
    turned = []
    for c in range(4):
        first, many = (16 * c, 16) if c < 3 else (48, 8)
        rows = jnp.concatenate([w[first : first + many] for w in windows], axis=0)
        turned.append(jnp.transpose(rows)[:SLOT])
    gathered = stacked(jnp.concatenate(turned[:3], axis=0), picks, ((1,), (0,)))
    beyond = stacked(turned[3], ends[:, : 3 * 128], ((1,), (0,)))
    for c in range(3):
        for a in range(5):
            part = gathered[SLOT * c : SLOT * (c + 1), 128 * a : 128 * (a + 1)]
            if a == 4:
                part = part + beyond[:, 128 * c : 128 * (c + 1)]
            part = jnp.where(upper, pltpu.roll(part, SLOT - 4, 0), part)
            u_s[SLOT * a : SLOT * (a + 1), 128 * c : 128 * (c + 1)] = part

    for cp in copies[15:]:
        cp.wait()
    local = product(deriv_s, u_s[...])
    for cp in copies[10:15]:
        cp.wait()
    grads = [
        [local[l * 128 : l * 128 + 125, c * 128 : (c + 1) * 128] for c in range(3)]
        for l in range(3)
    ]
    maps = [[inv_s[3 * l + j] for j in range(3)] for l in range(3)]
    weight = jac_s[...]
    lam = lame_s[...]
    mu = shear_s[...]
    h = [
        [sum(grads[l][c] * maps[l][j] for l in range(3)) for j in range(3)] for c in range(3)
    ]
    div = lam * (h[0][0] + h[1][1] + h[2][2])
    stress = [[None] * 3 for _ in range(3)]
    for c in range(3):
        for j in range(c, 3):
            s = mu * (h[c][j] + h[j][c])
            if c == j:
                s = s + div
            s = s * weight
            stress[c][j] = s
            stress[j][c] = s
    for l in range(3):
        for c in range(3):
            fl_s[l * 128 : l * 128 + 125, c * 128 : (c + 1) * 128] = sum(
                stress[c][j] * maps[l][j] for j in range(3)
            )
    md_s[0:125, :] = dens_s[...] * weight
    terms = product(back_s, fl_s[...])
    heavy = sum(
        jnp.dot(spread_s[...], part, preferred_element_type=jnp.float32)
        for part in split2(md_s[...])
    )

    columns = []
    tops = []
    for c in range(4):
        blocks = []
        for a in range(5):
            at = slice(SLOT * a, SLOT * (a + 1))
            part = terms[at, 128 * c : 128 * (c + 1)] if c < 3 else heavy[at]
            blocks.append(jnp.where(upper, pltpu.roll(part, 4, 0), part))
        columns.append(jnp.concatenate(blocks, axis=1))
        tops.append(blocks[4])
    placed = stacked(jnp.concatenate(columns, axis=0), picks, ((1,), (1,)))
    topped = stacked(jnp.concatenate(tops, axis=1), ends, ((1,), (1,)))
    blank = jnp.zeros((128, 128 - SLOT), jnp.float32)
    for c in range(5):
        if c < 4:
            part = placed[SLOT * c : SLOT * (c + 1)]
            halves_ = [part[:, :128], part[:, 128:]]
            first, many = 16 * c, 16
        else:
            halves_ = [topped]
            first, many = 64, 8
        back = [jnp.concatenate([jnp.transpose(h), blank], axis=1) for h in halves_]
        back = jnp.concatenate(back, axis=0) if c < 4 else back[0]
        sums = [None] * CHUNKS
        for ey in range(EY):
            j, at = divmod(STRIDE * ey, 128)
            part = back[many * ey : many * (ey + 1)]
            part = pltpu.roll(part, at, 1) if at else part
            pieces = [(j, part)]
            if at + SLOT > 128:
                pieces = [
                    (j, jnp.where(lane >= at, part, 0.0)),
                    (j + 1, jnp.where(lane < at, part, 0.0)),
                ]
            for k, piece in pieces:
                sums[k] = piece if sums[k] is None else sums[k] + piece
        for j in range(CHUNKS):
            grid_s[j, first : first + many, :] = sums[j]

    sides = (pl.ds(0, 4, stride=16), pl.ds(64, 4))
    lanes = lax.broadcasted_iota(jnp.int32, (SROW, 128), 1)
    far = CHUNKS - 1
    where_z = jnp.where(lanes < 64, NZ * lanes, NZ * (lanes - 64) + NZ - 1)
    both = None
    for j in range(CHUNKS):
        got = jnp.take_along_axis(
            grid_s[j], where_z & 127, axis=1, mode="promise_in_bounds"
        )
        both = got if both is None else jnp.where(where_z >= 128 * j, got, both)
    edge = grid_s[far]
    m_send[0] = jnp.where(lanes < 64, both, jnp.where(lanes == TAIL, edge, 0.0))
    upper_face = pltpu.roll(both, 64, 1)
    upper_edge = pltpu.roll(edge, 128 - (NZ - 1), 1)
    m_send[1] = jnp.where(lanes < 64, upper_face, jnp.where(lanes == TAIL, upper_edge, 0.0))
    rims = (grid_s[0], pltpu.roll(edge, 128 - TAIL, 1))
    lane8 = lax.broadcasted_iota(jnp.int32, (8, 128), 1)
    for side in range(2):
        for j in range(CHUNKS):
            x_send[side, j] = grid_s[j, sides[side], :]
        for dz in range(2):
            e_send[side, dz] = m_send[dz, sides[side], :]
        packed = None
        for i in range(SROW // 8):
            got = jnp.where(lane8 < NZ, rims[side][8 * i : 8 * i + 8], 0.0)
            got = pltpu.roll(got, PITCH * i, 1) if i else got
            packed = got if packed is None else packed + got
        p_send[side] = packed

    def copy(k, way, peer, arriving):
        ref_from, ref_to = route(way, arriving)
        return pltpu.make_async_remote_copy(
            src_ref=ref_from,
            dst_ref=ref_to,
            send_sem=send_sem.at[k],
            recv_sem=recv_sem.at[len(WAYS) - 1 - k if not arriving else k],
            device_id=peer,
            device_id_type=MESH,
        )

    def route(way, arriving):
        low = tuple((w + 1) // 2 for w in way)
        sx, sy, sz = low
        if arriving:
            ox, oy, oz = low
            sx, sy, sz = 1 - sx, 1 - sy, 1 - sz
        else:
            ox, oy, oz = 1 - sx, 1 - sy, 1 - sz
        dx, dy, dz = (w != 0 for w in way)
        end = far * sy
        if dx and dy and dz:
            return x_send.at[sx, end], c_recv.at[ox, oy, oz]
        if dx and dy:
            return x_send.at[sx, end], f_recv.at[ox, oy]
        if dx and dz:
            return e_send.at[sx, sz], e_recv.at[ox, oz]
        if dy and dz:
            return p_send.at[sy], q_recv.at[oy, oz]
        if dx:
            return x_send.at[sx], x_recv.at[ox]
        if dy:
            return p_send.at[sy], p_recv.at[oy]
        return m_send.at[sz], m_recv.at[oz]

    peers = sum(there.astype(jnp.int32) for way, there, peer in links)
    pl.semaphore_wait(barrier, peers)
    farthest = sorted(range(len(WAYS)), key=lambda k: -sum(map(abs, WAYS[k])))
    for k in farthest:
        way, there, peer = links[k]

        @pl.when(there)
        def _():
            copy(k, way, peer, False).start()

    for k, (way, there, peer) in enumerate(links):

        @pl.when(there)
        def _():
            copy(k, way, peer, True).wait_recv()

    for dz in range(2):
        for sx in range(2):
            m_recv[dz, sides[sx], :] += e_recv[sx, dz]
    full = [m_recv[dz] for dz in range(2)]
    strips = []
    for sy in range(2):
        sums = p_recv[sy]
        for dz in range(2):
            got = pltpu.roll(q_recv[sy, dz], 128 - 8 if dz == 0 else 8, 1)
            here = lax.rem(lane8, PITCH) == (NZ - 1) * dz
            sums = sums + jnp.where(here & (lane8 < PITCH * 9), got, 0.0)
        parts = []
        for i in range(SROW // 8):
            got = pltpu.roll(sums, 128 - PITCH * i, 1) if i else sums
            parts.append(jnp.where(lane8 < NZ, got, 0.0))
        strip = jnp.concatenate(parts, axis=0)
        strips.append(strip if sy == 0 else pltpu.roll(strip, TAIL, 1))
    lane4 = lax.broadcasted_iota(jnp.int32, (4, 128), 1)
    for sx in range(2):
        for sy in range(2):
            shift = 128 - TAIL if sy == 0 else TAIL
            first = TAIL * sy
            got = pltpu.roll(f_recv[sx, sy], shift, 1)
            got = jnp.where((lane4 >= first) & (lane4 < first + NZ), got, 0.0)
            for dz in range(2):
                turn = (shift + (128 - 8 if dz == 0 else 8)) % 128
                corner = pltpu.roll(c_recv[sx, sy, dz], turn, 1)
                got = got + jnp.where(lane4 == first + (NZ - 1) * dz, corner, 0.0)
            x_recv[sx, far * sy] += got
    for j in range(CHUNKS):
        node = lanes + 128 * j
        along = lax.div(node, NZ)
        depth = node - NZ * along
        sums = grid_s[j]
        for dz in range(2):
            got = jnp.take_along_axis(
                full[dz], jnp.minimum(along, 127), axis=1, mode="promise_in_bounds"
            )
            sums = sums + jnp.where((depth == (NZ - 1) * dz) & (along < NY), got, 0.0)
        if j == 0:
            sums = sums + strips[0]
        if j == far:
            sums = sums + strips[1]
        grid_s[j] = sums
        for sx in range(2):
            grid_s[j, sides[sx], :] += x_recv[sx, j]
        mass = grid_s[j, 48:64, :]
        for c in range(3):
            grid_s[j, 16 * c : 16 * c + 16, :] = grid_s[j, 16 * c : 16 * c + 16, :] / mass
        grid_s[j, 64:67, :] = grid_s[j, 64:67, :] / grid_s[j, 67:68, :]

    for x in range(NX):
        rows = pl.ds(x, 3, stride=16) if x < NX - 1 else pl.ds(64, 3)
        for j in range(CHUNKS):
            width = min(128, PLANE - 128 * j)
            at = PLANE * x + 128 * j
            acc_out[:, at : at + width] = grid_s[j, rows, 0:width]
    for k, (way, there, peer) in enumerate(links):

        @pl.when(there)
        def _():
            copy(k, way, peer, False).wait_send()


def finish(pos, vel, acc, pos_out, vel_out, acc_out, v_s, sem):
    def put(src, dst, k):
        copies = [
            pltpu.make_async_copy(src.at[pl.ds(c, 1)], dst.at[c], sem.at[k + c]) for c in range(3)
        ]
        for cp in copies:
            cp.start()
        return copies

    copies = put(pos, pos_out, 0) + put(acc, acc_out, 3)
    v_s[...] = vel[...] + (0.5 * time_step) * acc[...]
    for cp in copies + put(v_s, vel_out, 6):
        cp.wait()


def body(displ, veloc, accel, node_index, inv_map, jac_weight, lame_first, shear_mod, density):
    nodes = displ.shape[4]
    elements = node_index.shape[4]
    deriv, back, spread = constants()
    deriv, back = halves(deriv), halves(back)
    fields = [x.reshape(3, 1, nodes) for x in (displ, veloc, accel)]
    elems = [
        x.reshape(125, 1, elements) for x in (jac_weight, lame_first, shear_mod, density)
    ]
    vmem = pl.BlockSpec(memory_space=pltpu.VMEM)
    hbm = pl.BlockSpec(memory_space=pltpu.HBM)
    f32 = jnp.float32
    out = jax.ShapeDtypeStruct((3, 1, nodes), f32)
    elem = pltpu.VMEM((125, elements), f32)
    result = pl.pallas_call(
        kernel,
        out_shape=[pltpu.VMEM((3, nodes), f32)] * 3,
        in_specs=[hbm] * 12,
        out_specs=[vmem] * 3,
        scratch_shapes=[
            pltpu.VMEM(deriv.shape, jnp.bfloat16),
            pltpu.VMEM(back.shape, jnp.bfloat16),
            pltpu.VMEM(spread.shape, jnp.bfloat16),
            pltpu.VMEM((3, nodes), f32),
            pltpu.VMEM((3, nodes), f32),
            pltpu.VMEM((3, nodes), f32),
            pltpu.VMEM((125, elements), jnp.int32),
            pltpu.VMEM((9, 125, elements), f32),
            elem, elem, elem, elem,
            pltpu.VMEM((CHUNKS, GROWS, 128), f32),
            pltpu.VMEM((5 * SLOT, 384), f32),
            pltpu.VMEM((384, 384), f32),
            pltpu.VMEM((128, 128), f32),
            pltpu.VMEM((CHUNKS, SROW, 128), f32),
            pltpu.VMEM((2, SROW, 128), f32),
            pltpu.VMEM((2, 8, 128), f32),
            pltpu.VMEM((2, CHUNKS, 4, 128), f32),
            pltpu.VMEM((2, 2, 4, 128), f32),
            pltpu.VMEM((2, SROW, 128), f32),
            pltpu.VMEM((2, 8, 128), f32),
            pltpu.VMEM((2, 2, 8, 128), f32),
            pltpu.VMEM((2, CHUNKS, 4, 128), f32),
            pltpu.VMEM((2, 2, 4, 128), f32),
            pltpu.VMEM((2, 2, 4, 128), f32),
            pltpu.VMEM((2, 2, 2, 4, 128), f32),
            pltpu.SemaphoreType.DMA((18,)),
            pltpu.SemaphoreType.DMA((26,)),
            pltpu.SemaphoreType.DMA((26,)),
        ],
        compiler_params=pltpu.CompilerParams(
            collective_id=0, has_side_effects=True, vmem_limit_bytes=LIMIT
        ),
    )(
        *fields,
        node_index.reshape(125, 1, elements),
        inv_map.reshape(9, 125, 1, elements),
        *elems,
        jnp.asarray(deriv),
        jnp.asarray(back),
        jnp.asarray(spread, jnp.bfloat16),
    )
    final = pl.pallas_call(
        finish,
        out_shape=[out] * 3,
        in_specs=[vmem] * 3,
        out_specs=[hbm] * 3,
        scratch_shapes=[pltpu.VMEM((3, nodes), f32), pltpu.SemaphoreType.DMA((9,))],
        compiler_params=pltpu.CompilerParams(vmem_limit_bytes=LIMIT),
    )(*[pltpu.with_memory_space_constraint(x, pltpu.VMEM) for x in result])
    return tuple(x.reshape(displ.shape) for x in final)


def solution(mesh):
    field = P(None, "gx", "gy", "gz", None)
    elem = P("gx", "gy", "gz", None, None)
    placed = (field,) * 3 + (elem, P("gx", "gy", "gz", None, None, None)) + (elem,) * 4
    return jax.shard_map(
        body, mesh=mesh, in_specs=placed, out_specs=(field,) * 3, check_vma=False
    )
```

```python
import jax
import jax.numpy as jnp
import numpy as np
from jax import lax
from jax.experimental import pallas as pl
from jax.experimental.pallas import tpu as pltpu
from jax.sharding import PartitionSpec as P

EX = 4
EY = 16
EZ = 2
NX = 4 * EX + 1
NY = 4 * EY + 1
NZ = 4 * EZ + 1
PLANE = NY * NZ
CHUNKS = -(-PLANE // 128)
STRIDE = 4 * NZ
SPAN = 5 * NZ
SLOT = 48
SROW = 72
TAIL = PLANE - NZ - 128 * (CHUNKS - 1)
PITCH = 14

LIMIT = 65 * 1000 * 1000

time_step = 0.1
MESH = pl.DeviceIdType.MESH


def derivative_table():
    points = np.array([-1.0, -np.sqrt(3.0 / 7.0), 0.0, np.sqrt(3.0 / 7.0), 1.0])
    count = points.shape[0]
    weights = np.array(
        [
            1.0 / np.prod([points[s] - points[o] for o in range(count) if o != s])
            for s in range(count)
        ]
    )
    table = np.zeros((count, count))
    for t in range(count):
        for s in range(count):
            if t != s:
                table[t, s] = weights[s] / weights[t] / (points[t] - points[s])
        table[t, t] = -np.sum(table[t])
    return table


def constants():
    table = derivative_table()
    eye = np.eye(5)
    parts = [
        np.kron(table, np.kron(eye, eye)),
        np.kron(eye, np.kron(table, eye)),
        np.kron(eye, np.kron(eye, table)),
    ]
    pad = np.zeros((125, 5 * SLOT))
    for a in range(5):
        for b in range(5):
            for c in range(5):
                pad[a * 25 + 5 * b + c, a * SLOT + NZ * b + c] = 1.0
    deriv = np.zeros((384, 5 * SLOT), np.float32)
    for l in range(3):
        deriv[l * 128 : l * 128 + 125] = parts[l] @ pad
    spread = np.zeros((5 * SLOT, 128), np.float32)
    spread[:, :125] = pad.T
    return deriv, -deriv.T.copy(), spread


def split2(x):
    hi = x.astype(jnp.bfloat16)
    low = (x - hi.astype(jnp.float32)).astype(jnp.bfloat16)
    return (hi, low)


def halves(x):
    hi = np.asarray(x, jnp.bfloat16)
    low = np.asarray(x - hi.astype(np.float32), jnp.bfloat16)
    return np.stack([hi, low])


def product(pair, y):
    hi, low = split2(y)
    dot = lambda a, b: jnp.dot(a, b, preferred_element_type=jnp.float32)
    return dot(pair[0], hi) + dot(pair[0], low) + dot(pair[1], hi)


def stacked(x, y, dims):
    rows = x.shape[0]
    out = lax.dot_general(
        jnp.concatenate(split2(x), axis=0),
        y,
        (dims, ((), ())),
        preferred_element_type=jnp.float32,
    )
    return out[:rows] + out[rows:]


def ways():
    steps = (0, -1, 1)
    found = [(x, y, z) for z in steps for y in steps for x in steps][1:]
    half = [w for w in found if w > (0, 0, 0)]
    half.sort(key=lambda w: (sum(map(abs, w)), -abs(w[2])))
    other = [tuple(-v for v in w) for w in half]
    return half + other[::-1]


WAYS = ways()


def neighbours():
    names = ("gx", "gy", "gz")
    spots = [lax.axis_index(n) for n in names]
    sizes = [lax.axis_size(n) for n in names]
    links = []
    for way in WAYS:
        there = None
        peer = {}
        for n, s, z, w in zip(names, spots, sizes, way):
            if w:
                ok = s > 0 if w < 0 else s < z - 1
                there = ok if there is None else there & ok
                peer[n] = s + w
        links.append((way, there, peer))
    return links


def classes():
    found = [((), None)]
    for name in ("gx", "gy", "gz"):
        size, spot = lax.axis_size(name), lax.axis_index(name)
        inner = (spot > 0) & (spot < size - 1)
        choices = [(min(size - 1, 1), None)]
        if size > 2:
            choices = [(1, jnp.logical_not(inner)), (2, inner)]
        grown = []
        for counts, here in found:
            for count, ok in choices:
                both = here if ok is None else ok if here is None else here & ok
                grown.append((counts + (count,), both))
        found = grown
    return [(counts, True if here is None else here) for counts, here in found]


def squeezed(ref):
    return ref.at[:, 0] if len(ref.shape) == 3 else ref.at[:, :, 0]


def kernel(
    displ, veloc, accel, node, inv, jac, lame, shear, dens,
    deriv_ref, back_ref, spread_ref,
    pos_out, vel_out, acc_out,
    deriv_s, back_s, spread_s,
    d_s, v_s, a_s, node_s, inv_s, elem_s,
    picks_s, ends_s, w_s, u_s, fl_s, md_s, grid_s,
    m_send, p_send, x_send, e_send, q_send, f_send, c_send,
    m_recv, p_recv, q_recv, x_recv, e_recv, f_recv, c_recv,
    tally, in_sem, send_sem, recv_sem,
):
    links = neighbours()
    head = node.at[pl.ds(0, 1), 0]
    copies = [pltpu.make_async_copy(head, node_s, in_sem.at[0])]
    for k, (src, dst) in enumerate(((displ, d_s), (veloc, v_s), (accel, a_s))):
        copies.append(pltpu.make_async_copy(src.at[:, 0], dst, in_sem.at[1 + k]))
    whole = squeezed(inv)
    copies.append(pltpu.make_async_copy(whole, inv_s, in_sem.at[4]))
    for k, src in enumerate((jac, lame, shear, dens)):
        copies.append(pltpu.make_async_copy(squeezed(src), elem_s.at[k], in_sem.at[5]))
    consts = ((deriv_ref, deriv_s), (back_ref, back_s), (spread_ref, spread_s))
    for k, (src, dst) in enumerate(consts):
        copies.append(pltpu.make_async_copy(src, dst, in_sem.at[6 + k]))
    for cp in copies:
        cp.start()
    w_s[768:, :] = jnp.zeros((128, 128), jnp.float32)
    u_s[...] = jnp.zeros_like(u_s)
    fl_s[...] = jnp.zeros_like(fl_s)
    md_s[...] = jnp.zeros_like(md_s)
    for ref in (m_recv, p_recv, q_recv, x_recv, e_recv, f_recv, c_recv):
        ref[...] = jnp.zeros_like(ref)
    copies[0].wait()
    corner = node_s[0:1, :].astype(jnp.float32)
    x0 = jnp.floor((corner + 0.5) * (1.0 / PLANE))
    rem = corner - PLANE * x0
    y0 = jnp.floor((rem + 0.5) * (1.0 / NZ))
    z0 = rem - NZ * y0
    upper = z0 > 1.0
    last = x0 > NX - 6.0
    iota = lax.broadcasted_iota(jnp.int32, (256, 128), 0).astype(jnp.float32)
    goal = 4.0 * y0 + x0
    for a in range(5):
        aim = goal + a if a < 4 else jnp.where(last, -1.0, goal + a)
        picks_s[:, 128 * a : 128 * (a + 1)] = jnp.where(iota == aim, 1.0, 0.0).astype(jnp.bfloat16)
    goal = 2.0 * y0
    for c in range(4):
        aim = jnp.where(last, goal + c, -1.0)
        ends_s[:, 128 * c : 128 * (c + 1)] = jnp.where(iota[0:128] == aim, 1.0, 0.0).astype(jnp.bfloat16)

    barrier = pltpu.get_barrier_semaphore()
    for way, there, peer in links:

        @pl.when(there)
        def _():
            pl.semaphore_signal(barrier, inc=1, device_id=peer, device_id_type=MESH)

    for cp in copies[1:4]:
        cp.wait()

    half = 0.5 * time_step
    pos = d_s[...] + time_step * v_s[...] + (half * time_step) * a_s[...]
    pos_out[...] = pos

    lane = lax.broadcasted_iota(jnp.int32, (1, 128), 1)

    def chunk(q):
        width = min(128, PLANE * NX - 128 * q)
        part = pos_out[:, 128 * q : 128 * q + width]
        if width < 128:
            part = jnp.concatenate([part, jnp.zeros((3, 128 - width), jnp.float32)], axis=1)
        return part

    for x in range(NX):
        for ey in range(EY):
            q, at = divmod(PLANE * x + STRIDE * ey, 128)
            part = chunk(q)
            if at + SPAN > 128:
                part = jnp.where(lane >= at, part, chunk(q + 1))
            part = pltpu.roll(part, 128 - at, 1) if at else part
            if x < NX - 1:
                w_s[pl.ds(16 * ey + x, 3, stride=256), :] = part
            else:
                w_s[768 + 8 * ey : 768 + 8 * ey + 3, :] = part
    turned = [jnp.transpose(w_s[256 * c : 256 * (c + 1), :])[:SLOT] for c in range(3)]
    turned.append(jnp.transpose(w_s[768:896, :])[:SLOT])
    gathered = stacked(jnp.concatenate(turned[:3], axis=0), picks_s[...], ((1,), (0,)))
    beyond = stacked(turned[3], ends_s[:, : 3 * 128], ((1,), (0,)))
    for c in range(3):
        for a in range(5):
            part = gathered[SLOT * c : SLOT * (c + 1), 128 * a : 128 * (a + 1)]
            if a == 4:
                part = part + beyond[:, 128 * c : 128 * (c + 1)]
            part = jnp.where(upper, pltpu.roll(part, SLOT - 4, 0), part)
            u_s[SLOT * a : SLOT * (a + 1), 128 * c : 128 * (c + 1)] = part

    for cp in copies[9:]:
        cp.wait()
    local = product(deriv_s, u_s[...])
    copies[4].wait()
    pltpu.make_async_copy(whole.at[pl.ds(0, 4)], elem_s, in_sem.at[5]).wait()
    grads = [
        [local[l * 128 : l * 128 + 125, c * 128 : (c + 1) * 128] for c in range(3)]
        for l in range(3)
    ]
    maps = [[inv_s[3 * l + j] for j in range(3)] for l in range(3)]
    weight, lam, mu, dens_e = (elem_s[k] for k in range(4))
    h = [
        [sum(grads[l][c] * maps[l][j] for l in range(3)) for j in range(3)] for c in range(3)
    ]
    div = lam * (h[0][0] + h[1][1] + h[2][2])
    stress = [[None] * 3 for _ in range(3)]
    for c in range(3):
        for j in range(c, 3):
            s = mu * (h[c][j] + h[j][c])
            if c == j:
                s = s + div
            s = s * weight
            stress[c][j] = s
            stress[j][c] = s
    for l in range(3):
        for c in range(3):
            fl_s[l * 128 : l * 128 + 125, c * 128 : (c + 1) * 128] = sum(
                stress[c][j] * maps[l][j] for j in range(3)
            )
    md_s[0:125, :] = dens_e * weight
    terms = product(back_s, fl_s[...])
    heavy = sum(
        jnp.dot(spread_s[...], part, preferred_element_type=jnp.float32)
        for part in split2(md_s[...])
    )

    columns = []
    tops = []
    for c in range(4):
        blocks = []
        for a in range(5):
            at = slice(SLOT * a, SLOT * (a + 1))
            part = terms[at, 128 * c : 128 * (c + 1)] if c < 3 else heavy[at]
            blocks.append(jnp.where(upper, pltpu.roll(part, 4, 0), part))
        columns.append(jnp.concatenate(blocks, axis=1))
        tops.append(blocks[4])
    placed = stacked(jnp.concatenate(columns, axis=0), picks_s[...], ((1,), (1,)))
    topped = stacked(jnp.concatenate(tops, axis=1), ends_s[...], ((1,), (1,)))
    blank = jnp.zeros((128, 128 - SLOT), jnp.float32)
    for c in range(5):
        if c < 4:
            part = placed[SLOT * c : SLOT * (c + 1)]
            halves_ = [part[:, :128], part[:, 128:]]
            first, many = 16 * c, 16
        else:
            halves_ = [topped]
            first, many = 64, 8
        back = [jnp.concatenate([jnp.transpose(h), blank], axis=1) for h in halves_]
        back = jnp.concatenate(back, axis=0) if c < 4 else back[0]
        sums = [None] * CHUNKS
        for ey in range(EY):
            j, at = divmod(STRIDE * ey, 128)
            part = back[many * ey : many * (ey + 1)]
            part = pltpu.roll(part, at, 1) if at else part
            pieces = [(j, part)]
            if at + SLOT > 128:
                pieces = [
                    (j, jnp.where(lane >= at, part, 0.0)),
                    (j + 1, jnp.where(lane < at, part, 0.0)),
                ]
            for k, piece in pieces:
                sums[k] = piece if sums[k] is None else sums[k] + piece
        for j in range(CHUNKS):
            grid_s[j, first : first + many, :] = sums[j]

    sides = (pl.ds(0, 4, stride=16), pl.ds(64, 4))
    lanes = lax.broadcasted_iota(jnp.int32, (SROW, 128), 1)
    far = CHUNKS - 1
    edge = grid_s[far]
    rims = (grid_s[0], pltpu.roll(edge, 128 - TAIL, 1))
    lane8 = lax.broadcasted_iota(jnp.int32, (8, 128), 1)
    for side in range(2):
        for j in range(CHUNKS):
            x_send[side, j] = grid_s[j, sides[side], :]
    for sy in range(2):
        rows = jnp.concatenate([x_send[0, far * sy], x_send[1, far * sy]], axis=0)
        shift, first = (TAIL, TAIL) if sy == 0 else (128 - TAIL, 0)
        got = pltpu.roll(rows, shift, 1)
        got = jnp.where((lane8 >= first) & (lane8 < first + NZ), got, 0.0)
        f_send[0, sy] = got[:4]
        f_send[1, sy] = got[4:]
        for sz in range(2):
            got = pltpu.roll(rows, (shift + (8 if sz == 0 else 128 - 8)) % 128, 1)
            got = jnp.where(lane8 == first + (NZ - 1) * (1 - sz), got, 0.0)
            c_send[0, sy, sz] = got[:4]
            c_send[1, sy, sz] = got[4:]
        packed = None
        for i in range(SROW // 8):
            got = jnp.where(lane8 < NZ, rims[sy][8 * i : 8 * i + 8], 0.0)
            got = pltpu.roll(got, PITCH * i, 1) if i else got
            packed = got if packed is None else packed + got
        p_send[sy] = packed
        place = lax.rem(lane8, PITCH)
        for sz in range(2):
            got = jnp.where(place == (NZ - 1) * sz, packed, 0.0)
            q_send[sy, sz] = pltpu.roll(got, 8 if sz == 0 else 128 - 8, 1)

    def route(way):
        sx, sy, sz = ((w + 1) // 2 for w in way)
        ox, oy, oz = 1 - sx, 1 - sy, 1 - sz
        dx, dy, dz = (w != 0 for w in way)
        if dx and dy and dz:
            return c_send.at[sx, sy, sz], c_recv.at[ox, oy, oz]
        if dx and dy:
            return f_send.at[sx, sy], f_recv.at[ox, oy]
        if dx and dz:
            return e_send.at[sx, sz], e_recv.at[ox, oz]
        if dy and dz:
            return q_send.at[sy, sz], q_recv.at[oy, oz]
        if dx:
            return x_send.at[sx], x_recv.at[ox]
        if dy:
            return p_send.at[sy], p_recv.at[oy]
        return m_send.at[sz], m_recv.at[oz]

    def copy(source, target, peer):
        return pltpu.make_async_remote_copy(
            src_ref=source,
            dst_ref=target,
            send_sem=send_sem.at[0],
            recv_sem=recv_sem.at[0],
            device_id=peer,
            device_id_type=MESH,
        )

    def await_all(settle):
        for (nx, ny, nz), here in classes():
            count = nx * CHUNKS + nx * ny + nx * nz + nx * ny * nz
            count += 2 * ny + 2 * ny * nz + nz * SROW // 4
            whole = tally.at[pl.ds(0, count)]

            @pl.when(here)
            def _():
                settle(copy(whole, whole, links[0][2]))

    peers = sum(there.astype(jnp.int32) for way, there, peer in links)
    pl.semaphore_wait(barrier, peers)
    farthest = sorted(range(len(WAYS)), key=lambda k: -sum(map(abs, WAYS[k])))

    def depart(chosen):
        for k in farthest:
            way, there, peer = links[k]
            if chosen(way):

                @pl.when(there)
                def _():
                    copy(*route(way), peer).start()

    flat = lambda way: way[1] == 0 and way[2] != 0
    depart(lambda way: not flat(way))
    for dz in range(2):
        face = None
        source = jnp.minimum(NZ * lanes + (NZ - 1) * dz, 128 * CHUNKS - 1)
        for j in range(CHUNKS):
            got = jnp.take_along_axis(
                grid_s[j], source & 127, axis=1, mode="promise_in_bounds"
            )
            face = got if face is None else jnp.where(source >= 128 * j, got, face)
        m_send[dz] = jnp.where(lanes < NY, face, 0.0)
        for side in range(2):
            e_send[side, dz] = m_send[dz, sides[side], :]
    depart(flat)
    vel_out[...] = v_s[...] + half * a_s[...]

    await_all(lambda copied: copied.wait_recv())

    for dz in range(2):
        for sx in range(2):
            m_recv[dz, sides[sx], :] += e_recv[sx, dz]
    full = [m_recv[dz] for dz in range(2)]
    strips = []
    for sy in range(2):
        sums = p_recv[sy] + q_recv[sy, 0] + q_recv[sy, 1]
        parts = []
        for i in range(SROW // 8):
            shift = (TAIL * sy - PITCH * i) % 128
            got = pltpu.roll(sums, shift, 1) if shift else sums
            parts.append(
                jnp.where((lane8 >= TAIL * sy) & (lane8 < TAIL * sy + NZ), got, 0.0)
            )
        strips.append(jnp.concatenate(parts, axis=0))
        for sx in range(2):
            x_recv[sx, far * sy] += f_recv[sx, sy] + (c_recv[sx, sy, 0] + c_recv[sx, sy, 1])
    for j in range(CHUNKS):
        node = lanes + 128 * j
        along = lax.div(node, NZ)
        depth = node - NZ * along
        sums = grid_s[j]
        for dz in range(2):
            got = jnp.take_along_axis(
                full[dz], jnp.minimum(along, 127), axis=1, mode="promise_in_bounds"
            )
            sums = sums + jnp.where((depth == (NZ - 1) * dz) & (along < NY), got, 0.0)
        if j == 0:
            sums = sums + strips[0]
        if j == far:
            sums = sums + strips[1]
        grid_s[j] = sums
        for sx in range(2):
            grid_s[j, sides[sx], :] += x_recv[sx, j]
        mass = grid_s[j, 48:64, :]
        for c in range(3):
            grid_s[j, 16 * c : 16 * c + 16, :] = grid_s[j, 16 * c : 16 * c + 16, :] / mass
        grid_s[j, 64:67, :] = grid_s[j, 64:67, :] / grid_s[j, 67:68, :]

    for x in range(NX):
        rows = pl.ds(x, 3, stride=16) if x < NX - 1 else pl.ds(64, 3)
        for j in range(CHUNKS):
            width = min(128, PLANE - 128 * j)
            at = PLANE * x + 128 * j
            acc_out[:, at : at + width] = grid_s[j, rows, 0:width]
    await_all(lambda copied: copied.wait_send())


def finish(pos, vel, acc, pos_out, vel_out, acc_out, v_s, sem):
    def put(src, dst, k):
        copy = pltpu.make_async_copy(src, dst.at[:, 0], sem.at[k])
        copy.start()
        return copy

    copies = [put(pos, pos_out, 0), put(acc, acc_out, 1)]
    v_s[...] = vel[...] + (0.5 * time_step) * acc[...]
    copies.append(put(v_s, vel_out, 2))
    for cp in copies:
        cp.wait()


def body(displ, veloc, accel, node_index, inv_map, jac_weight, lame_first, shear_mod, density):
    nodes = displ.shape[4]
    elements = node_index.shape[4]
    deriv, back, spread = constants()
    deriv, back = halves(deriv), halves(back)
    fields = [x.reshape(3, 1, nodes) for x in (displ, veloc, accel)]
    elems = [
        x.reshape(125, 1, elements) for x in (jac_weight, lame_first, shear_mod, density)
    ]
    vmem = pl.BlockSpec(memory_space=pltpu.VMEM)
    hbm = pl.BlockSpec(memory_space=pltpu.HBM)
    f32 = jnp.float32
    out = jax.ShapeDtypeStruct((3, 1, nodes), f32)
    result = pl.pallas_call(
        kernel,
        out_shape=[pltpu.VMEM((3, nodes), f32)] * 3,
        in_specs=[hbm] * 12,
        out_specs=[vmem] * 3,
        scratch_shapes=[
            pltpu.VMEM(deriv.shape, jnp.bfloat16),
            pltpu.VMEM(back.shape, jnp.bfloat16),
            pltpu.VMEM(spread.shape, jnp.bfloat16),
            pltpu.VMEM((3, nodes), f32),
            pltpu.VMEM((3, nodes), f32),
            pltpu.VMEM((3, nodes), f32),
            pltpu.VMEM((1, elements), jnp.int32),
            pltpu.VMEM((9, 125, elements), f32),
            pltpu.VMEM((4, 125, elements), f32),
            pltpu.VMEM((256, 5 * 128), jnp.bfloat16),
            pltpu.VMEM((128, 4 * 128), jnp.bfloat16),
            pltpu.VMEM((896, 128), f32),
            pltpu.VMEM((5 * SLOT, 384), f32),
            pltpu.VMEM((384, 384), f32),
            pltpu.VMEM((128, 128), f32),
            pltpu.VMEM((CHUNKS, SROW, 128), f32),
            pltpu.VMEM((2, SROW, 128), f32),
            pltpu.VMEM((2, 8, 128), f32),
            pltpu.VMEM((2, CHUNKS, 4, 128), f32),
            pltpu.VMEM((2, 2, 4, 128), f32),
            pltpu.VMEM((2, 2, 8, 128), f32),
            pltpu.VMEM((2, 2, 4, 128), f32),
            pltpu.VMEM((2, 2, 2, 4, 128), f32),
            pltpu.VMEM((2, SROW, 128), f32),
            pltpu.VMEM((2, 8, 128), f32),
            pltpu.VMEM((2, 2, 8, 128), f32),
            pltpu.VMEM((2, CHUNKS, 4, 128), f32),
            pltpu.VMEM((2, 2, 4, 128), f32),
            pltpu.VMEM((2, 2, 4, 128), f32),
            pltpu.VMEM((2, 2, 2, 4, 128), f32),
            pltpu.VMEM((2 * SROW // 4 + 2 * CHUNKS + 28, 4, 128), f32),
            pltpu.SemaphoreType.DMA((9,)),
            pltpu.SemaphoreType.DMA((1,)),
            pltpu.SemaphoreType.DMA((1,)),
        ],
        compiler_params=pltpu.CompilerParams(
            collective_id=0, has_side_effects=True, vmem_limit_bytes=LIMIT
        ),
    )(
        *fields,
        node_index.reshape(125, 1, elements),
        inv_map.reshape(9, 125, 1, elements),
        *elems,
        jnp.asarray(deriv),
        jnp.asarray(back),
        jnp.asarray(spread, jnp.bfloat16),
    )
    final = pl.pallas_call(
        finish,
        out_shape=[out] * 3,
        in_specs=[vmem] * 3,
        out_specs=[hbm] * 3,
        scratch_shapes=[pltpu.VMEM((3, nodes), f32), pltpu.SemaphoreType.DMA((3,))],
        compiler_params=pltpu.CompilerParams(vmem_limit_bytes=LIMIT),
    )(*[pltpu.with_memory_space_constraint(x, pltpu.VMEM) for x in result])
    return tuple(x.reshape(displ.shape) for x in final)


def solution(mesh):
    field = P(None, "gx", "gy", "gz", None)
    elem = P("gx", "gy", "gz", None, None)
    placed = (field,) * 3 + (elem, P("gx", "gy", "gz", None, None, None)) + (elem,) * 4
    return jax.shard_map(
        body, mesh=mesh, in_specs=placed, out_specs=(field,) * 3, check_vma=False
    )
```

```python
import jax
import jax.numpy as jnp
import numpy as np
from jax import lax
from jax.experimental import pallas as pl
from jax.experimental.pallas import tpu as pltpu
from jax.sharding import PartitionSpec as P

EX = 4
EY = 16
EZ = 2
NX = 4 * EX + 1
NY = 4 * EY + 1
NZ = 4 * EZ + 1
PLANE = NY * NZ
CHUNKS = -(-PLANE // 128)
STRIDE = 4 * NZ
SPAN = 5 * NZ
SLOT = 48
SROW = 72
TAIL = PLANE - NZ - 128 * (CHUNKS - 1)
PITCH = 14
SPLITS = ((0, 7), (7, 6))
PAIRS = tuple(((c, a), (c, a + 1)) for c in range(4) for a in (0, 2))

LIMIT = 65 * 1000 * 1000

time_step = 0.1
MESH = pl.DeviceIdType.MESH


def derivative_table():
    points = np.array([-1.0, -np.sqrt(3.0 / 7.0), 0.0, np.sqrt(3.0 / 7.0), 1.0])
    count = points.shape[0]
    weights = np.array(
        [
            1.0 / np.prod([points[s] - points[o] for o in range(count) if o != s])
            for s in range(count)
        ]
    )
    table = np.zeros((count, count))
    for t in range(count):
        for s in range(count):
            if t != s:
                table[t, s] = weights[s] / weights[t] / (points[t] - points[s])
        table[t, t] = -np.sum(table[t])
    return table


def constants():
    table = derivative_table()
    eye = np.eye(5)
    parts = [
        np.kron(table, np.kron(eye, eye)),
        np.kron(eye, np.kron(table, eye)),
        np.kron(eye, np.kron(eye, table)),
    ]
    pad = np.zeros((125, 5 * SLOT))
    for a in range(5):
        for b in range(5):
            for c in range(5):
                pad[a * 25 + 5 * b + c, a * SLOT + NZ * b + c] = 1.0
    deriv = np.zeros((384, 5 * SLOT), np.float32)
    for l in range(3):
        deriv[l * 128 : l * 128 + 125] = parts[l] @ pad
    spread = np.zeros((5 * SLOT, 128), np.float32)
    spread[:, :125] = pad.T
    return deriv, -deriv.T.copy(), spread


def split2(x):
    hi = x.astype(jnp.bfloat16)
    low = (x - hi.astype(jnp.float32)).astype(jnp.bfloat16)
    return (hi, low)


def halves(x):
    hi = np.asarray(x, jnp.bfloat16)
    low = np.asarray(x - hi.astype(np.float32), jnp.bfloat16)
    return np.stack([hi, low])


def product(pair, y):
    hi, low = split2(y)
    dot = lambda a, b: jnp.dot(a, b, preferred_element_type=jnp.float32)
    return dot(pair[0], hi) + dot(pair[0], low) + dot(pair[1], hi)


def ways():
    steps = (0, -1, 1)
    found = [(x, y, z) for z in steps for y in steps for x in steps][1:]
    half = [w for w in found if w > (0, 0, 0)]
    half.sort(key=lambda w: (sum(map(abs, w)), -abs(w[2])))
    other = [tuple(-v for v in w) for w in half]
    return half + other[::-1]


WAYS = ways()


def neighbours():
    names = ("gx", "gy", "gz")
    spots = [lax.axis_index(n) for n in names]
    sizes = [lax.axis_size(n) for n in names]
    links = []
    for way in WAYS:
        there = None
        peer = {}
        for n, s, z, w in zip(names, spots, sizes, way):
            if w:
                ok = s > 0 if w < 0 else s < z - 1
                there = ok if there is None else there & ok
                peer[n] = s + w
        links.append((way, there, peer))
    return links


def classes():
    found = [((), None)]
    for name in ("gx", "gy", "gz"):
        size, spot = lax.axis_size(name), lax.axis_index(name)
        inner = (spot > 0) & (spot < size - 1)
        choices = [(min(size - 1, 1), None)]
        if size > 2:
            choices = [(1, jnp.logical_not(inner)), (2, inner)]
        grown = []
        for counts, here in found:
            for count, ok in choices:
                both = here if ok is None else ok if here is None else here & ok
                grown.append((counts + (count,), both))
        found = grown
    return [(counts, True if here is None else here) for counts, here in found]


def squeezed(ref):
    return ref.at[:, 0] if len(ref.shape) == 3 else ref.at[:, :, 0]


def kernel(
    displ, veloc, accel, node, inv, jac, lame, shear, dens,
    deriv_ref, back_ref, spread_ref,
    pos_out, vel_out, acc_out,
    deriv_s, back_s, spread_s,
    d_s, v_s, a_s, node_s, raw_s,
    order_s, sorted_s, w_s, z_s, top_s, u_s, fl_s, md_s, grid_s,
    m_send, p_send, x_send, e_send, q_send, f_send, c_send,
    m_recv, p_recv, q_recv, x_recv, e_recv, f_recv, c_recv,
    tally, in_sem, send_sem, recv_sem,
):
    links = neighbours()
    head = node.at[pl.ds(0, 1), 0]
    copies = [pltpu.make_async_copy(head, node_s, in_sem.at[0])]
    for k, (src, dst) in enumerate(((displ, d_s), (veloc, v_s), (accel, a_s))):
        copies.append(pltpu.make_async_copy(src.at[:, 0], dst, in_sem.at[1 + k]))
    whole = squeezed(inv)
    point = pl.ds(0, 125)
    copies.append(pltpu.make_async_copy(whole, raw_s.at[pl.ds(0, 9), point], in_sem.at[4]))
    for k, src in enumerate((jac, lame, shear, dens)):
        copies.append(pltpu.make_async_copy(squeezed(src), raw_s.at[9 + k, point], in_sem.at[5]))
    consts = ((deriv_ref, deriv_s), (back_ref, back_s), (spread_ref, spread_s))
    for k, (src, dst) in enumerate(consts):
        copies.append(pltpu.make_async_copy(src, dst, in_sem.at[6 + k]))
    for cp in copies:
        cp.start()
    z_s[...] = jnp.zeros_like(z_s)
    u_s[...] = jnp.zeros_like(u_s)
    fl_s[...] = jnp.zeros_like(fl_s)
    md_s[...] = jnp.zeros_like(md_s)
    for ref in (m_recv, p_recv, q_recv, x_recv, e_recv, f_recv, c_recv):
        ref[...] = jnp.zeros_like(ref)
    copies[0].wait()
    corner = node_s[0:1, :].astype(jnp.float32)
    x0 = jnp.floor((corner + 0.5) * (1.0 / PLANE))
    rem = corner - PLANE * x0
    y0 = jnp.floor((rem + 0.5) * (1.0 / NZ))
    z0 = rem - NZ * y0
    goal = EY * EX * 0.25 * z0 + EX * 0.25 * y0 + 0.25 * x0
    goal = jnp.transpose(jnp.broadcast_to(goal, (128, 128)))
    slots = lax.broadcasted_iota(jnp.int32, (128, 128), 1).astype(jnp.float32)
    order = jnp.where(slots == goal, 1.0, 0.0).astype(jnp.bfloat16)
    order_s[0:128, :] = order
    order_s[128:256, :] = order
    barrier = pltpu.get_barrier_semaphore()
    for way, there, peer in links:

        @pl.when(there)
        def _():
            pl.semaphore_signal(barrier, inc=1, device_id=peer, device_id_type=MESH)

    for cp in copies[1:4]:
        cp.wait()

    half = 0.5 * time_step
    pos = d_s[...] + time_step * v_s[...] + (half * time_step) * a_s[...]
    pos_out[...] = pos

    lane = lax.broadcasted_iota(jnp.int32, (1, 128), 1)

    def chunk(q):
        width = min(128, PLANE * NX - 128 * q)
        part = pos_out[:, 128 * q : 128 * q + width]
        if width < 128:
            part = jnp.concatenate([part, jnp.zeros((3, 128 - width), jnp.float32)], axis=1)
        return part

    ahead = (4 * PLANE - STRIDE) // 128
    blank = jnp.zeros((3, 128), jnp.float32)
    single = [chunk(q) for q in range(-(-PLANE * NX // 128))]
    double = [
        jnp.concatenate([v, single[q + ahead] if q + ahead < len(single) else blank], axis=0)
        for q, v in enumerate(single)
    ]

    def window(source, x, ey):
        q, at = divmod(PLANE * x + STRIDE * ey, 128)
        part = source[q]
        if at + SPAN > 128:
            part = jnp.where(lane >= at, part, source[q + 1])
        return pltpu.roll(part, 128 - at, 1) if at else part

    def keep(x, ey, part):
        ex, a = divmod(x, 4)
        spots = [(a, ex)] if x < NX - 1 else []
        if x and a == 0:
            spots.append((4, ex - 1))
        for a, ex in spots:
            first = 3 * ((a * EY + ey) * EX + ex)
            w_s[first : first + 3, :] = part

    for x in range(NX):
        paired = x < NX - 1 and x % 8 < 4
        for ey in range(EY):
            if paired:
                part = window(double, x, ey)
                keep(x, ey, part[:3])
                if ey:
                    keep(x + 4, ey - 1, part[3:])
            elif x == NX - 1 or ey == EY - 1:
                keep(x, ey, window(single, x, ey))

    copies[4].wait()
    pltpu.make_async_copy(
        whole.at[pl.ds(0, 4)], raw_s.at[pl.ds(9, 4), point], in_sem.at[5]
    ).wait()
    copies[9].wait()
    for first, many in SPLITS:
        raw = raw_s[first : first + many].reshape(many * 128, 128)
        sorted_s[first : first + many] = jnp.dot(
            jnp.concatenate(split2(raw), axis=1),
            order_s[...],
            preferred_element_type=jnp.float32,
        ).reshape(many, 128, 128)

    left = lax.broadcasted_iota(jnp.int32, (SLOT, 128), 1) < 64
    each = EX * EY

    def block(c, a):
        return w_s[pl.ds(3 * each * a + c, each, stride=3), :]

    for (c, a), (d, b) in PAIRS[:6] + (((0, 4), (1, 4)), ((2, 4), (2, 4))):
        turned = jnp.transpose(jnp.concatenate([block(c, a), block(d, b)], axis=0))[:SLOT]
        other = pltpu.roll(turned, 64, 1)
        rise = lambda v: pltpu.roll(v, SLOT - 4, 0)
        u_s[SLOT * a : SLOT * (a + 1), 128 * c : 128 * (c + 1)] = jnp.where(
            left, turned, rise(other)
        )
        if (c, a) != (d, b):
            u_s[SLOT * b : SLOT * (b + 1), 128 * d : 128 * (d + 1)] = jnp.where(
                left, other, rise(turned)
            )

    local = product(deriv_s, u_s[...])
    grads = [
        [local[l * 128 : l * 128 + 125, c * 128 : (c + 1) * 128] for c in range(3)]
        for l in range(3)
    ]
    maps = [[sorted_s[3 * l + j, 0:125] for j in range(3)] for l in range(3)]
    weight, lam, mu, dens_e = (sorted_s[9 + k, 0:125] for k in range(4))
    h = [
        [sum(grads[l][c] * maps[l][j] for l in range(3)) for j in range(3)] for c in range(3)
    ]
    div = lam * (h[0][0] + h[1][1] + h[2][2])
    stress = [[None] * 3 for _ in range(3)]
    for c in range(3):
        for j in range(c, 3):
            s = mu * (h[c][j] + h[j][c])
            if c == j:
                s = s + div
            s = s * weight
            stress[c][j] = s
            stress[j][c] = s
    for l in range(3):
        for c in range(3):
            fl_s[l * 128 : l * 128 + 125, c * 128 : (c + 1) * 128] = sum(
                stress[c][j] * maps[l][j] for j in range(3)
            )
    md_s[0:125, :] = dens_e * weight
    for cp in copies[10:]:
        cp.wait()
    terms = product(back_s, fl_s[...])
    heavy = sum(
        jnp.dot(spread_s[...], part, preferred_element_type=jnp.float32)
        for part in split2(md_s[...])
    )

    def term(c, a):
        at = slice(SLOT * a, SLOT * (a + 1))
        return terms[at, 128 * c : 128 * (c + 1)] if c < 3 else heavy[at]

    sink = lambda v: pltpu.roll(v, 4, 0)
    tail = jnp.zeros((128, 128 - SLOT), jnp.float32)
    crest = {}
    rows = lax.broadcasted_iota(jnp.int32, (each, 128), 0)
    for (c, a), (d, b) in (((0, 4), (1, 4)), ((2, 4), (3, 4))) + PAIRS:
        one, two = term(c, a), term(d, b)
        both = jnp.where(left, one, sink(two)) + pltpu.roll(jnp.where(left, two, sink(one)), 64, 1)
        turned = jnp.concatenate([jnp.transpose(both), tail], axis=1)
        for k, part in (((c, a), turned[:each]), ((d, b), turned[each:])):
            if k[1] == 4:
                top_s[each * k[0] : each * (k[0] + 1), :] = part
                crest[k[0]] = jnp.where(rows % EX == 0, 0.0, pltpu.roll(part, 1, 0))
                continue
            if k[1] == 0:
                part = part + crest[k[0]]
            for ey in range(EY):
                first = ((k[0] * EY + ey) * 4 + k[1]) * EX
                z_s[first : first + EX, :] = part[EX * ey : EX * (ey + 1)]
    for c in range(5):
        first, many = (16 * c, 16) if c < 4 else (64, 8)
        sums = [None] * CHUNKS
        for ey in range(EY):
            j, at = divmod(STRIDE * ey, 128)
            if c < 4:
                part = z_s[16 * (c * EY + ey) : 16 * (c * EY + ey + 1), :]
            else:
                part = top_s[pl.ds(EX * ey + EX - 1, 4, stride=each), :]
                part = jnp.concatenate([part, jnp.zeros((4, 128), jnp.float32)], axis=0)
            part = pltpu.roll(part, at, 1) if at else part
            pieces = [(j, part)]
            if at + SLOT > 128:
                pieces = [
                    (j, jnp.where(lane >= at, part, 0.0)),
                    (j + 1, jnp.where(lane < at, part, 0.0)),
                ]
            for k, piece in pieces:
                sums[k] = piece if sums[k] is None else sums[k] + piece
        for j in range(CHUNKS):
            grid_s[j, first : first + many, :] = sums[j]

    sides = (pl.ds(0, 4, stride=16), pl.ds(64, 4))
    lanes = lax.broadcasted_iota(jnp.int32, (SROW, 128), 1)
    far = CHUNKS - 1
    edge = grid_s[far]
    rims = (grid_s[0], pltpu.roll(edge, 128 - TAIL, 1))
    lane8 = lax.broadcasted_iota(jnp.int32, (8, 128), 1)
    for side in range(2):
        for j in range(CHUNKS):
            x_send[side, j] = grid_s[j, sides[side], :]
    for sy in range(2):
        rows = jnp.concatenate([x_send[0, far * sy], x_send[1, far * sy]], axis=0)
        shift, first = (TAIL, TAIL) if sy == 0 else (128 - TAIL, 0)
        got = pltpu.roll(rows, shift, 1)
        got = jnp.where((lane8 >= first) & (lane8 < first + NZ), got, 0.0)
        f_send[0, sy] = got[:4]
        f_send[1, sy] = got[4:]
        for sz in range(2):
            got = pltpu.roll(rows, (shift + (8 if sz == 0 else 128 - 8)) % 128, 1)
            got = jnp.where(lane8 == first + (NZ - 1) * (1 - sz), got, 0.0)
            c_send[0, sy, sz] = got[:4]
            c_send[1, sy, sz] = got[4:]
        packed = None
        for i in range(SROW // 8):
            got = jnp.where(lane8 < NZ, rims[sy][8 * i : 8 * i + 8], 0.0)
            got = pltpu.roll(got, PITCH * i, 1) if i else got
            packed = got if packed is None else packed + got
        p_send[sy] = packed
        place = lax.rem(lane8, PITCH)
        for sz in range(2):
            got = jnp.where(place == (NZ - 1) * sz, packed, 0.0)
            q_send[sy, sz] = pltpu.roll(got, 8 if sz == 0 else 128 - 8, 1)

    def route(way):
        sx, sy, sz = ((w + 1) // 2 for w in way)
        ox, oy, oz = 1 - sx, 1 - sy, 1 - sz
        dx, dy, dz = (w != 0 for w in way)
        if dx and dy and dz:
            return c_send.at[sx, sy, sz], c_recv.at[ox, oy, oz]
        if dx and dy:
            return f_send.at[sx, sy], f_recv.at[ox, oy]
        if dx and dz:
            return e_send.at[sx, sz], e_recv.at[ox, oz]
        if dy and dz:
            return q_send.at[sy, sz], q_recv.at[oy, oz]
        if dx:
            return x_send.at[sx], x_recv.at[ox]
        if dy:
            return p_send.at[sy], p_recv.at[oy]
        return m_send.at[sz], m_recv.at[oz]

    def copy(source, target, peer):
        return pltpu.make_async_remote_copy(
            src_ref=source,
            dst_ref=target,
            send_sem=send_sem.at[0],
            recv_sem=recv_sem.at[0],
            device_id=peer,
            device_id_type=MESH,
        )

    def await_all(settle):
        for (nx, ny, nz), here in classes():
            count = nx * CHUNKS + nx * ny + nx * nz + nx * ny * nz
            count += 2 * ny + 2 * ny * nz + nz * SROW // 4
            whole = tally.at[pl.ds(0, count)]

            @pl.when(here)
            def _():
                settle(copy(whole, whole, links[0][2]))

    peers = sum(there.astype(jnp.int32) for way, there, peer in links)
    pl.semaphore_wait(barrier, peers)
    farthest = sorted(range(len(WAYS)), key=lambda k: -sum(map(abs, WAYS[k])))

    def depart(chosen):
        for k in farthest:
            way, there, peer = links[k]
            if chosen(way):

                @pl.when(there)
                def _():
                    copy(*route(way), peer).start()

    flat = lambda way: way[1] == 0 and way[2] != 0
    depart(lambda way: not flat(way))
    for dz in range(2):
        face = None
        source = jnp.minimum(NZ * lanes + (NZ - 1) * dz, 128 * CHUNKS - 1)
        for j in range(CHUNKS):
            got = jnp.take_along_axis(
                grid_s[j], source & 127, axis=1, mode="promise_in_bounds"
            )
            face = got if face is None else jnp.where(source >= 128 * j, got, face)
        m_send[dz] = jnp.where(lanes < NY, face, 0.0)
        for side in range(2):
            e_send[side, dz] = m_send[dz, sides[side], :]
    depart(flat)
    vel_out[...] = v_s[...] + half * a_s[...]

    await_all(lambda copied: copied.wait_recv())

    for dz in range(2):
        for sx in range(2):
            m_recv[dz, sides[sx], :] += e_recv[sx, dz]
    full = [m_recv[dz] for dz in range(2)]
    strips = []
    for sy in range(2):
        sums = p_recv[sy] + q_recv[sy, 0] + q_recv[sy, 1]
        parts = []
        for i in range(SROW // 8):
            shift = (TAIL * sy - PITCH * i) % 128
            got = pltpu.roll(sums, shift, 1) if shift else sums
            parts.append(
                jnp.where((lane8 >= TAIL * sy) & (lane8 < TAIL * sy + NZ), got, 0.0)
            )
        strips.append(jnp.concatenate(parts, axis=0))
        for sx in range(2):
            x_recv[sx, far * sy] += f_recv[sx, sy] + (c_recv[sx, sy, 0] + c_recv[sx, sy, 1])
    for j in range(CHUNKS):
        node = lanes + 128 * j
        along = lax.div(node, NZ)
        depth = node - NZ * along
        sums = grid_s[j]
        for dz in range(2):
            got = jnp.take_along_axis(
                full[dz], jnp.minimum(along, 127), axis=1, mode="promise_in_bounds"
            )
            sums = sums + jnp.where((depth == (NZ - 1) * dz) & (along < NY), got, 0.0)
        if j == 0:
            sums = sums + strips[0]
        if j == far:
            sums = sums + strips[1]
        grid_s[j] = sums
        for sx in range(2):
            grid_s[j, sides[sx], :] += x_recv[sx, j]
        mass = grid_s[j, 48:64, :]
        for c in range(3):
            grid_s[j, 16 * c : 16 * c + 16, :] = grid_s[j, 16 * c : 16 * c + 16, :] / mass
        grid_s[j, 64:67, :] = grid_s[j, 64:67, :] / grid_s[j, 67:68, :]

    for x in range(NX):
        rows = pl.ds(4 * (x % 4) + x // 4, 3, stride=16) if x < NX - 1 else pl.ds(64, 3)
        for j in range(CHUNKS):
            width = min(128, PLANE - 128 * j)
            at = PLANE * x + 128 * j
            acc_out[:, at : at + width] = grid_s[j, rows, 0:width]
    await_all(lambda copied: copied.wait_send())


def finish(pos, vel, acc, pos_out, vel_out, acc_out, v_s, sem):
    def put(src, dst, k):
        copy = pltpu.make_async_copy(src, dst.at[:, 0], sem.at[k])
        copy.start()
        return copy

    copies = [put(pos, pos_out, 0), put(acc, acc_out, 1)]
    v_s[...] = vel[...] + (0.5 * time_step) * acc[...]
    copies.append(put(v_s, vel_out, 2))
    for cp in copies:
        cp.wait()


def body(displ, veloc, accel, node_index, inv_map, jac_weight, lame_first, shear_mod, density):
    nodes = displ.shape[4]
    elements = node_index.shape[4]
    deriv, back, spread = constants()
    deriv, back = halves(deriv), halves(back)
    fields = [x.reshape(3, 1, nodes) for x in (displ, veloc, accel)]
    elems = [
        x.reshape(125, 1, elements) for x in (jac_weight, lame_first, shear_mod, density)
    ]
    vmem = pl.BlockSpec(memory_space=pltpu.VMEM)
    hbm = pl.BlockSpec(memory_space=pltpu.HBM)
    f32 = jnp.float32
    out = jax.ShapeDtypeStruct((3, 1, nodes), f32)
    result = pl.pallas_call(
        kernel,
        out_shape=[pltpu.VMEM((3, nodes), f32)] * 3,
        in_specs=[hbm] * 12,
        out_specs=[vmem] * 3,
        scratch_shapes=[
            pltpu.VMEM(deriv.shape, jnp.bfloat16),
            pltpu.VMEM(back.shape, jnp.bfloat16),
            pltpu.VMEM(spread.shape, jnp.bfloat16),
            pltpu.VMEM((3, nodes), f32),
            pltpu.VMEM((3, nodes), f32),
            pltpu.VMEM((3, nodes), f32),
            pltpu.VMEM((1, elements), jnp.int32),
            pltpu.VMEM((13, 128, elements), f32),
            pltpu.VMEM((256, 128), jnp.bfloat16),
            pltpu.VMEM((13, 128, 128), f32),
            pltpu.VMEM((15 * EX * EY, 128), f32),
            pltpu.VMEM((16 * EX * EY, 128), f32),
            pltpu.VMEM((4 * EX * EY, 128), f32),
            pltpu.VMEM((5 * SLOT, 384), f32),
            pltpu.VMEM((384, 384), f32),
            pltpu.VMEM((128, 128), f32),
            pltpu.VMEM((CHUNKS, SROW, 128), f32),
            pltpu.VMEM((2, SROW, 128), f32),
            pltpu.VMEM((2, 8, 128), f32),
            pltpu.VMEM((2, CHUNKS, 4, 128), f32),
            pltpu.VMEM((2, 2, 4, 128), f32),
            pltpu.VMEM((2, 2, 8, 128), f32),
            pltpu.VMEM((2, 2, 4, 128), f32),
            pltpu.VMEM((2, 2, 2, 4, 128), f32),
            pltpu.VMEM((2, SROW, 128), f32),
            pltpu.VMEM((2, 8, 128), f32),
            pltpu.VMEM((2, 2, 8, 128), f32),
            pltpu.VMEM((2, CHUNKS, 4, 128), f32),
            pltpu.VMEM((2, 2, 4, 128), f32),
            pltpu.VMEM((2, 2, 4, 128), f32),
            pltpu.VMEM((2, 2, 2, 4, 128), f32),
            pltpu.VMEM((2 * SROW // 4 + 2 * CHUNKS + 28, 4, 128), f32),
            pltpu.SemaphoreType.DMA((9,)),
            pltpu.SemaphoreType.DMA((1,)),
            pltpu.SemaphoreType.DMA((1,)),
        ],
        compiler_params=pltpu.CompilerParams(
            collective_id=0, has_side_effects=True, vmem_limit_bytes=LIMIT
        ),
    )(
        *fields,
        node_index.reshape(125, 1, elements),
        inv_map.reshape(9, 125, 1, elements),
        *elems,
        jnp.asarray(deriv),
        jnp.asarray(back),
        jnp.asarray(spread, jnp.bfloat16),
    )
    final = pl.pallas_call(
        finish,
        out_shape=[out] * 3,
        in_specs=[vmem] * 3,
        out_specs=[hbm] * 3,
        scratch_shapes=[pltpu.VMEM((3, nodes), f32), pltpu.SemaphoreType.DMA((3,))],
        compiler_params=pltpu.CompilerParams(vmem_limit_bytes=LIMIT),
    )(*[pltpu.with_memory_space_constraint(x, pltpu.VMEM) for x in result])
    return tuple(x.reshape(displ.shape) for x in final)


def solution(mesh):
    field = P(None, "gx", "gy", "gz", None)
    elem = P("gx", "gy", "gz", None, None)
    placed = (field,) * 3 + (elem, P("gx", "gy", "gz", None, None, None)) + (elem,) * 4
    return jax.shard_map(
        body, mesh=mesh, in_specs=placed, out_specs=(field,) * 3, check_vma=False
    )
```

```python
import jax
import jax.numpy as jnp
import numpy as np
from jax import lax
from jax.experimental import pallas as pl
from jax.experimental.pallas import tpu as pltpu
from jax.sharding import PartitionSpec as P

EX = 4
EY = 16
EZ = 2
NX = 4 * EX + 1
NY = 4 * EY + 1
NZ = 4 * EZ + 1
PLANE = NY * NZ
CHUNKS = -(-PLANE // 128)
STRIDE = 4 * NZ
SPAN = 5 * NZ
SLOT = 48
SROW = 72
TAIL = PLANE - NZ - 128 * (CHUNKS - 1)
PITCH = 14
SPLITS = ((0, 7), (7, 6))
PAIRS = tuple(((c, a), (c, a + 1)) for c in range(4) for a in (0, 2))

LIMIT = 65 * 1000 * 1000

time_step = 0.1
MESH = pl.DeviceIdType.MESH


def derivative_table():
    points = np.array([-1.0, -np.sqrt(3.0 / 7.0), 0.0, np.sqrt(3.0 / 7.0), 1.0])
    count = points.shape[0]
    weights = np.array(
        [
            1.0 / np.prod([points[s] - points[o] for o in range(count) if o != s])
            for s in range(count)
        ]
    )
    table = np.zeros((count, count))
    for t in range(count):
        for s in range(count):
            if t != s:
                table[t, s] = weights[s] / weights[t] / (points[t] - points[s])
        table[t, t] = -np.sum(table[t])
    return table


def constants():
    table = derivative_table()
    eye = np.eye(5)
    parts = [
        np.kron(table, np.kron(eye, eye)),
        np.kron(eye, np.kron(table, eye)),
        np.kron(eye, np.kron(eye, table)),
    ]
    pad = np.zeros((125, 5 * SLOT))
    for a in range(5):
        for b in range(5):
            for c in range(5):
                pad[a * 25 + 5 * b + c, a * SLOT + NZ * b + c] = 1.0
    deriv = np.zeros((384, 5 * SLOT), np.float32)
    for l in range(3):
        deriv[l * 128 : l * 128 + 125] = parts[l] @ pad
    spread = np.zeros((5 * SLOT, 128), np.float32)
    spread[:, :125] = pad.T
    return deriv, -deriv.T.copy(), spread


def split2(x):
    hi = x.astype(jnp.bfloat16)
    low = (x - hi.astype(jnp.float32)).astype(jnp.bfloat16)
    return (hi, low)


def halves(x):
    hi = np.asarray(x, jnp.bfloat16)
    low = np.asarray(x - hi.astype(np.float32), jnp.bfloat16)
    return np.stack([hi, low])


def product(hi, low, y):
    top, rest = split2(y)
    dot = lambda a, b: jnp.dot(a, b, preferred_element_type=jnp.float32)
    wide = lambda *parts: jnp.concatenate(parts, axis=1)
    if y.shape[0] > 256:
        first = dot(
            wide(hi, hi, low),
            jnp.concatenate([top[:, :256], rest[:, :256], top[:, :256]], axis=0),
        )
    else:
        first = dot(hi, top[:, :256]) + dot(hi, rest[:, :256]) + dot(low, top[:, :256])
    both = dot(hi, wide(top[:, 256:], rest[:, 256:]))
    last = both[:, :128] + both[:, 128:] + dot(low, top[:, 256:])
    return first[:, :128], first[:, 128:], last


def ways():
    steps = (0, -1, 1)
    found = [(x, y, z) for z in steps for y in steps for x in steps][1:]
    half = [w for w in found if w > (0, 0, 0)]
    half.sort(key=lambda w: (sum(map(abs, w)), -abs(w[2])))
    other = [tuple(-v for v in w) for w in half]
    return half + other[::-1]


WAYS = ways()


def neighbours():
    names = ("gx", "gy", "gz")
    spots = [lax.axis_index(n) for n in names]
    sizes = [lax.axis_size(n) for n in names]
    links = []
    for way in WAYS:
        there = None
        peer = {}
        for n, s, z, w in zip(names, spots, sizes, way):
            if w:
                ok = s > 0 if w < 0 else s < z - 1
                there = ok if there is None else there & ok
                peer[n] = s + w
        links.append((way, there, peer))
    return links


def classes():
    found = [((), None)]
    for name in ("gx", "gy", "gz"):
        size, spot = lax.axis_size(name), lax.axis_index(name)
        inner = (spot > 0) & (spot < size - 1)
        choices = [(min(size - 1, 1), None)]
        if size > 2:
            choices = [(1, jnp.logical_not(inner)), (2, inner)]
        grown = []
        for counts, here in found:
            for count, ok in choices:
                both = here if ok is None else ok if here is None else here & ok
                grown.append((counts + (count,), both))
        found = grown
    return [(counts, True if here is None else here) for counts, here in found]


def squeezed(ref):
    return ref.at[:, 0] if len(ref.shape) == 3 else ref.at[:, :, 0]


def kernel(
    displ, veloc, accel, node, inv, jac, lame, shear, dens,
    deriv_ref, back_ref, spread_ref,
    pos_out, vel_out, acc_out,
    deriv_s, back_s, spread_s,
    d_s, v_s, a_s, node_s, raw_s,
    order_s, sorted_s, w_s, z_s, top_s, u_s, fl_s, md_s, grid_s,
    m_send, p_send, x_send, e_send, q_send, f_send, c_send,
    m_recv, p_recv, q_recv, x_recv, e_recv, f_recv, c_recv,
    tally, in_sem, send_sem, recv_sem,
):
    links = neighbours()
    head = node.at[pl.ds(0, 1), 0]
    copies = [pltpu.make_async_copy(head, node_s, in_sem.at[0])]
    for k, (src, dst) in enumerate(((displ, d_s), (veloc, v_s), (accel, a_s))):
        copies.append(pltpu.make_async_copy(src.at[:, 0], dst, in_sem.at[1 + k]))
    whole = squeezed(inv)
    point = pl.ds(0, 125)
    copies.append(pltpu.make_async_copy(whole, raw_s.at[pl.ds(0, 9), point], in_sem.at[4]))
    for k, src in enumerate((jac, lame, shear, dens)):
        copies.append(pltpu.make_async_copy(squeezed(src), raw_s.at[9 + k, point], in_sem.at[5]))
    consts = ((deriv_ref, deriv_s), (back_ref, back_s), (spread_ref, spread_s))
    for k, (src, dst) in enumerate(consts):
        copies.append(pltpu.make_async_copy(src, dst, in_sem.at[6 + k]))
    for cp in copies:
        cp.start()
    raw_s[:, 125:128, :] = jnp.zeros((13, 3, 128), jnp.float32)
    for ref in (m_recv, p_recv, q_recv, x_recv, e_recv, f_recv, c_recv):
        ref[...] = jnp.zeros_like(ref)
    copies[0].wait()
    corner = node_s[0:1, :].astype(jnp.float32)
    x0 = jnp.floor((corner + 0.5) * (1.0 / PLANE))
    rem = corner - PLANE * x0
    y0 = jnp.floor((rem + 0.5) * (1.0 / NZ))
    z0 = rem - NZ * y0
    goal = EY * EX * 0.25 * z0 + EX * 0.25 * y0 + 0.25 * x0
    goal = jnp.transpose(jnp.broadcast_to(goal, (128, 128)))
    slots = lax.broadcasted_iota(jnp.int32, (128, 128), 1).astype(jnp.float32)
    order = jnp.where(slots == goal, 1.0, 0.0).astype(jnp.bfloat16)
    order_s[0:128, :] = order
    order_s[128:256, :] = order
    barrier = pltpu.get_barrier_semaphore()
    for way, there, peer in links:

        @pl.when(there)
        def _():
            pl.semaphore_signal(barrier, inc=1, device_id=peer, device_id_type=MESH)

    for cp in copies[1:4]:
        cp.wait()

    half = 0.5 * time_step
    pos = d_s[...] + time_step * v_s[...] + (half * time_step) * a_s[...]
    pos_out[...] = pos

    lane = lax.broadcasted_iota(jnp.int32, (1, 128), 1)

    def chunk(q):
        width = min(128, PLANE * NX - 128 * q)
        part = pos_out[:, 128 * q : 128 * q + width]
        if width < 128:
            part = jnp.concatenate([part, jnp.zeros((3, 128 - width), jnp.float32)], axis=1)
        return part

    ahead = (4 * PLANE - STRIDE) // 128
    blank = jnp.zeros((3, 128), jnp.float32)
    single = [chunk(q) for q in range(-(-PLANE * NX // 128))]
    double = [
        jnp.concatenate([v, single[q + ahead] if q + ahead < len(single) else blank], axis=0)
        for q, v in enumerate(single)
    ]

    def window(source, x, ey):
        q, at = divmod(PLANE * x + STRIDE * ey, 128)
        part = source[q]
        if at + SPAN > 128:
            part = jnp.where(lane >= at, part, source[q + 1])
        return pltpu.roll(part, 128 - at, 1) if at else part

    def keep(x, ey, part):
        ex, a = divmod(x, 4)
        spots = [(a, ex)] if x < NX - 1 else []
        if x and a == 0:
            spots.append((4, ex - 1))
        for a, ex in spots:
            first = 3 * ((a * EY + ey) * EX + ex)
            w_s[first : first + 3, :] = part

    for x in range(NX):
        paired = x < NX - 1 and x % 8 < 4
        for ey in range(EY):
            if paired:
                part = window(double, x, ey)
                keep(x, ey, part[:3])
                if ey:
                    keep(x + 4, ey - 1, part[3:])
            elif x == NX - 1 or ey == EY - 1:
                keep(x, ey, window(single, x, ey))

    copies[4].wait()
    pltpu.make_async_copy(
        whole.at[pl.ds(0, 4)], raw_s.at[pl.ds(9, 4), point], in_sem.at[5]
    ).wait()
    copies[9].wait()
    for first, many in SPLITS:
        raw = raw_s[first : first + many].reshape(many * 128, 128)
        sorted_s[first : first + many] = jnp.dot(
            jnp.concatenate(split2(raw), axis=1),
            order_s[...],
            preferred_element_type=jnp.float32,
        ).reshape(many, 128, 128)

    left = lax.broadcasted_iota(jnp.int32, (SLOT, 128), 1) < 64
    each = EX * EY

    def block(c, a):
        return w_s[pl.ds(3 * each * a + c, each, stride=3), :]

    for (c, a), (d, b) in PAIRS[:6] + (((0, 4), (1, 4)), ((2, 4), (2, 4))):
        turned = jnp.transpose(jnp.concatenate([block(c, a), block(d, b)], axis=0))[:SLOT]
        other = pltpu.roll(turned, 64, 1)
        rise = lambda v: pltpu.roll(v, SLOT - 4, 0)
        u_s[SLOT * a : SLOT * (a + 1), 128 * c : 128 * (c + 1)] = jnp.where(
            left, turned, rise(other)
        )
        if (c, a) != (d, b):
            u_s[SLOT * b : SLOT * (b + 1), 128 * d : 128 * (d + 1)] = jnp.where(
                left, other, rise(turned)
            )

    local = product(deriv_s[0], deriv_s[1], u_s[...])
    for i in range(16):
        at = slice(8 * i, 8 * i + 8)
        maps = [[sorted_s[3 * l + j, at] for j in range(3)] for l in range(3)]
        weight, lam, mu, dens_e = (sorted_s[9 + k, at] for k in range(4))
        grads = [[local[c][128 * l + 8 * i : 128 * l + 8 * i + 8] for c in range(3)] for l in range(3)]
        h = [
            [sum(grads[l][c] * maps[l][j] for l in range(3)) for j in range(3)]
            for c in range(3)
        ]
        mu = mu * weight
        div = lam * weight * (h[0][0] + h[1][1] + h[2][2])
        stress = [[None] * 3 for _ in range(3)]
        for c in range(3):
            for j in range(c, 3):
                s = mu * (h[c][j] + h[j][c])
                stress[c][j] = stress[j][c] = s + div if c == j else s
        for l in range(3):
            for c in range(3):
                fl_s[128 * l + 8 * i : 128 * l + 8 * i + 8, 128 * c : 128 * (c + 1)] = sum(
                    stress[c][j] * maps[l][j] for j in range(3)
                )
        md_s[at, :] = dens_e * weight
    for cp in copies[10:]:
        cp.wait()
    terms = product(back_s[0], back_s[1], fl_s[...])
    heavy = sum(
        jnp.dot(spread_s[...], part, preferred_element_type=jnp.float32)
        for part in split2(md_s[...])
    )

    def term(c, a):
        at = slice(SLOT * a, SLOT * (a + 1))
        return terms[c][at] if c < 3 else heavy[at]

    sink = lambda v: pltpu.roll(v, 4, 0)
    tail = jnp.zeros((128, 128 - SLOT), jnp.float32)
    crest = {}
    rows = lax.broadcasted_iota(jnp.int32, (each, 128), 0)
    for (c, a), (d, b) in (((0, 4), (1, 4)), ((2, 4), (3, 4))) + PAIRS:
        one, two = term(c, a), term(d, b)
        both = jnp.where(left, one, sink(two)) + pltpu.roll(jnp.where(left, two, sink(one)), 64, 1)
        turned = jnp.concatenate([jnp.transpose(both), tail], axis=1)
        for k, part in (((c, a), turned[:each]), ((d, b), turned[each:])):
            if k[1] == 4:
                top_s[each * k[0] : each * (k[0] + 1), :] = part
                crest[k[0]] = jnp.where(rows % EX == 0, 0.0, pltpu.roll(part, 1, 0))
                continue
            if k[1] == 0:
                part = part + crest[k[0]]
            for ey in range(EY):
                first = ((k[0] * EY + ey) * 4 + k[1]) * EX
                z_s[first : first + EX, :] = part[EX * ey : EX * (ey + 1)]
    sides = (pl.ds(0, 4, stride=16), pl.ds(64, 4))
    lanes = lax.broadcasted_iota(jnp.int32, (SROW, 128), 1)
    lane8 = lax.broadcasted_iota(jnp.int32, (8, 128), 1)
    far = CHUNKS - 1
    for sy in range(2):
        ey = (EY - 1) * sy
        base = STRIDE * sy
        crown = top_s[pl.ds(EX * ey + EX - 1, 4, stride=each), :]
        rows = jnp.concatenate([z_s[pl.ds(16 * ey, 4, stride=16 * EY), :], crown], axis=0)
        first = TAIL * (1 - sy)
        got = pltpu.roll(rows, (first - base) % 128, 1)
        got = jnp.where((lane8 >= first) & (lane8 < first + NZ), got, 0.0)
        f_send[0, sy] = got[:4]
        f_send[1, sy] = got[4:]
        for sz in range(2):
            got = pltpu.roll(rows, (first - base + (8 if sz == 0 else -8)) % 128, 1)
            got = jnp.where(lane8 == first + (NZ - 1) * (1 - sz), got, 0.0)
            c_send[0, sy, sz] = got[:4]
            c_send[1, sy, sz] = got[4:]
        parts = [z_s[pl.ds(16 * (c * EY + ey) + 8 * h, 8), :] for c in range(4) for h in range(2)]
        parts.append(jnp.concatenate([crown, jnp.zeros((4, 128), jnp.float32)], axis=0))
        packed = None
        for i, part in enumerate(parts):
            got = jnp.where((lane8 >= base) & (lane8 < base + NZ), part, 0.0)
            shift = (PITCH * i - base) % 128
            got = pltpu.roll(got, shift, 1) if shift else got
            packed = got if packed is None else packed + got
        p_send[sy] = packed
        place = lax.rem(lane8, PITCH)
        for sz in range(2):
            got = jnp.where(place == (NZ - 1) * sz, packed, 0.0)
            q_send[sy, sz] = pltpu.roll(got, 8 if sz == 0 else 128 - 8, 1)

    def route(way):
        sx, sy, sz = ((w + 1) // 2 for w in way)
        ox, oy, oz = 1 - sx, 1 - sy, 1 - sz
        dx, dy, dz = (w != 0 for w in way)
        if dx and dy and dz:
            return c_send.at[sx, sy, sz], c_recv.at[ox, oy, oz]
        if dx and dy:
            return f_send.at[sx, sy], f_recv.at[ox, oy]
        if dx and dz:
            return e_send.at[sx, sz], e_recv.at[ox, oz]
        if dy and dz:
            return q_send.at[sy, sz], q_recv.at[oy, oz]
        if dx:
            return x_send.at[sx], x_recv.at[ox]
        if dy:
            return p_send.at[sy], p_recv.at[oy]
        return m_send.at[sz], m_recv.at[oz]

    def copy(source, target, peer):
        return pltpu.make_async_remote_copy(
            src_ref=source,
            dst_ref=target,
            send_sem=send_sem.at[0],
            recv_sem=recv_sem.at[0],
            device_id=peer,
            device_id_type=MESH,
        )

    def await_all(settle):
        for (nx, ny, nz), here in classes():
            count = nx * CHUNKS + nx * ny + nx * nz + nx * ny * nz
            count += 2 * ny + 2 * ny * nz + nz * SROW // 4
            whole = tally.at[pl.ds(0, count)]

            @pl.when(here)
            def _():
                settle(copy(whole, whole, links[0][2]))

    peers = sum(there.astype(jnp.int32) for way, there, peer in links)
    pl.semaphore_wait(barrier, peers)
    farthest = sorted(range(len(WAYS)), key=lambda k: -sum(map(abs, WAYS[k])))

    def depart(chosen):
        for k in farthest:
            way, there, peer = links[k]
            if chosen(way):

                @pl.when(there)
                def _():
                    copy(*route(way), peer).start()

    depart(lambda way: way[1] != 0)

    for c in range(5):
        first, many = (16 * c, 16) if c < 4 else (64, 8)
        sums = [None] * CHUNKS
        for ey in range(EY):
            j, at = divmod(STRIDE * ey, 128)
            if c < 4:
                part = z_s[16 * (c * EY + ey) : 16 * (c * EY + ey + 1), :]
            else:
                part = top_s[pl.ds(EX * ey + EX - 1, 4, stride=each), :]
                part = jnp.concatenate([part, jnp.zeros((4, 128), jnp.float32)], axis=0)
            part = pltpu.roll(part, at, 1) if at else part
            pieces = [(j, part)]
            if at + SLOT > 128:
                pieces = [
                    (j, jnp.where(lane >= at, part, 0.0)),
                    (j + 1, jnp.where(lane < at, part, 0.0)),
                ]
            for k, piece in pieces:
                sums[k] = piece if sums[k] is None else sums[k] + piece
        for j in range(CHUNKS):
            grid_s[j, first : first + many, :] = sums[j]

    for side in range(2):
        for j in range(CHUNKS):
            x_send[side, j] = grid_s[j, sides[side], :]
    sources = [
        jnp.minimum(NZ * lanes + (NZ - 1) * dz, 128 * CHUNKS - 1) for dz in range(2)
    ]

    def face(parts, dz):
        many = parts[0].shape[0]
        source = sources[dz][:many]
        found = None
        for j in range(CHUNKS):
            got = jnp.take_along_axis(
                parts[j], source & 127, axis=1, mode="promise_in_bounds"
            )
            found = got if found is None else jnp.where(source >= 128 * j, got, found)
        return jnp.where(lanes[:many] < NY, found, 0.0)

    rims = [
        jnp.concatenate([x_send[0, j], x_send[1, j]], axis=0) for j in range(CHUNKS)
    ]
    for dz in range(2):
        got = face(rims, dz)
        e_send[0, dz] = got[:4]
        e_send[1, dz] = got[4:]
    depart(lambda way: way[1] == 0 and way[0] != 0)
    for dz in range(2):
        m_send[dz] = face([grid_s[j] for j in range(CHUNKS)], dz)
    depart(lambda way: way[1] == 0 and way[0] == 0)
    vel_out[...] = v_s[...] + half * a_s[...]

    await_all(lambda copied: copied.wait_recv())

    for dz in range(2):
        for sx in range(2):
            m_recv[dz, sides[sx], :] += e_recv[sx, dz]
    full = [m_recv[dz] for dz in range(2)]
    strips = []
    for sy in range(2):
        sums = p_recv[sy] + q_recv[sy, 0] + q_recv[sy, 1]
        parts = []
        for i in range(SROW // 8):
            shift = (TAIL * sy - PITCH * i) % 128
            got = pltpu.roll(sums, shift, 1) if shift else sums
            parts.append(
                jnp.where((lane8 >= TAIL * sy) & (lane8 < TAIL * sy + NZ), got, 0.0)
            )
        strips.append(jnp.concatenate(parts, axis=0))
        for sx in range(2):
            x_recv[sx, far * sy] += f_recv[sx, sy] + (c_recv[sx, sy, 0] + c_recv[sx, sy, 1])
    for j in range(CHUNKS):
        node = lanes + 128 * j
        along = lax.div(node, NZ)
        depth = node - NZ * along
        sums = grid_s[j]
        for dz in range(2):
            got = jnp.take_along_axis(
                full[dz], jnp.minimum(along, 127), axis=1, mode="promise_in_bounds"
            )
            sums = sums + jnp.where((depth == (NZ - 1) * dz) & (along < NY), got, 0.0)
        if j == 0:
            sums = sums + strips[0]
        if j == far:
            sums = sums + strips[1]
        grid_s[j] = sums
        for sx in range(2):
            grid_s[j, sides[sx], :] += x_recv[sx, j]
        mass = grid_s[j, 48:64, :]
        for c in range(3):
            grid_s[j, 16 * c : 16 * c + 16, :] = grid_s[j, 16 * c : 16 * c + 16, :] / mass
        grid_s[j, 64:67, :] = grid_s[j, 64:67, :] / grid_s[j, 67:68, :]

    for x in range(NX):
        rows = pl.ds(4 * (x % 4) + x // 4, 3, stride=16) if x < NX - 1 else pl.ds(64, 3)
        for j in range(CHUNKS):
            width = min(128, PLANE - 128 * j)
            at = PLANE * x + 128 * j
            acc_out[:, at : at + width] = grid_s[j, rows, 0:width]
    await_all(lambda copied: copied.wait_send())


def finish(pos, vel, acc, pos_out, vel_out, acc_out, v_s, sem):
    def put(src, dst, k):
        copy = pltpu.make_async_copy(src, dst.at[:, 0], sem.at[k])
        copy.start()
        return copy

    copies = [put(pos, pos_out, 0), put(acc, acc_out, 1)]
    v_s[...] = vel[...] + (0.5 * time_step) * acc[...]
    copies.append(put(v_s, vel_out, 2))
    for cp in copies:
        cp.wait()


def body(displ, veloc, accel, node_index, inv_map, jac_weight, lame_first, shear_mod, density):
    nodes = displ.shape[4]
    elements = node_index.shape[4]
    deriv, back, spread = constants()
    deriv, back = halves(deriv), halves(back)
    fields = [x.reshape(3, 1, nodes) for x in (displ, veloc, accel)]
    elems = [
        x.reshape(125, 1, elements) for x in (jac_weight, lame_first, shear_mod, density)
    ]
    vmem = pl.BlockSpec(memory_space=pltpu.VMEM)
    hbm = pl.BlockSpec(memory_space=pltpu.HBM)
    f32 = jnp.float32
    out = jax.ShapeDtypeStruct((3, 1, nodes), f32)
    result = pl.pallas_call(
        kernel,
        out_shape=[pltpu.VMEM((3, nodes), f32)] * 3,
        in_specs=[hbm] * 12,
        out_specs=[vmem] * 3,
        scratch_shapes=[
            pltpu.VMEM(deriv.shape, jnp.bfloat16),
            pltpu.VMEM(back.shape, jnp.bfloat16),
            pltpu.VMEM(spread.shape, jnp.bfloat16),
            pltpu.VMEM((3, nodes), f32),
            pltpu.VMEM((3, nodes), f32),
            pltpu.VMEM((3, nodes), f32),
            pltpu.VMEM((1, elements), jnp.int32),
            pltpu.VMEM((13, 128, elements), f32),
            pltpu.VMEM((256, 128), jnp.bfloat16),
            pltpu.VMEM((13, 128, 128), f32),
            pltpu.VMEM((15 * EX * EY, 128), f32),
            pltpu.VMEM((16 * EX * EY, 128), f32),
            pltpu.VMEM((4 * EX * EY, 128), f32),
            pltpu.VMEM((5 * SLOT, 384), f32),
            pltpu.VMEM((384, 384), f32),
            pltpu.VMEM((128, 128), f32),
            pltpu.VMEM((CHUNKS, SROW, 128), f32),
            pltpu.VMEM((2, SROW, 128), f32),
            pltpu.VMEM((2, 8, 128), f32),
            pltpu.VMEM((2, CHUNKS, 4, 128), f32),
            pltpu.VMEM((2, 2, 4, 128), f32),
            pltpu.VMEM((2, 2, 8, 128), f32),
            pltpu.VMEM((2, 2, 4, 128), f32),
            pltpu.VMEM((2, 2, 2, 4, 128), f32),
            pltpu.VMEM((2, SROW, 128), f32),
            pltpu.VMEM((2, 8, 128), f32),
            pltpu.VMEM((2, 2, 8, 128), f32),
            pltpu.VMEM((2, CHUNKS, 4, 128), f32),
            pltpu.VMEM((2, 2, 4, 128), f32),
            pltpu.VMEM((2, 2, 4, 128), f32),
            pltpu.VMEM((2, 2, 2, 4, 128), f32),
            pltpu.VMEM((2 * SROW // 4 + 2 * CHUNKS + 28, 4, 128), f32),
            pltpu.SemaphoreType.DMA((9,)),
            pltpu.SemaphoreType.DMA((1,)),
            pltpu.SemaphoreType.DMA((1,)),
        ],
        compiler_params=pltpu.CompilerParams(
            collective_id=0, has_side_effects=True, vmem_limit_bytes=LIMIT
        ),
    )(
        *fields,
        node_index.reshape(125, 1, elements),
        inv_map.reshape(9, 125, 1, elements),
        *elems,
        jnp.asarray(deriv),
        jnp.asarray(back),
        jnp.asarray(spread, jnp.bfloat16),
    )
    final = pl.pallas_call(
        finish,
        out_shape=[out] * 3,
        in_specs=[vmem] * 3,
        out_specs=[hbm] * 3,
        scratch_shapes=[pltpu.VMEM((3, nodes), f32), pltpu.SemaphoreType.DMA((3,))],
        compiler_params=pltpu.CompilerParams(vmem_limit_bytes=LIMIT),
    )(*[pltpu.with_memory_space_constraint(x, pltpu.VMEM) for x in result])
    return tuple(x.reshape(displ.shape) for x in final)


def solution(mesh):
    field = P(None, "gx", "gy", "gz", None)
    elem = P("gx", "gy", "gz", None, None)
    placed = (field,) * 3 + (elem, P("gx", "gy", "gz", None, None, None)) + (elem,) * 4
    return jax.shard_map(
        body, mesh=mesh, in_specs=placed, out_specs=(field,) * 3, check_vma=False
    )
```

```python
import jax
import jax.numpy as jnp
import numpy as np
from jax import lax
from jax.experimental import pallas as pl
from jax.experimental.pallas import tpu as pltpu
from jax.sharding import PartitionSpec as P

EX = 4
EY = 16
EZ = 2
NX = 4 * EX + 1
NY = 4 * EY + 1
NZ = 4 * EZ + 1
PLANE = NY * NZ
CHUNKS = -(-PLANE // 128)
STRIDE = 4 * NZ
SPAN = 5 * NZ
SLOT = 48
SROW = 72
TAIL = PLANE - NZ - 128 * (CHUNKS - 1)
PITCH = 14
SPLITS = ((0, 7), (7, 6))
PAIRS = tuple(((c, a), (c, a + 1)) for c in range(4) for a in (0, 2))

LIMIT = 65 * 1000 * 1000

time_step = 0.1
MESH = pl.DeviceIdType.MESH


def derivative_table():
    points = np.array([-1.0, -np.sqrt(3.0 / 7.0), 0.0, np.sqrt(3.0 / 7.0), 1.0])
    count = points.shape[0]
    weights = np.array(
        [
            1.0 / np.prod([points[s] - points[o] for o in range(count) if o != s])
            for s in range(count)
        ]
    )
    table = np.zeros((count, count))
    for t in range(count):
        for s in range(count):
            if t != s:
                table[t, s] = weights[s] / weights[t] / (points[t] - points[s])
        table[t, t] = -np.sum(table[t])
    return table


def constants():
    table = derivative_table()
    eye = np.eye(5)
    parts = [
        np.kron(table, np.kron(eye, eye)),
        np.kron(eye, np.kron(table, eye)),
        np.kron(eye, np.kron(eye, table)),
    ]
    pad = np.zeros((125, 5 * SLOT))
    for a in range(5):
        for b in range(5):
            for c in range(5):
                pad[a * 25 + 5 * b + c, a * SLOT + NZ * b + c] = 1.0
    deriv = np.zeros((384, 5 * SLOT), np.float32)
    for l in range(3):
        deriv[l * 128 : l * 128 + 125] = parts[l] @ pad
    spread = np.zeros((5 * SLOT, 128), np.float32)
    spread[:, :125] = pad.T
    return deriv, -deriv.T.copy(), spread


def split2(x):
    hi = x.astype(jnp.bfloat16)
    low = (x - hi.astype(jnp.float32)).astype(jnp.bfloat16)
    return (hi, low)


def halves(x):
    hi = np.asarray(x, jnp.bfloat16)
    low = np.asarray(x - hi.astype(np.float32), jnp.bfloat16)
    return np.stack([hi, low])


def product(hi, low, y):
    top, rest = split2(y)
    dot = lambda a, b: jnp.dot(a, b, preferred_element_type=jnp.float32)
    wide = lambda *parts: jnp.concatenate(parts, axis=1)
    if y.shape[0] > 256:
        first = dot(
            wide(hi, hi, low),
            jnp.concatenate([top[:, :256], rest[:, :256], top[:, :256]], axis=0),
        )
    else:
        first = dot(hi, top[:, :256]) + dot(hi, rest[:, :256]) + dot(low, top[:, :256])
    both = dot(hi, wide(top[:, 256:], rest[:, 256:]))
    last = both[:, :128] + both[:, 128:] + dot(low, top[:, 256:])
    return first[:, :128], first[:, 128:], last


def ways():
    steps = (0, -1, 1)
    found = [(x, y, z) for z in steps for y in steps for x in steps][1:]
    half = [w for w in found if w > (0, 0, 0)]
    half.sort(key=lambda w: (sum(map(abs, w)), -abs(w[2])))
    other = [tuple(-v for v in w) for w in half]
    return half + other[::-1]


WAYS = ways()


def neighbours():
    names = ("gx", "gy", "gz")
    spots = [lax.axis_index(n) for n in names]
    sizes = [lax.axis_size(n) for n in names]
    links = []
    for way in WAYS:
        there = None
        peer = {}
        for n, s, z, w in zip(names, spots, sizes, way):
            if w:
                ok = s > 0 if w < 0 else s < z - 1
                there = ok if there is None else there & ok
                peer[n] = s + w
        links.append((way, there, peer))
    return links


def classes():
    found = [((), None)]
    for name in ("gx", "gy", "gz"):
        size, spot = lax.axis_size(name), lax.axis_index(name)
        inner = (spot > 0) & (spot < size - 1)
        choices = [(min(size - 1, 1), None)]
        if size > 2:
            choices = [(1, jnp.logical_not(inner)), (2, inner)]
        grown = []
        for counts, here in found:
            for count, ok in choices:
                both = here if ok is None else ok if here is None else here & ok
                grown.append((counts + (count,), both))
        found = grown
    return [(counts, True if here is None else here) for counts, here in found]


def squeezed(ref):
    return ref.at[:, 0] if len(ref.shape) == 3 else ref.at[:, :, 0]


def kernel(
    displ, veloc, accel, node, inv, jac, lame, shear, dens,
    deriv_ref, back_ref, spread_ref,
    pos_out, vel_out, acc_out,
    deriv_s, back_s, spread_s,
    d_s, v_s, a_s, node_s, raw_s,
    order_s, sorted_s, w_s, z_s, top_s, u_s, fl_s, md_s, grid_s,
    m_send, p_send, x_send, e_send, q_send, f_send, c_send,
    m_recv, p_recv, q_recv, x_recv, e_recv, f_recv, c_recv,
    tally, in_sem, send_sem, recv_sem,
):
    links = neighbours()
    head = node.at[pl.ds(0, 1), 0]
    copies = [pltpu.make_async_copy(head, node_s, in_sem.at[0])]
    for k, (src, dst) in enumerate(((displ, d_s), (veloc, v_s), (accel, a_s))):
        copies.append(pltpu.make_async_copy(src.at[:, 0], dst, in_sem.at[1 + k]))
    whole = squeezed(inv)
    point = pl.ds(0, 125)
    copies.append(pltpu.make_async_copy(whole, raw_s.at[pl.ds(0, 9), point], in_sem.at[4]))
    for k, src in enumerate((jac, lame, shear, dens)):
        copies.append(pltpu.make_async_copy(squeezed(src), raw_s.at[9 + k, point], in_sem.at[5]))
    consts = ((deriv_ref, deriv_s), (back_ref, back_s), (spread_ref, spread_s))
    for k, (src, dst) in enumerate(consts):
        copies.append(pltpu.make_async_copy(src, dst, in_sem.at[6 + k]))
    for cp in copies:
        cp.start()
    raw_s[:, 125:128, :] = jnp.zeros((13, 3, 128), jnp.float32)
    for ref in (m_recv, p_recv, q_recv, x_recv, e_recv, f_recv, c_recv):
        ref[...] = jnp.zeros_like(ref)
    copies[0].wait()
    corner = node_s[0:1, :].astype(jnp.float32)
    x0 = jnp.floor((corner + 0.5) * (1.0 / PLANE))
    rem = corner - PLANE * x0
    y0 = jnp.floor((rem + 0.5) * (1.0 / NZ))
    z0 = rem - NZ * y0
    goal = EY * EX * 0.25 * z0 + EX * 0.25 * y0 + 0.25 * x0
    goal = jnp.transpose(jnp.broadcast_to(goal, (128, 128)))
    slots = lax.broadcasted_iota(jnp.int32, (128, 128), 1).astype(jnp.float32)
    order = jnp.where(slots == goal, 1.0, 0.0).astype(jnp.bfloat16)
    order_s[0:128, :] = order
    order_s[128:256, :] = order
    barrier = pltpu.get_barrier_semaphore()
    for way, there, peer in links:

        @pl.when(there)
        def _():
            pl.semaphore_signal(barrier, inc=1, device_id=peer, device_id_type=MESH)

    for cp in copies[1:4]:
        cp.wait()

    half = 0.5 * time_step
    pos = d_s[...] + time_step * v_s[...] + (half * time_step) * a_s[...]
    pos_out[...] = pos

    lane = lax.broadcasted_iota(jnp.int32, (1, 128), 1)

    def chunk(q):
        width = min(128, PLANE * NX - 128 * q)
        part = pos_out[:, 128 * q : 128 * q + width]
        if width < 128:
            part = jnp.concatenate([part, jnp.zeros((3, 128 - width), jnp.float32)], axis=1)
        return part

    ahead = (4 * PLANE - STRIDE) // 128
    blank = jnp.zeros((3, 128), jnp.float32)
    single = [chunk(q) for q in range(-(-PLANE * NX // 128))]
    double = [
        jnp.concatenate([v, single[q + ahead] if q + ahead < len(single) else blank], axis=0)
        for q, v in enumerate(single)
    ]

    def window(source, x, ey):
        q, at = divmod(PLANE * x + STRIDE * ey, 128)
        part = source[q]
        if at + SPAN > 128:
            part = jnp.where(lane >= at, part, source[q + 1])
        return pltpu.roll(part, 128 - at, 1) if at else part

    def keep(x, ey, part):
        ex, a = divmod(x, 4)
        spots = [(a, ex)] if x < NX - 1 else []
        if x and a == 0:
            spots.append((4, ex - 1))
        for a, ex in spots:
            first = 3 * ((a * EY + ey) * EX + ex)
            w_s[first : first + 3, :] = part

    for x in range(NX):
        paired = x < NX - 1 and x % 8 < 4
        for ey in range(EY):
            if paired:
                part = window(double, x, ey)
                keep(x, ey, part[:3])
                if ey:
                    keep(x + 4, ey - 1, part[3:])
            elif x == NX - 1 or ey == EY - 1:
                keep(x, ey, window(single, x, ey))

    copies[4].wait()
    pltpu.make_async_copy(
        whole.at[pl.ds(0, 4)], raw_s.at[pl.ds(9, 4), point], in_sem.at[5]
    ).wait()
    copies[9].wait()
    for first, many in SPLITS:
        raw = raw_s[first : first + many].reshape(many * 128, 128)
        sorted_s[first : first + many] = jnp.dot(
            jnp.concatenate(split2(raw), axis=1),
            order_s[...],
            preferred_element_type=jnp.float32,
        ).reshape(many, 128, 128)

    left = lax.broadcasted_iota(jnp.int32, (SLOT, 128), 1) < 64
    each = EX * EY

    def block(c, a):
        return w_s[pl.ds(3 * each * a + c, each, stride=3), :]

    for (c, a), (d, b) in PAIRS[:6] + (((0, 4), (1, 4)), ((2, 4), (2, 4))):
        turned = jnp.transpose(jnp.concatenate([block(c, a), block(d, b)], axis=0))[:SLOT]
        other = pltpu.roll(turned, 64, 1)
        rise = lambda v: pltpu.roll(v, SLOT - 4, 0)
        u_s[SLOT * a : SLOT * (a + 1), 128 * c : 128 * (c + 1)] = jnp.where(
            left, turned, rise(other)
        )
        if (c, a) != (d, b):
            u_s[SLOT * b : SLOT * (b + 1), 128 * d : 128 * (d + 1)] = jnp.where(
                left, other, rise(turned)
            )

    local = product(deriv_s[0], deriv_s[1], u_s[...])
    for i in range(16):
        at = slice(8 * i, 8 * i + 8)
        maps = [[sorted_s[3 * l + j, at] for j in range(3)] for l in range(3)]
        weight, lam, mu, dens_e = (sorted_s[9 + k, at] for k in range(4))
        grads = [[local[c][128 * l + 8 * i : 128 * l + 8 * i + 8] for c in range(3)] for l in range(3)]
        h = [
            [sum(grads[l][c] * maps[l][j] for l in range(3)) for j in range(3)]
            for c in range(3)
        ]
        mu = mu * weight
        div = lam * weight * (h[0][0] + h[1][1] + h[2][2])
        stress = [[None] * 3 for _ in range(3)]
        for c in range(3):
            for j in range(c, 3):
                s = mu * (h[c][j] + h[j][c])
                stress[c][j] = stress[j][c] = s + div if c == j else s
        for l in range(3):
            for c in range(3):
                fl_s[128 * l + 8 * i : 128 * l + 8 * i + 8, 128 * c : 128 * (c + 1)] = sum(
                    stress[c][j] * maps[l][j] for j in range(3)
                )
        md_s[at, :] = dens_e * weight
    for cp in copies[10:]:
        cp.wait()
    terms = product(back_s[0], back_s[1], fl_s[...])
    heavy = sum(
        jnp.dot(spread_s[...], part, preferred_element_type=jnp.float32)
        for part in split2(md_s[...])
    )

    def term(c, a):
        at = slice(SLOT * a, SLOT * (a + 1))
        return terms[c][at] if c < 3 else heavy[at]

    sink = lambda v: pltpu.roll(v, 4, 0)
    tail = jnp.zeros((128, 128 - SLOT), jnp.float32)
    crest = {}
    rows = lax.broadcasted_iota(jnp.int32, (each, 128), 0)
    def settle_block(one_at, two_at):
        (c, a), (d, b) = one_at, two_at
        one, two = term(c, a), term(d, b)
        both = jnp.where(left, one, sink(two)) + pltpu.roll(jnp.where(left, two, sink(one)), 64, 1)
        turned = jnp.concatenate([jnp.transpose(both), tail], axis=1)
        for k, part in (((c, a), turned[:each]), ((d, b), turned[each:])):
            if k[1] == 4:
                top_s[each * k[0] : each * (k[0] + 1), :] = part
                crest[k[0]] = jnp.where(rows % EX == 0, 0.0, pltpu.roll(part, 1, 0))
                continue
            if k[1] == 0:
                part = part + crest[k[0]]
            for ey in range(EY):
                first = ((k[0] * EY + ey) * 4 + k[1]) * EX
                z_s[first : first + EX, :] = part[EX * ey : EX * (ey + 1)]

    def row_ends(sy):
        ey = (EY - 1) * sy
        crown = top_s[pl.ds(EX * ey + EX - 1, 4, stride=each), :]
        return ey, STRIDE * sy, crown

    sides = (pl.ds(0, 4, stride=16), pl.ds(64, 4))
    lanes = lax.broadcasted_iota(jnp.int32, (SROW, 128), 1)
    lane8 = lax.broadcasted_iota(jnp.int32, (8, 128), 1)
    far = CHUNKS - 1
    def route(way):
        sx, sy, sz = ((w + 1) // 2 for w in way)
        ox, oy, oz = 1 - sx, 1 - sy, 1 - sz
        dx, dy, dz = (w != 0 for w in way)
        if dx and dy and dz:
            return c_send.at[sx, sy, sz], c_recv.at[ox, oy, oz]
        if dx and dy:
            return f_send.at[sx, sy], f_recv.at[ox, oy]
        if dx and dz:
            return e_send.at[sx, sz], e_recv.at[ox, oz]
        if dy and dz:
            return q_send.at[sy, sz], q_recv.at[oy, oz]
        if dx:
            return x_send.at[sx], x_recv.at[ox]
        if dy:
            return p_send.at[sy], p_recv.at[oy]
        return m_send.at[sz], m_recv.at[oz]

    def copy(source, target, peer):
        return pltpu.make_async_remote_copy(
            src_ref=source,
            dst_ref=target,
            send_sem=send_sem.at[0],
            recv_sem=recv_sem.at[0],
            device_id=peer,
            device_id_type=MESH,
        )

    def await_all(settle):
        for (nx, ny, nz), here in classes():
            count = nx * CHUNKS + nx * ny + nx * nz + nx * ny * nz
            count += 2 * ny + 2 * ny * nz + nz * SROW // 4
            whole = tally.at[pl.ds(0, count)]

            @pl.when(here)
            def _():
                settle(copy(whole, whole, links[0][2]))

    peers = sum(there.astype(jnp.int32) for way, there, peer in links)
    farthest = sorted(range(len(WAYS)), key=lambda k: -sum(map(abs, WAYS[k])))

    def depart(chosen):
        for dy in (0, -1, 1):
            leaving = [k for k in farthest if WAYS[k][1] == dy and chosen(WAYS[k])]

            def send():
                for k in leaving:
                    way, there, peer = links[k]
                    if way in ((0, -1, 0), (0, 1, 0)):
                        copy(*route(way), peer).start()
                        continue

                    @pl.when(there)
                    def _():
                        copy(*route(way), peer).start()

            if leaving and dy:
                pl.when(links[WAYS.index((0, dy, 0))][1])(send)
            elif leaving:
                send()

    for one_at, two_at in (((0, 4), (1, 4)), ((2, 4), (3, 4))) + PAIRS[::2] + PAIRS[1::2]:
        settle_block(one_at, two_at)
    for sy in range(2):
        ey, base, crown = row_ends(sy)
        rows = jnp.concatenate([z_s[pl.ds(16 * ey, 4, stride=16 * EY), :], crown], axis=0)
        first = TAIL * (1 - sy)
        got = pltpu.roll(rows, (first - base) % 128, 1)
        got = jnp.where((lane8 >= first) & (lane8 < first + NZ), got, 0.0)
        f_send[0, sy] = got[:4]
        f_send[1, sy] = got[4:]
        for sz in range(2):
            got = pltpu.roll(rows, (first - base + (8 if sz == 0 else -8)) % 128, 1)
            got = jnp.where(lane8 == first + (NZ - 1) * (1 - sz), got, 0.0)
            c_send[0, sy, sz] = got[:4]
            c_send[1, sy, sz] = got[4:]
    pl.semaphore_wait(barrier, peers)
    depart(lambda way: way[0] != 0 and way[1] != 0)
    for sy in range(2):
        ey, base, crown = row_ends(sy)
        parts = [z_s[pl.ds(16 * (c * EY + ey) + 8 * h, 8), :] for c in range(4) for h in range(2)]
        parts.append(jnp.concatenate([crown, jnp.zeros((4, 128), jnp.float32)], axis=0))

        def pack(low, high, move):
            packed = None
            for i, part in enumerate(parts):
                got = jnp.where((lane8 >= base + low) & (lane8 < base + high), part, 0.0)
                shift = (PITCH * i - base + move) % 128
                got = pltpu.roll(got, shift, 1) if shift else got
                packed = got if packed is None else packed + got
            return packed

        p_send[sy] = pack(0, NZ, 0)
        q_send[sy, 0] = pack(0, 1, NZ - 1)
        q_send[sy, 1] = pack(NZ - 1, NZ, 1 - NZ)
    depart(lambda way: way[0] == 0 and way[1] != 0)

    for c in range(5):
        first, many = (16 * c, 16) if c < 4 else (64, 8)
        sums = [None] * CHUNKS
        for ey in range(EY):
            j, at = divmod(STRIDE * ey, 128)
            if c < 4:
                part = z_s[16 * (c * EY + ey) : 16 * (c * EY + ey + 1), :]
            else:
                part = top_s[pl.ds(EX * ey + EX - 1, 4, stride=each), :]
                part = jnp.concatenate([part, jnp.zeros((4, 128), jnp.float32)], axis=0)
            part = pltpu.roll(part, at, 1) if at else part
            pieces = [(j, part)]
            if at + SLOT > 128:
                pieces = [
                    (j, jnp.where(lane >= at, part, 0.0)),
                    (j + 1, jnp.where(lane < at, part, 0.0)),
                ]
            for k, piece in pieces:
                sums[k] = piece if sums[k] is None else sums[k] + piece
        for j in range(CHUNKS):
            grid_s[j, first : first + many, :] = sums[j]

    for side in range(2):
        for j in range(CHUNKS):
            x_send[side, j] = grid_s[j, sides[side], :]
    sources = [
        jnp.minimum(NZ * lanes + (NZ - 1) * dz, 128 * CHUNKS - 1) for dz in range(2)
    ]

    def face(parts, dz):
        many = parts[0].shape[0]
        source = sources[dz][:many]
        found = None
        for j in range(CHUNKS):
            got = jnp.take_along_axis(
                parts[j], source & 127, axis=1, mode="promise_in_bounds"
            )
            found = got if found is None else jnp.where(source >= 128 * j, got, found)
        return jnp.where(lanes[:many] < NY, found, 0.0)

    rims = [
        jnp.concatenate([x_send[0, j], x_send[1, j]], axis=0) for j in range(CHUNKS)
    ]
    for dz in range(2):
        got = face(rims, dz)
        e_send[0, dz] = got[:4]
        e_send[1, dz] = got[4:]
    depart(lambda way: way[1] == 0 and way[0] != 0)
    for dz in range(2):
        m_send[dz] = face([grid_s[j] for j in range(CHUNKS)], dz)
    depart(lambda way: way[1] == 0 and way[0] == 0)
    vel_out[...] = v_s[...] + half * a_s[...]

    await_all(lambda copied: copied.wait_recv())

    for dz in range(2):
        for sx in range(2):
            m_recv[dz, sides[sx], :] += e_recv[sx, dz]
    full = [m_recv[dz] for dz in range(2)]
    strips = []
    for sy in range(2):
        sums = p_recv[sy] + q_recv[sy, 0] + q_recv[sy, 1]
        parts = []
        for i in range(SROW // 8):
            shift = (TAIL * sy - PITCH * i) % 128
            got = pltpu.roll(sums, shift, 1) if shift else sums
            parts.append(
                jnp.where((lane8 >= TAIL * sy) & (lane8 < TAIL * sy + NZ), got, 0.0)
            )
        strips.append(jnp.concatenate(parts, axis=0))
        for sx in range(2):
            x_recv[sx, far * sy] += f_recv[sx, sy] + (c_recv[sx, sy, 0] + c_recv[sx, sy, 1])
    for j in range(CHUNKS):
        node = lanes + 128 * j
        along = lax.div(node, NZ)
        depth = node - NZ * along
        sums = grid_s[j]
        for dz in range(2):
            got = jnp.take_along_axis(
                full[dz], jnp.minimum(along, 127), axis=1, mode="promise_in_bounds"
            )
            sums = sums + jnp.where((depth == (NZ - 1) * dz) & (along < NY), got, 0.0)
        if j == 0:
            sums = sums + strips[0]
        if j == far:
            sums = sums + strips[1]
        grid_s[j] = sums
        for sx in range(2):
            grid_s[j, sides[sx], :] += x_recv[sx, j]
        mass = grid_s[j, 48:64, :]
        for c in range(3):
            grid_s[j, 16 * c : 16 * c + 16, :] = grid_s[j, 16 * c : 16 * c + 16, :] / mass
        grid_s[j, 64:67, :] = grid_s[j, 64:67, :] / grid_s[j, 67:68, :]

    for x in range(NX):
        rows = pl.ds(4 * (x % 4) + x // 4, 3, stride=16) if x < NX - 1 else pl.ds(64, 3)
        for j in range(CHUNKS):
            width = min(128, PLANE - 128 * j)
            at = PLANE * x + 128 * j
            acc_out[:, at : at + width] = grid_s[j, rows, 0:width]
    await_all(lambda copied: copied.wait_send())


def finish(pos, vel, acc, pos_out, vel_out, acc_out, v_s, sem):
    def put(src, dst, k):
        copy = pltpu.make_async_copy(src, dst.at[:, 0], sem.at[k])
        copy.start()
        return copy

    copies = [put(pos, pos_out, 0), put(acc, acc_out, 1)]
    v_s[...] = vel[...] + (0.5 * time_step) * acc[...]
    copies.append(put(v_s, vel_out, 2))
    for cp in copies:
        cp.wait()


def body(displ, veloc, accel, node_index, inv_map, jac_weight, lame_first, shear_mod, density):
    nodes = displ.shape[4]
    elements = node_index.shape[4]
    deriv, back, spread = constants()
    deriv, back = halves(deriv), halves(back)
    fields = [x.reshape(3, 1, nodes) for x in (displ, veloc, accel)]
    elems = [
        x.reshape(125, 1, elements) for x in (jac_weight, lame_first, shear_mod, density)
    ]
    vmem = pl.BlockSpec(memory_space=pltpu.VMEM)
    hbm = pl.BlockSpec(memory_space=pltpu.HBM)
    f32 = jnp.float32
    out = jax.ShapeDtypeStruct((3, 1, nodes), f32)
    result = pl.pallas_call(
        kernel,
        out_shape=[pltpu.VMEM((3, nodes), f32)] * 3,
        in_specs=[hbm] * 12,
        out_specs=[vmem] * 3,
        scratch_shapes=[
            pltpu.VMEM(deriv.shape, jnp.bfloat16),
            pltpu.VMEM(back.shape, jnp.bfloat16),
            pltpu.VMEM(spread.shape, jnp.bfloat16),
            pltpu.VMEM((3, nodes), f32),
            pltpu.VMEM((3, nodes), f32),
            pltpu.VMEM((3, nodes), f32),
            pltpu.VMEM((1, elements), jnp.int32),
            pltpu.VMEM((13, 128, elements), f32),
            pltpu.VMEM((256, 128), jnp.bfloat16),
            pltpu.VMEM((13, 128, 128), f32),
            pltpu.VMEM((15 * EX * EY, 128), f32),
            pltpu.VMEM((16 * EX * EY, 128), f32),
            pltpu.VMEM((4 * EX * EY, 128), f32),
            pltpu.VMEM((5 * SLOT, 384), f32),
            pltpu.VMEM((384, 384), f32),
            pltpu.VMEM((128, 128), f32),
            pltpu.VMEM((CHUNKS, SROW, 128), f32),
            pltpu.VMEM((2, SROW, 128), f32),
            pltpu.VMEM((2, 8, 128), f32),
            pltpu.VMEM((2, CHUNKS, 4, 128), f32),
            pltpu.VMEM((2, 2, 4, 128), f32),
            pltpu.VMEM((2, 2, 8, 128), f32),
            pltpu.VMEM((2, 2, 4, 128), f32),
            pltpu.VMEM((2, 2, 2, 4, 128), f32),
            pltpu.VMEM((2, SROW, 128), f32),
            pltpu.VMEM((2, 8, 128), f32),
            pltpu.VMEM((2, 2, 8, 128), f32),
            pltpu.VMEM((2, CHUNKS, 4, 128), f32),
            pltpu.VMEM((2, 2, 4, 128), f32),
            pltpu.VMEM((2, 2, 4, 128), f32),
            pltpu.VMEM((2, 2, 2, 4, 128), f32),
            pltpu.VMEM((2 * SROW // 4 + 2 * CHUNKS + 28, 4, 128), f32),
            pltpu.SemaphoreType.DMA((9,)),
            pltpu.SemaphoreType.DMA((1,)),
            pltpu.SemaphoreType.DMA((1,)),
        ],
        compiler_params=pltpu.CompilerParams(
            collective_id=0, has_side_effects=True, vmem_limit_bytes=LIMIT
        ),
    )(
        *fields,
        node_index.reshape(125, 1, elements),
        inv_map.reshape(9, 125, 1, elements),
        *elems,
        jnp.asarray(deriv),
        jnp.asarray(back),
        jnp.asarray(spread, jnp.bfloat16),
    )
    final = pl.pallas_call(
        finish,
        out_shape=[out] * 3,
        in_specs=[vmem] * 3,
        out_specs=[hbm] * 3,
        scratch_shapes=[pltpu.VMEM((3, nodes), f32), pltpu.SemaphoreType.DMA((3,))],
        compiler_params=pltpu.CompilerParams(vmem_limit_bytes=LIMIT),
    )(*[pltpu.with_memory_space_constraint(x, pltpu.VMEM) for x in result])
    return tuple(x.reshape(displ.shape) for x in final)


def solution(mesh):
    field = P(None, "gx", "gy", "gz", None)
    elem = P("gx", "gy", "gz", None, None)
    placed = (field,) * 3 + (elem, P("gx", "gy", "gz", None, None, None)) + (elem,) * 4
    return jax.shard_map(
        body, mesh=mesh, in_specs=placed, out_specs=(field,) * 3, check_vma=False
    )
```

```python
import jax
import jax.numpy as jnp
import numpy as np
from jax import lax
from jax.experimental import pallas as pl
from jax.experimental.pallas import tpu as pltpu
from jax.sharding import PartitionSpec as P

EX = 4
EY = 16
EZ = 2
NX = 4 * EX + 1
NY = 4 * EY + 1
NZ = 4 * EZ + 1
PLANE = NY * NZ
CHUNKS = -(-PLANE // 128)
STRIDE = 4 * NZ
SPAN = 5 * NZ
SLOT = 48
SROW = 72
TAIL = PLANE - NZ - 128 * (CHUNKS - 1)
PITCH = 14
ORDER = (4, 0, 1, 2, 3)
SPLITS = ((0, 7), (7, 6))
PAIRS = tuple(((c, a), (c, a + 1)) for c in range(4) for a in (0, 2))

LIMIT = 65 * 1000 * 1000

time_step = 0.1
MESH = pl.DeviceIdType.MESH


def derivative_table():
    points = np.array([-1.0, -np.sqrt(3.0 / 7.0), 0.0, np.sqrt(3.0 / 7.0), 1.0])
    count = points.shape[0]
    weights = np.array(
        [
            1.0 / np.prod([points[s] - points[o] for o in range(count) if o != s])
            for s in range(count)
        ]
    )
    table = np.zeros((count, count))
    for t in range(count):
        for s in range(count):
            if t != s:
                table[t, s] = weights[s] / weights[t] / (points[t] - points[s])
        table[t, t] = -np.sum(table[t])
    return table


def constants():
    table = derivative_table()
    eye = np.eye(5)
    parts = [
        np.kron(table, np.kron(eye, eye)),
        np.kron(eye, np.kron(table, eye)),
        np.kron(eye, np.kron(eye, table)),
    ]
    pad = np.zeros((125, 5 * SLOT))
    for a in range(5):
        for b in range(5):
            for c in range(5):
                pad[a * 25 + 5 * b + c, a * SLOT + NZ * b + c] = 1.0
    deriv = np.zeros((384, 5 * SLOT), np.float32)
    for l in range(3):
        deriv[l * 128 : l * 128 + 125] = parts[l] @ pad
    spread = np.zeros((5 * SLOT, 128), np.float32)
    spread[:, :125] = pad.T
    rows = np.concatenate([np.arange(SLOT * a, SLOT * (a + 1)) for a in ORDER])
    return deriv, -deriv.T[rows], spread[rows]


def split2(x):
    hi = x.astype(jnp.bfloat16)
    low = (x - hi.astype(jnp.float32)).astype(jnp.bfloat16)
    return (hi, low)


def halves(x):
    hi = np.asarray(x, jnp.bfloat16)
    low = np.asarray(x - hi.astype(np.float32), jnp.bfloat16)
    return np.stack([hi, low])


def product(hi, low, y):
    top, rest = split2(y)
    dot = lambda a, b: jnp.dot(a, b, preferred_element_type=jnp.float32)
    wide = lambda *parts: jnp.concatenate(parts, axis=1)
    if y.shape[0] > 256:
        first = dot(
            wide(hi, hi, low),
            jnp.concatenate([top[:, :256], rest[:, :256], top[:, :256]], axis=0),
        )
    else:
        first = dot(hi, top[:, :256]) + dot(hi, rest[:, :256]) + dot(low, top[:, :256])
    both = dot(hi, wide(top[:, 256:], rest[:, 256:]))
    last = both[:, :128] + both[:, 128:] + dot(low, top[:, 256:])
    return first[:, :128], first[:, 128:], last


def ways():
    steps = (0, -1, 1)
    found = [(x, y, z) for z in steps for y in steps for x in steps][1:]
    half = [w for w in found if w > (0, 0, 0)]
    half.sort(key=lambda w: (sum(map(abs, w)), -abs(w[2])))
    other = [tuple(-v for v in w) for w in half]
    return half + other[::-1]


WAYS = ways()


def neighbours():
    names = ("gx", "gy", "gz")
    spots = [lax.axis_index(n) for n in names]
    sizes = [lax.axis_size(n) for n in names]
    links = []
    for way in WAYS:
        there = None
        peer = {}
        for n, s, z, w in zip(names, spots, sizes, way):
            if w:
                ok = s > 0 if w < 0 else s < z - 1
                there = ok if there is None else there & ok
                peer[n] = s + w
        links.append((way, there, peer))
    return links


def classes():
    found = [((), None)]
    for name in ("gx", "gy", "gz"):
        size, spot = lax.axis_size(name), lax.axis_index(name)
        inner = (spot > 0) & (spot < size - 1)
        choices = [(min(size - 1, 1), None)]
        if size > 2:
            choices = [(1, jnp.logical_not(inner)), (2, inner)]
        grown = []
        for counts, here in found:
            for count, ok in choices:
                both = here if ok is None else ok if here is None else here & ok
                grown.append((counts + (count,), both))
        found = grown
    return [(counts, True if here is None else here) for counts, here in found]


def squeezed(ref):
    return ref.at[:, 0] if len(ref.shape) == 3 else ref.at[:, :, 0]


def kernel(
    displ, veloc, accel, node, inv, jac, lame, shear, dens,
    deriv_ref, back_ref, spread_ref,
    pos_out, vel_out, acc_out,
    deriv_s, back_s, spread_s,
    d_s, v_s, a_s, node_s, raw_s,
    order_s, sorted_s, w_s, z_s, top_s, u_s, fl_s, md_s, grid_s,
    m_send, p_send, x_send, e_send, q_send, f_send, c_send,
    m_recv, p_recv, q_recv, x_recv, e_recv, f_recv, c_recv,
    tally, in_sem, send_sem, recv_sem,
):
    links = neighbours()
    head = node.at[pl.ds(0, 1), 0]
    copies = [pltpu.make_async_copy(head, node_s, in_sem.at[0])]
    for k, (src, dst) in enumerate(((displ, d_s), (veloc, v_s), (accel, a_s))):
        copies.append(pltpu.make_async_copy(src.at[:, 0], dst, in_sem.at[1 + k]))
    whole = squeezed(inv)
    point = pl.ds(0, 125)
    copies.append(pltpu.make_async_copy(whole, raw_s.at[pl.ds(0, 9), point], in_sem.at[4]))
    for k, src in enumerate((jac, lame, shear, dens)):
        copies.append(pltpu.make_async_copy(squeezed(src), raw_s.at[9 + k, point], in_sem.at[5]))
    consts = ((deriv_ref, deriv_s), (back_ref, back_s), (spread_ref, spread_s))
    for k, (src, dst) in enumerate(consts):
        copies.append(pltpu.make_async_copy(src, dst, in_sem.at[6 + k]))
    for cp in copies:
        cp.start()
    raw_s[:, 125:128, :] = jnp.zeros((13, 3, 128), jnp.float32)
    for ref in (m_recv, p_recv, q_recv, x_recv, e_recv, f_recv, c_recv):
        ref[...] = jnp.zeros_like(ref)
    copies[0].wait()
    corner = node_s[0:1, :].astype(jnp.float32)
    x0 = jnp.floor((corner + 0.5) * (1.0 / PLANE))
    rem = corner - PLANE * x0
    y0 = jnp.floor((rem + 0.5) * (1.0 / NZ))
    z0 = rem - NZ * y0
    goal = EY * EX * 0.25 * z0 + EX * 0.25 * y0 + 0.25 * x0
    goal = jnp.transpose(jnp.broadcast_to(goal, (128, 128)))
    slots = lax.broadcasted_iota(jnp.int32, (128, 128), 1).astype(jnp.float32)
    order = jnp.where(slots == goal, 1.0, 0.0).astype(jnp.bfloat16)
    order_s[0:128, :] = order
    order_s[128:256, :] = order
    barrier = pltpu.get_barrier_semaphore()
    for way, there, peer in links:

        @pl.when(there)
        def _():
            pl.semaphore_signal(barrier, inc=1, device_id=peer, device_id_type=MESH)

    for cp in copies[1:4]:
        cp.wait()

    half = 0.5 * time_step
    pos = d_s[...] + time_step * v_s[...] + (half * time_step) * a_s[...]
    pos_out[...] = pos

    lane = lax.broadcasted_iota(jnp.int32, (1, 128), 1)

    def chunk(q):
        width = min(128, PLANE * NX - 128 * q)
        part = pos_out[:, 128 * q : 128 * q + width]
        if width < 128:
            part = jnp.concatenate([part, jnp.zeros((3, 128 - width), jnp.float32)], axis=1)
        return part

    ahead = (4 * PLANE - STRIDE) // 128
    blank = jnp.zeros((3, 128), jnp.float32)
    single = [chunk(q) for q in range(-(-PLANE * NX // 128))]
    double = [
        jnp.concatenate([v, single[q + ahead] if q + ahead < len(single) else blank], axis=0)
        for q, v in enumerate(single)
    ]

    def window(source, x, ey):
        q, at = divmod(PLANE * x + STRIDE * ey, 128)
        part = source[q]
        if at + SPAN > 128:
            part = jnp.where(lane >= at, part, source[q + 1])
        return pltpu.roll(part, 128 - at, 1) if at else part

    def keep(x, ey, part):
        ex, a = divmod(x, 4)
        spots = [(a, ex)] if x < NX - 1 else []
        if x and a == 0:
            spots.append((4, ex - 1))
        for a, ex in spots:
            first = 3 * ((a * EY + ey) * EX + ex)
            w_s[first : first + 3, :] = part

    for x in range(NX):
        paired = x < NX - 1 and x % 8 < 4
        for ey in range(EY):
            if paired:
                part = window(double, x, ey)
                keep(x, ey, part[:3])
                if ey:
                    keep(x + 4, ey - 1, part[3:])
            elif x == NX - 1 or ey == EY - 1:
                keep(x, ey, window(single, x, ey))

    copies[4].wait()
    pltpu.make_async_copy(
        whole.at[pl.ds(0, 4)], raw_s.at[pl.ds(9, 4), point], in_sem.at[5]
    ).wait()
    copies[9].wait()
    for first, many in SPLITS:
        raw = raw_s[first : first + many].reshape(many * 128, 128)
        sorted_s[first : first + many] = jnp.dot(
            jnp.concatenate(split2(raw), axis=1),
            order_s[...],
            preferred_element_type=jnp.float32,
        ).reshape(many, 128, 128)

    left = lax.broadcasted_iota(jnp.int32, (SLOT, 128), 1) < 64
    each = EX * EY

    def block(c, a):
        return w_s[pl.ds(3 * each * a + c, each, stride=3), :]

    for (c, a), (d, b) in PAIRS[:6] + (((0, 4), (1, 4)), ((2, 4), (2, 4))):
        turned = jnp.transpose(jnp.concatenate([block(c, a), block(d, b)], axis=0))[:SLOT]
        other = pltpu.roll(turned, 64, 1)
        rise = lambda v: pltpu.roll(v, SLOT - 4, 0)
        u_s[SLOT * a : SLOT * (a + 1), 128 * c : 128 * (c + 1)] = jnp.where(
            left, turned, rise(other)
        )
        if (c, a) != (d, b):
            u_s[SLOT * b : SLOT * (b + 1), 128 * d : 128 * (d + 1)] = jnp.where(
                left, other, rise(turned)
            )

    local = product(deriv_s[0], deriv_s[1], u_s[...])
    for i in range(16):
        at = slice(8 * i, 8 * i + 8)
        maps = [[sorted_s[3 * l + j, at] for j in range(3)] for l in range(3)]
        weight, lam, mu, dens_e = (sorted_s[9 + k, at] for k in range(4))
        grads = [[local[c][128 * l + 8 * i : 128 * l + 8 * i + 8] for c in range(3)] for l in range(3)]
        h = [
            [sum(grads[l][c] * maps[l][j] for l in range(3)) for j in range(3)]
            for c in range(3)
        ]
        mu = mu * weight
        div = lam * weight * (h[0][0] + h[1][1] + h[2][2])
        stress = [[None] * 3 for _ in range(3)]
        for c in range(3):
            for j in range(c, 3):
                s = mu * (h[c][j] + h[j][c])
                stress[c][j] = stress[j][c] = s + div if c == j else s
        for l in range(3):
            for c in range(3):
                fl_s[128 * l + 8 * i : 128 * l + 8 * i + 8, 128 * c : 128 * (c + 1)] = sum(
                    stress[c][j] * maps[l][j] for j in range(3)
                )
        md_s[at, :] = dens_e * weight
    for cp in copies[10:]:
        cp.wait()
    terms = product(back_s[0], back_s[1], fl_s[...])
    heavy = sum(
        jnp.dot(spread_s[...], part, preferred_element_type=jnp.float32)
        for part in split2(md_s[...])
    )

    def term(c, a):
        at = slice(SLOT * ORDER.index(a), SLOT * (ORDER.index(a) + 1))
        return terms[c][at] if c < 3 else heavy[at]

    sink = lambda v: pltpu.roll(v, 4, 0)
    tail = jnp.zeros((128, 128 - SLOT), jnp.float32)
    crest = {}
    rows = lax.broadcasted_iota(jnp.int32, (each, 128), 0)
    def settle_block(one_at, two_at):
        (c, a), (d, b) = one_at, two_at
        one, two = term(c, a), term(d, b)
        both = jnp.where(left, one, sink(two)) + pltpu.roll(jnp.where(left, two, sink(one)), 64, 1)
        turned = jnp.concatenate([jnp.transpose(both), tail], axis=1)
        for k, part in (((c, a), turned[:each]), ((d, b), turned[each:])):
            if k[1] == 4:
                top_s[each * k[0] : each * (k[0] + 1), :] = part
                crest[k[0]] = jnp.where(rows % EX == 0, 0.0, pltpu.roll(part, 1, 0))
                continue
            if k[1] == 0:
                part = part + crest[k[0]]
            for ey in range(EY):
                first = ((k[0] * EY + ey) * 4 + k[1]) * EX
                z_s[first : first + EX, :] = part[EX * ey : EX * (ey + 1)]

    def row_ends(sy):
        ey = (EY - 1) * sy
        crown = top_s[pl.ds(EX * ey + EX - 1, 4, stride=each), :]
        return ey, STRIDE * sy, crown

    sides = (pl.ds(0, 4, stride=16), pl.ds(64, 4))
    lanes = lax.broadcasted_iota(jnp.int32, (SROW, 128), 1)
    lane8 = lax.broadcasted_iota(jnp.int32, (8, 128), 1)
    far = CHUNKS - 1
    def route(way):
        sx, sy, sz = ((w + 1) // 2 for w in way)
        ox, oy, oz = 1 - sx, 1 - sy, 1 - sz
        dx, dy, dz = (w != 0 for w in way)
        if dx and dy and dz:
            return c_send.at[sx, sy, sz], c_recv.at[ox, oy, oz]
        if dx and dy:
            return f_send.at[sx, sy], f_recv.at[ox, oy]
        if dx and dz:
            return e_send.at[sx, sz], e_recv.at[ox, oz]
        if dy and dz:
            return q_send.at[sy, sz], q_recv.at[oy, oz]
        if dx:
            return x_send.at[sx], x_recv.at[ox]
        if dy:
            return p_send.at[sy], p_recv.at[oy]
        return m_send.at[sz], m_recv.at[oz]

    def copy(source, target, peer):
        return pltpu.make_async_remote_copy(
            src_ref=source,
            dst_ref=target,
            send_sem=send_sem.at[0],
            recv_sem=recv_sem.at[0],
            device_id=peer,
            device_id_type=MESH,
        )

    def await_all(settle):
        for (nx, ny, nz), here in classes():
            count = nx * CHUNKS + nx * ny + nx * nz + nx * ny * nz
            count += 2 * ny + 2 * ny * nz + nz * SROW // 4
            whole = tally.at[pl.ds(0, count)]

            @pl.when(here)
            def _():
                settle(copy(whole, whole, links[0][2]))

    peers = sum(there.astype(jnp.int32) for way, there, peer in links)
    farthest = sorted(range(len(WAYS)), key=lambda k: -sum(map(abs, WAYS[k])))

    def depart(chosen):
        for dy in (0, -1, 1):
            leaving = [k for k in farthest if WAYS[k][1] == dy and chosen(WAYS[k])]

            def send():
                for k in leaving:
                    way, there, peer = links[k]
                    if way in ((0, -1, 0), (0, 1, 0)):
                        copy(*route(way), peer).start()
                        continue

                    @pl.when(there)
                    def _():
                        copy(*route(way), peer).start()

            if leaving and dy:
                pl.when(links[WAYS.index((0, dy, 0))][1])(send)
            elif leaving:
                send()

    for one_at, two_at in (((0, 4), (1, 4)), ((2, 4), (3, 4))) + PAIRS[::2] + PAIRS[1::2]:
        settle_block(one_at, two_at)
    for sy in range(2):
        ey, base, crown = row_ends(sy)
        rows = jnp.concatenate([z_s[pl.ds(16 * ey, 4, stride=16 * EY), :], crown], axis=0)
        first = TAIL * (1 - sy)
        got = pltpu.roll(rows, (first - base) % 128, 1)
        got = jnp.where((lane8 >= first) & (lane8 < first + NZ), got, 0.0)
        f_send[0, sy] = got[:4]
        f_send[1, sy] = got[4:]
        for sz in range(2):
            got = pltpu.roll(rows, (first - base + (8 if sz == 0 else -8)) % 128, 1)
            got = jnp.where(lane8 == first + (NZ - 1) * (1 - sz), got, 0.0)
            c_send[0, sy, sz] = got[:4]
            c_send[1, sy, sz] = got[4:]
    pl.semaphore_wait(barrier, peers)
    depart(lambda way: way[0] != 0 and way[1] != 0)
    for sy in range(2):
        ey, base, crown = row_ends(sy)
        parts = [z_s[pl.ds(16 * (c * EY + ey) + 8 * h, 8), :] for c in range(4) for h in range(2)]
        parts.append(jnp.concatenate([crown, jnp.zeros((4, 128), jnp.float32)], axis=0))

        def pack(low, high, move):
            packed = None
            for i, part in enumerate(parts):
                got = jnp.where((lane8 >= base + low) & (lane8 < base + high), part, 0.0)
                shift = (PITCH * i - base + move) % 128
                got = pltpu.roll(got, shift, 1) if shift else got
                packed = got if packed is None else packed + got
            return packed

        p_send[sy] = pack(0, NZ, 0)
        q_send[sy, 0] = pack(0, 1, NZ - 1)
        q_send[sy, 1] = pack(NZ - 1, NZ, 1 - NZ)
    depart(lambda way: way[0] == 0 and way[1] != 0)

    for c in range(5):
        first, many = (16 * c, 16) if c < 4 else (64, 8)
        sums = [None] * CHUNKS
        for ey in range(EY):
            j, at = divmod(STRIDE * ey, 128)
            if c < 4:
                part = z_s[16 * (c * EY + ey) : 16 * (c * EY + ey + 1), :]
            else:
                part = top_s[pl.ds(EX * ey + EX - 1, 4, stride=each), :]
                part = jnp.concatenate([part, jnp.zeros((4, 128), jnp.float32)], axis=0)
            part = pltpu.roll(part, at, 1) if at else part
            pieces = [(j, part)]
            if at + SLOT > 128:
                pieces = [
                    (j, jnp.where(lane >= at, part, 0.0)),
                    (j + 1, jnp.where(lane < at, part, 0.0)),
                ]
            for k, piece in pieces:
                sums[k] = piece if sums[k] is None else sums[k] + piece
        for j in range(CHUNKS):
            grid_s[j, first : first + many, :] = sums[j]

    for side in range(2):
        for j in range(CHUNKS):
            x_send[side, j] = grid_s[j, sides[side], :]
    sources = [
        jnp.minimum(NZ * lanes + (NZ - 1) * dz, 128 * CHUNKS - 1) for dz in range(2)
    ]

    def face(parts, dz):
        many = parts[0].shape[0]
        source = sources[dz][:many]
        found = None
        for j in range(CHUNKS):
            got = jnp.take_along_axis(
                parts[j], source & 127, axis=1, mode="promise_in_bounds"
            )
            found = got if found is None else jnp.where(source >= 128 * j, got, found)
        return jnp.where(lanes[:many] < NY, found, 0.0)

    rims = [
        jnp.concatenate([x_send[0, j], x_send[1, j]], axis=0) for j in range(CHUNKS)
    ]
    for dz in range(2):
        got = face(rims, dz)
        e_send[0, dz] = got[:4]
        e_send[1, dz] = got[4:]
    depart(lambda way: way[1] == 0 and way[0] != 0)
    for dz in range(2):
        m_send[dz] = face([grid_s[j] for j in range(CHUNKS)], dz)
    depart(lambda way: way[1] == 0 and way[0] == 0)
    vel_out[...] = v_s[...] + half * a_s[...]

    await_all(lambda copied: copied.wait_recv())

    for dz in range(2):
        for sx in range(2):
            m_recv[dz, sides[sx], :] += e_recv[sx, dz]
    full = [m_recv[dz] for dz in range(2)]
    strips = []
    for sy in range(2):
        sums = p_recv[sy] + q_recv[sy, 0] + q_recv[sy, 1]
        parts = []
        for i in range(SROW // 8):
            shift = (TAIL * sy - PITCH * i) % 128
            got = pltpu.roll(sums, shift, 1) if shift else sums
            parts.append(
                jnp.where((lane8 >= TAIL * sy) & (lane8 < TAIL * sy + NZ), got, 0.0)
            )
        strips.append(jnp.concatenate(parts, axis=0))
        for sx in range(2):
            x_recv[sx, far * sy] += f_recv[sx, sy] + (c_recv[sx, sy, 0] + c_recv[sx, sy, 1])
    for j in range(CHUNKS):
        node = lanes + 128 * j
        along = lax.div(node, NZ)
        depth = node - NZ * along
        sums = grid_s[j]
        for dz in range(2):
            got = jnp.take_along_axis(
                full[dz], jnp.minimum(along, 127), axis=1, mode="promise_in_bounds"
            )
            sums = sums + jnp.where((depth == (NZ - 1) * dz) & (along < NY), got, 0.0)
        if j == 0:
            sums = sums + strips[0]
        if j == far:
            sums = sums + strips[1]
        grid_s[j] = sums
        for sx in range(2):
            grid_s[j, sides[sx], :] += x_recv[sx, j]
        mass = grid_s[j, 48:64, :]
        for c in range(3):
            grid_s[j, 16 * c : 16 * c + 16, :] = grid_s[j, 16 * c : 16 * c + 16, :] / mass
        grid_s[j, 64:67, :] = grid_s[j, 64:67, :] / grid_s[j, 67:68, :]

    for x in range(NX):
        rows = pl.ds(4 * (x % 4) + x // 4, 3, stride=16) if x < NX - 1 else pl.ds(64, 3)
        for j in range(CHUNKS):
            width = min(128, PLANE - 128 * j)
            at = PLANE * x + 128 * j
            acc_out[:, at : at + width] = grid_s[j, rows, 0:width]
    await_all(lambda copied: copied.wait_send())


def finish(pos, vel, acc, pos_out, vel_out, acc_out, v_s, sem):
    def put(src, dst, k):
        copy = pltpu.make_async_copy(src, dst.at[:, 0], sem.at[k])
        copy.start()
        return copy

    copies = [put(pos, pos_out, 0), put(acc, acc_out, 1)]
    v_s[...] = vel[...] + (0.5 * time_step) * acc[...]
    copies.append(put(v_s, vel_out, 2))
    for cp in copies:
        cp.wait()


def body(displ, veloc, accel, node_index, inv_map, jac_weight, lame_first, shear_mod, density):
    nodes = displ.shape[4]
    elements = node_index.shape[4]
    deriv, back, spread = constants()
    deriv, back = halves(deriv), halves(back)
    fields = [x.reshape(3, 1, nodes) for x in (displ, veloc, accel)]
    elems = [
        x.reshape(125, 1, elements) for x in (jac_weight, lame_first, shear_mod, density)
    ]
    vmem = pl.BlockSpec(memory_space=pltpu.VMEM)
    hbm = pl.BlockSpec(memory_space=pltpu.HBM)
    f32 = jnp.float32
    out = jax.ShapeDtypeStruct((3, 1, nodes), f32)
    result = pl.pallas_call(
        kernel,
        out_shape=[pltpu.VMEM((3, nodes), f32)] * 3,
        in_specs=[hbm] * 12,
        out_specs=[vmem] * 3,
        scratch_shapes=[
            pltpu.VMEM(deriv.shape, jnp.bfloat16),
            pltpu.VMEM(back.shape, jnp.bfloat16),
            pltpu.VMEM(spread.shape, jnp.bfloat16),
            pltpu.VMEM((3, nodes), f32),
            pltpu.VMEM((3, nodes), f32),
            pltpu.VMEM((3, nodes), f32),
            pltpu.VMEM((1, elements), jnp.int32),
            pltpu.VMEM((13, 128, elements), f32),
            pltpu.VMEM((256, 128), jnp.bfloat16),
            pltpu.VMEM((13, 128, 128), f32),
            pltpu.VMEM((15 * EX * EY, 128), f32),
            pltpu.VMEM((16 * EX * EY, 128), f32),
            pltpu.VMEM((4 * EX * EY, 128), f32),
            pltpu.VMEM((5 * SLOT, 384), f32),
            pltpu.VMEM((384, 384), f32),
            pltpu.VMEM((128, 128), f32),
            pltpu.VMEM((CHUNKS, SROW, 128), f32),
            pltpu.VMEM((2, SROW, 128), f32),
            pltpu.VMEM((2, 8, 128), f32),
            pltpu.VMEM((2, CHUNKS, 4, 128), f32),
            pltpu.VMEM((2, 2, 4, 128), f32),
            pltpu.VMEM((2, 2, 8, 128), f32),
            pltpu.VMEM((2, 2, 4, 128), f32),
            pltpu.VMEM((2, 2, 2, 4, 128), f32),
            pltpu.VMEM((2, SROW, 128), f32),
            pltpu.VMEM((2, 8, 128), f32),
            pltpu.VMEM((2, 2, 8, 128), f32),
            pltpu.VMEM((2, CHUNKS, 4, 128), f32),
            pltpu.VMEM((2, 2, 4, 128), f32),
            pltpu.VMEM((2, 2, 4, 128), f32),
            pltpu.VMEM((2, 2, 2, 4, 128), f32),
            pltpu.VMEM((2 * SROW // 4 + 2 * CHUNKS + 28, 4, 128), f32),
            pltpu.SemaphoreType.DMA((9,)),
            pltpu.SemaphoreType.DMA((1,)),
            pltpu.SemaphoreType.DMA((1,)),
        ],
        compiler_params=pltpu.CompilerParams(
            collective_id=0, has_side_effects=True, vmem_limit_bytes=LIMIT
        ),
    )(
        *fields,
        node_index.reshape(125, 1, elements),
        inv_map.reshape(9, 125, 1, elements),
        *elems,
        jnp.asarray(deriv),
        jnp.asarray(back),
        jnp.asarray(spread, jnp.bfloat16),
    )
    final = pl.pallas_call(
        finish,
        out_shape=[out] * 3,
        in_specs=[vmem] * 3,
        out_specs=[hbm] * 3,
        scratch_shapes=[pltpu.VMEM((3, nodes), f32), pltpu.SemaphoreType.DMA((3,))],
        compiler_params=pltpu.CompilerParams(vmem_limit_bytes=LIMIT),
    )(*[pltpu.with_memory_space_constraint(x, pltpu.VMEM) for x in result])
    return tuple(x.reshape(displ.shape) for x in final)


def solution(mesh):
    field = P(None, "gx", "gy", "gz", None)
    elem = P("gx", "gy", "gz", None, None)
    placed = (field,) * 3 + (elem, P("gx", "gy", "gz", None, None, None)) + (elem,) * 4
    return jax.shard_map(
        body, mesh=mesh, in_specs=placed, out_specs=(field,) * 3, check_vma=False
    )
```

```python
import jax
import jax.numpy as jnp
import numpy as np
from jax import lax
from jax.experimental import pallas as pl
from jax.experimental.pallas import tpu as pltpu
from jax.sharding import PartitionSpec as P

EX = 4
EY = 16
EZ = 2
NX = 4 * EX + 1
NY = 4 * EY + 1
NZ = 4 * EZ + 1
PLANE = NY * NZ
CHUNKS = -(-PLANE // 128)
STRIDE = 4 * NZ
SPAN = 5 * NZ
SLOT = 48
SROW = 72
TAIL = PLANE - NZ - 128 * (CHUNKS - 1)
PITCH = 14
ORDER = (4, 0, 1, 2, 3)
SPLITS = ((0, 7), (7, 6))
PAIRS = tuple(((c, a), (c, a + 1)) for c in range(4) for a in (0, 2))
FIRST = (((0, 4), (1, 4)),) + PAIRS[:4:2] + (((2, 4), (3, 4)),) + PAIRS[4::2]

LIMIT = 65 * 1000 * 1000

time_step = 0.1
MESH = pl.DeviceIdType.MESH


def derivative_table():
    points = np.array([-1.0, -np.sqrt(3.0 / 7.0), 0.0, np.sqrt(3.0 / 7.0), 1.0])
    count = points.shape[0]
    weights = np.array(
        [
            1.0 / np.prod([points[s] - points[o] for o in range(count) if o != s])
            for s in range(count)
        ]
    )
    table = np.zeros((count, count))
    for t in range(count):
        for s in range(count):
            if t != s:
                table[t, s] = weights[s] / weights[t] / (points[t] - points[s])
        table[t, t] = -np.sum(table[t])
    return table


def constants():
    table = derivative_table()
    eye = np.eye(5)
    parts = [
        np.kron(table, np.kron(eye, eye)),
        np.kron(eye, np.kron(table, eye)),
        np.kron(eye, np.kron(eye, table)),
    ]
    pad = np.zeros((125, 5 * SLOT))
    for a in range(5):
        for b in range(5):
            for c in range(5):
                pad[a * 25 + 5 * b + c, a * SLOT + NZ * b + c] = 1.0
    deriv = np.zeros((384, 5 * SLOT), np.float32)
    for l in range(3):
        deriv[l * 128 : l * 128 + 125] = parts[l] @ pad
    spread = np.zeros((5 * SLOT, 128), np.float32)
    spread[:, :125] = pad.T
    rows = np.concatenate([np.arange(SLOT * a, SLOT * (a + 1)) for a in ORDER])
    return deriv, -deriv.T[rows], spread[rows]


def split2(x):
    hi = x.astype(jnp.bfloat16)
    low = (x - hi.astype(jnp.float32)).astype(jnp.bfloat16)
    return (hi, low)


def halves(x):
    hi = np.asarray(x, jnp.bfloat16)
    low = np.asarray(x - hi.astype(np.float32), jnp.bfloat16)
    return np.stack([hi, low])


def product(hi, low, y):
    top, rest = split2(y)
    dot = lambda a, b: jnp.dot(a, b, preferred_element_type=jnp.float32)
    wide = lambda *parts: jnp.concatenate(parts, axis=1)
    if y.shape[0] > 256:
        first = dot(
            wide(hi, hi, low),
            jnp.concatenate([top[:, :256], rest[:, :256], top[:, :256]], axis=0),
        )
    else:
        first = dot(hi, top[:, :256]) + dot(hi, rest[:, :256]) + dot(low, top[:, :256])
    both = dot(hi, wide(top[:, 256:], rest[:, 256:]))
    last = both[:, :128] + both[:, 128:] + dot(low, top[:, 256:])
    return first[:, :128], first[:, 128:], last


def ways():
    steps = (0, -1, 1)
    found = [(x, y, z) for z in steps for y in steps for x in steps][1:]
    half = [w for w in found if w > (0, 0, 0)]
    half.sort(key=lambda w: (sum(map(abs, w)), -abs(w[2])))
    other = [tuple(-v for v in w) for w in half]
    return half + other[::-1]


WAYS = ways()


def neighbours():
    names = ("gx", "gy", "gz")
    spots = [lax.axis_index(n) for n in names]
    sizes = [lax.axis_size(n) for n in names]
    links = []
    for way in WAYS:
        there = None
        peer = {}
        for n, s, z, w in zip(names, spots, sizes, way):
            if w:
                ok = s > 0 if w < 0 else s < z - 1
                there = ok if there is None else there & ok
                peer[n] = s + w
        links.append((way, there, peer))
    return links


def classes():
    found = [((), None)]
    for name in ("gx", "gy", "gz"):
        size, spot = lax.axis_size(name), lax.axis_index(name)
        inner = (spot > 0) & (spot < size - 1)
        choices = [(min(size - 1, 1), None)]
        if size > 2:
            choices = [(1, jnp.logical_not(inner)), (2, inner)]
        grown = []
        for counts, here in found:
            for count, ok in choices:
                both = here if ok is None else ok if here is None else here & ok
                grown.append((counts + (count,), both))
        found = grown
    return [(counts, True if here is None else here) for counts, here in found]


def squeezed(ref):
    return ref.at[:, 0] if len(ref.shape) == 3 else ref.at[:, :, 0]


def kernel(
    displ, veloc, accel, node, inv, jac, lame, shear, dens,
    deriv_ref, back_ref, spread_ref,
    pos_out, vel_out, acc_out,
    deriv_s, back_s, spread_s,
    d_s, v_s, a_s, node_s, raw_s,
    order_s, sorted_s, w_s, z_s, top_s, u_s, fl_s, md_s, grid_s,
    m_send, p_send, x_send, e_send, q_send, f_send, c_send,
    m_recv, p_recv, q_recv, x_recv, e_recv, f_recv, c_recv,
    tally, in_sem, send_sem, recv_sem,
):
    links = neighbours()
    head = node.at[pl.ds(0, 1), 0]
    copies = [pltpu.make_async_copy(head, node_s, in_sem.at[0])]
    for k, (src, dst) in enumerate(((displ, d_s), (veloc, v_s), (accel, a_s))):
        copies.append(pltpu.make_async_copy(src.at[:, 0], dst, in_sem.at[1 + k]))
    whole = squeezed(inv)
    point = pl.ds(0, 125)
    copies.append(pltpu.make_async_copy(whole, raw_s.at[pl.ds(0, 9), point], in_sem.at[4]))
    for k, src in enumerate((jac, lame, shear, dens)):
        copies.append(pltpu.make_async_copy(squeezed(src), raw_s.at[9 + k, point], in_sem.at[5]))
    consts = ((deriv_ref, deriv_s), (back_ref, back_s), (spread_ref, spread_s))
    for k, (src, dst) in enumerate(consts):
        copies.append(pltpu.make_async_copy(src, dst, in_sem.at[6 + k]))
    for cp in copies:
        cp.start()
    raw_s[:, 125:128, :] = jnp.zeros((13, 3, 128), jnp.float32)
    for ref in (m_recv, p_recv, q_recv, x_recv, e_recv, f_recv, c_recv):
        ref[...] = jnp.zeros_like(ref)
    copies[0].wait()
    corner = node_s[0:1, :].astype(jnp.float32)
    x0 = jnp.floor((corner + 0.5) * (1.0 / PLANE))
    rem = corner - PLANE * x0
    y0 = jnp.floor((rem + 0.5) * (1.0 / NZ))
    z0 = rem - NZ * y0
    goal = EY * EX * 0.25 * z0 + EX * 0.25 * y0 + 0.25 * x0
    goal = jnp.transpose(jnp.broadcast_to(goal, (128, 128)))
    slots = lax.broadcasted_iota(jnp.int32, (128, 128), 1).astype(jnp.float32)
    order = jnp.where(slots == goal, 1.0, 0.0).astype(jnp.bfloat16)
    order_s[0:128, :] = order
    order_s[128:256, :] = order
    barrier = pltpu.get_barrier_semaphore()
    for way, there, peer in links:

        @pl.when(there)
        def _():
            pl.semaphore_signal(barrier, inc=1, device_id=peer, device_id_type=MESH)

    for cp in copies[1:4]:
        cp.wait()

    half = 0.5 * time_step
    pos = d_s[...] + time_step * v_s[...] + (half * time_step) * a_s[...]
    pos_out[...] = pos

    lane = lax.broadcasted_iota(jnp.int32, (1, 128), 1)

    def chunk(q):
        width = min(128, PLANE * NX - 128 * q)
        part = pos_out[:, 128 * q : 128 * q + width]
        if width < 128:
            part = jnp.concatenate([part, jnp.zeros((3, 128 - width), jnp.float32)], axis=1)
        return part

    ahead = (4 * PLANE - STRIDE) // 128
    blank = jnp.zeros((3, 128), jnp.float32)
    single = [chunk(q) for q in range(-(-PLANE * NX // 128))]
    double = [
        jnp.concatenate([v, single[q + ahead] if q + ahead < len(single) else blank], axis=0)
        for q, v in enumerate(single)
    ]

    def window(source, x, ey):
        q, at = divmod(PLANE * x + STRIDE * ey, 128)
        part = source[q]
        if at + SPAN > 128:
            part = jnp.where(lane >= at, part, source[q + 1])
        return pltpu.roll(part, 128 - at, 1) if at else part

    def keep(x, ey, part):
        ex, a = divmod(x, 4)
        spots = [(a, ex)] if x < NX - 1 else []
        if x and a == 0:
            spots.append((4, ex - 1))
        for a, ex in spots:
            first = 3 * ((a * EY + ey) * EX + ex)
            w_s[first : first + 3, :] = part

    for x in range(NX):
        paired = x < NX - 1 and x % 8 < 4
        for ey in range(EY):
            if paired:
                part = window(double, x, ey)
                keep(x, ey, part[:3])
                if ey:
                    keep(x + 4, ey - 1, part[3:])
            elif x == NX - 1 or ey == EY - 1:
                keep(x, ey, window(single, x, ey))

    copies[4].wait()
    pltpu.make_async_copy(
        whole.at[pl.ds(0, 4)], raw_s.at[pl.ds(9, 4), point], in_sem.at[5]
    ).wait()
    copies[9].wait()
    for first, many in SPLITS:
        raw = raw_s[first : first + many].reshape(many * 128, 128)
        sorted_s[first : first + many] = jnp.dot(
            jnp.concatenate(split2(raw), axis=1),
            order_s[...],
            preferred_element_type=jnp.float32,
        ).reshape(many, 128, 128)

    left = lax.broadcasted_iota(jnp.int32, (SLOT, 128), 1) < 64
    each = EX * EY

    def block(c, a):
        return w_s[pl.ds(3 * each * a + c, each, stride=3), :]

    for (c, a), (d, b) in PAIRS[:6] + (((0, 4), (1, 4)), ((2, 4), (2, 4))):
        turned = jnp.transpose(jnp.concatenate([block(c, a), block(d, b)], axis=0))[:SLOT]
        other = pltpu.roll(turned, 64, 1)
        rise = lambda v: pltpu.roll(v, SLOT - 4, 0)
        u_s[SLOT * a : SLOT * (a + 1), 128 * c : 128 * (c + 1)] = jnp.where(
            left, turned, rise(other)
        )
        if (c, a) != (d, b):
            u_s[SLOT * b : SLOT * (b + 1), 128 * d : 128 * (d + 1)] = jnp.where(
                left, other, rise(turned)
            )

    local = product(deriv_s[0], deriv_s[1], u_s[...])
    for i in range(16):
        at = slice(8 * i, 8 * i + 8)
        maps = [[sorted_s[3 * l + j, at] for j in range(3)] for l in range(3)]
        weight, lam, mu, dens_e = (sorted_s[9 + k, at] for k in range(4))
        grads = [[local[c][128 * l + 8 * i : 128 * l + 8 * i + 8] for c in range(3)] for l in range(3)]
        h = [
            [sum(grads[l][c] * maps[l][j] for l in range(3)) for j in range(3)]
            for c in range(3)
        ]
        mu = mu * weight
        div = lam * weight * (h[0][0] + h[1][1] + h[2][2])
        stress = [[None] * 3 for _ in range(3)]
        for c in range(3):
            for j in range(c, 3):
                s = mu * (h[c][j] + h[j][c])
                stress[c][j] = stress[j][c] = s + div if c == j else s
        for l in range(3):
            for c in range(3):
                fl_s[128 * l + 8 * i : 128 * l + 8 * i + 8, 128 * c : 128 * (c + 1)] = sum(
                    stress[c][j] * maps[l][j] for j in range(3)
                )
        md_s[at, :] = dens_e * weight
    for cp in copies[10:]:
        cp.wait()
    terms = product(back_s[0], back_s[1], fl_s[...])
    heavy = sum(
        jnp.dot(spread_s[...], part, preferred_element_type=jnp.float32)
        for part in split2(md_s[...])
    )

    def term(c, a):
        at = slice(SLOT * ORDER.index(a), SLOT * (ORDER.index(a) + 1))
        return terms[c][at] if c < 3 else heavy[at]

    sink = lambda v: pltpu.roll(v, 4, 0)
    tail = jnp.zeros((128, 128 - SLOT), jnp.float32)
    crest = {}
    rows = lax.broadcasted_iota(jnp.int32, (each, 128), 0)
    def settle_block(one_at, two_at):
        (c, a), (d, b) = one_at, two_at
        one, two = term(c, a), term(d, b)
        both = jnp.where(left, one, sink(two)) + pltpu.roll(jnp.where(left, two, sink(one)), 64, 1)
        turned = jnp.concatenate([jnp.transpose(both), tail], axis=1)
        for k, part in (((c, a), turned[:each]), ((d, b), turned[each:])):
            if k[1] == 4:
                top_s[each * k[0] : each * (k[0] + 1), :] = part
                crest[k[0]] = jnp.where(rows % EX == 0, 0.0, pltpu.roll(part, 1, 0))
                continue
            if k[1] == 0:
                part = part + crest[k[0]]
            for ey in range(EY):
                first = ((k[0] * EY + ey) * 4 + k[1]) * EX
                z_s[first : first + EX, :] = part[EX * ey : EX * (ey + 1)]

    def row_ends(sy):
        ey = (EY - 1) * sy
        crown = top_s[pl.ds(EX * ey + EX - 1, 4, stride=each), :]
        return ey, STRIDE * sy, crown

    sides = (pl.ds(0, 4, stride=16), pl.ds(64, 4))
    lanes = lax.broadcasted_iota(jnp.int32, (SROW, 128), 1)
    lane8 = lax.broadcasted_iota(jnp.int32, (8, 128), 1)
    far = CHUNKS - 1
    def route(way):
        sx, sy, sz = ((w + 1) // 2 for w in way)
        ox, oy, oz = 1 - sx, 1 - sy, 1 - sz
        dx, dy, dz = (w != 0 for w in way)
        if dx and dy and dz:
            return c_send.at[sx, sy, sz], c_recv.at[ox, oy, oz]
        if dx and dy:
            return f_send.at[sx, sy], f_recv.at[ox, oy]
        if dx and dz:
            return e_send.at[sx, sz], e_recv.at[ox, oz]
        if dy and dz:
            return q_send.at[sy, sz], q_recv.at[oy, oz]
        if dx:
            return x_send.at[sx], x_recv.at[ox]
        if dy:
            return p_send.at[sy], p_recv.at[oy]
        return m_send.at[sz], m_recv.at[oz]

    def copy(source, target, peer):
        return pltpu.make_async_remote_copy(
            src_ref=source,
            dst_ref=target,
            send_sem=send_sem.at[0],
            recv_sem=recv_sem.at[0],
            device_id=peer,
            device_id_type=MESH,
        )

    def await_all(settle):
        for (nx, ny, nz), here in classes():
            count = nx * CHUNKS + nx * ny + nx * nz + nx * ny * nz
            count += 2 * ny + 2 * ny * nz + nz * SROW // 4
            whole = tally.at[pl.ds(0, count)]

            @pl.when(here)
            def _():
                settle(copy(whole, whole, links[0][2]))

    peers = sum(there.astype(jnp.int32) for way, there, peer in links)
    farthest = sorted(range(len(WAYS)), key=lambda k: -sum(map(abs, WAYS[k])))

    def depart(chosen):
        for dy in (0, -1, 1):
            leaving = [k for k in farthest if WAYS[k][1] == dy and chosen(WAYS[k])]

            def send():
                for k in leaving:
                    way, there, peer = links[k]
                    if way in ((0, -1, 0), (0, 1, 0)):
                        copy(*route(way), peer).start()
                        continue

                    @pl.when(there)
                    def _():
                        copy(*route(way), peer).start()

            if leaving and dy:
                pl.when(links[WAYS.index((0, dy, 0))][1])(send)
            elif leaving:
                send()

    for one_at, two_at in FIRST + PAIRS[1::2]:
        settle_block(one_at, two_at)
    for sy in range(2):
        ey, base, crown = row_ends(sy)
        rows = jnp.concatenate([z_s[pl.ds(16 * ey, 4, stride=16 * EY), :], crown], axis=0)
        first = TAIL * (1 - sy)
        got = pltpu.roll(rows, (first - base) % 128, 1)
        got = jnp.where((lane8 >= first) & (lane8 < first + NZ), got, 0.0)
        f_send[0, sy] = got[:4]
        f_send[1, sy] = got[4:]
        for sz in range(2):
            got = pltpu.roll(rows, (first - base + (8 if sz == 0 else -8)) % 128, 1)
            got = jnp.where(lane8 == first + (NZ - 1) * (1 - sz), got, 0.0)
            c_send[0, sy, sz] = got[:4]
            c_send[1, sy, sz] = got[4:]
    pl.semaphore_wait(barrier, peers)
    depart(lambda way: way[0] != 0 and way[1] != 0)
    for sy in range(2):
        ey, base, crown = row_ends(sy)
        parts = [z_s[pl.ds(16 * (c * EY + ey) + 8 * h, 8), :] for c in range(4) for h in range(2)]
        parts.append(jnp.concatenate([crown, jnp.zeros((4, 128), jnp.float32)], axis=0))

        def pack(low, high, move):
            packed = None
            for i, part in enumerate(parts):
                got = jnp.where((lane8 >= base + low) & (lane8 < base + high), part, 0.0)
                shift = (PITCH * i - base + move) % 128
                got = pltpu.roll(got, shift, 1) if shift else got
                packed = got if packed is None else packed + got
            return packed

        p_send[sy] = pack(0, NZ, 0)
        q_send[sy, 0] = pack(0, 1, NZ - 1)
        q_send[sy, 1] = pack(NZ - 1, NZ, 1 - NZ)
    depart(lambda way: way[0] == 0 and way[1] != 0)

    for c in range(5):
        first, many = (16 * c, 16) if c < 4 else (64, 8)
        sums = [None] * CHUNKS
        for ey in range(EY):
            j, at = divmod(STRIDE * ey, 128)
            if c < 4:
                part = z_s[16 * (c * EY + ey) : 16 * (c * EY + ey + 1), :]
            else:
                part = top_s[pl.ds(EX * ey + EX - 1, 4, stride=each), :]
                part = jnp.concatenate([part, jnp.zeros((4, 128), jnp.float32)], axis=0)
            part = pltpu.roll(part, at, 1) if at else part
            pieces = [(j, part)]
            if at + SLOT > 128:
                pieces = [
                    (j, jnp.where(lane >= at, part, 0.0)),
                    (j + 1, jnp.where(lane < at, part, 0.0)),
                ]
            for k, piece in pieces:
                sums[k] = piece if sums[k] is None else sums[k] + piece
        for j in range(CHUNKS):
            grid_s[j, first : first + many, :] = sums[j]

    for side in range(2):
        for j in range(CHUNKS):
            x_send[side, j] = grid_s[j, sides[side], :]
    sources = [
        jnp.minimum(NZ * lanes + (NZ - 1) * dz, 128 * CHUNKS - 1) for dz in range(2)
    ]

    def face(parts, dz):
        many = parts[0].shape[0]
        source = sources[dz][:many]
        found = None
        for j in range(CHUNKS):
            got = jnp.take_along_axis(
                parts[j], source & 127, axis=1, mode="promise_in_bounds"
            )
            found = got if found is None else jnp.where(source >= 128 * j, got, found)
        return jnp.where(lanes[:many] < NY, found, 0.0)

    rims = [
        jnp.concatenate([x_send[0, j], x_send[1, j]], axis=0) for j in range(CHUNKS)
    ]
    for dz in range(2):
        got = face(rims, dz)
        e_send[0, dz] = got[:4]
        e_send[1, dz] = got[4:]
    depart(lambda way: way[1] == 0 and way[0] != 0)
    for dz in range(2):
        m_send[dz] = face([grid_s[j] for j in range(CHUNKS)], dz)
    depart(lambda way: way[1] == 0 and way[0] == 0)
    vel_out[...] = v_s[...] + half * a_s[...]

    await_all(lambda copied: copied.wait_recv())

    for dz in range(2):
        for sx in range(2):
            m_recv[dz, sides[sx], :] += e_recv[sx, dz]
    full = [m_recv[dz] for dz in range(2)]
    strips = []
    for sy in range(2):
        sums = p_recv[sy] + q_recv[sy, 0] + q_recv[sy, 1]
        parts = []
        for i in range(SROW // 8):
            shift = (TAIL * sy - PITCH * i) % 128
            got = pltpu.roll(sums, shift, 1) if shift else sums
            parts.append(
                jnp.where((lane8 >= TAIL * sy) & (lane8 < TAIL * sy + NZ), got, 0.0)
            )
        strips.append(jnp.concatenate(parts, axis=0))
        for sx in range(2):
            x_recv[sx, far * sy] += f_recv[sx, sy] + (c_recv[sx, sy, 0] + c_recv[sx, sy, 1])
    for j in range(CHUNKS):
        node = lanes + 128 * j
        along = lax.div(node, NZ)
        depth = node - NZ * along
        sums = grid_s[j]
        for dz in range(2):
            got = jnp.take_along_axis(
                full[dz], jnp.minimum(along, 127), axis=1, mode="promise_in_bounds"
            )
            sums = sums + jnp.where((depth == (NZ - 1) * dz) & (along < NY), got, 0.0)
        if j == 0:
            sums = sums + strips[0]
        if j == far:
            sums = sums + strips[1]
        grid_s[j] = sums
        for sx in range(2):
            grid_s[j, sides[sx], :] += x_recv[sx, j]
        mass = grid_s[j, 48:64, :]
        for c in range(3):
            grid_s[j, 16 * c : 16 * c + 16, :] = grid_s[j, 16 * c : 16 * c + 16, :] / mass
        grid_s[j, 64:67, :] = grid_s[j, 64:67, :] / grid_s[j, 67:68, :]

    for x in range(NX):
        rows = pl.ds(4 * (x % 4) + x // 4, 3, stride=16) if x < NX - 1 else pl.ds(64, 3)
        for j in range(CHUNKS):
            width = min(128, PLANE - 128 * j)
            at = PLANE * x + 128 * j
            acc_out[:, at : at + width] = grid_s[j, rows, 0:width]
    await_all(lambda copied: copied.wait_send())


def finish(pos, vel, acc, pos_out, vel_out, acc_out, v_s, sem):
    def put(src, dst, k):
        copy = pltpu.make_async_copy(src, dst.at[:, 0], sem.at[k])
        copy.start()
        return copy

    copies = [put(pos, pos_out, 0), put(acc, acc_out, 1)]
    v_s[...] = vel[...] + (0.5 * time_step) * acc[...]
    copies.append(put(v_s, vel_out, 2))
    for cp in copies:
        cp.wait()


def body(displ, veloc, accel, node_index, inv_map, jac_weight, lame_first, shear_mod, density):
    nodes = displ.shape[4]
    elements = node_index.shape[4]
    deriv, back, spread = constants()
    deriv, back = halves(deriv), halves(back)
    fields = [x.reshape(3, 1, nodes) for x in (displ, veloc, accel)]
    elems = [
        x.reshape(125, 1, elements) for x in (jac_weight, lame_first, shear_mod, density)
    ]
    vmem = pl.BlockSpec(memory_space=pltpu.VMEM)
    hbm = pl.BlockSpec(memory_space=pltpu.HBM)
    f32 = jnp.float32
    out = jax.ShapeDtypeStruct((3, 1, nodes), f32)
    result = pl.pallas_call(
        kernel,
        out_shape=[pltpu.VMEM((3, nodes), f32)] * 3,
        in_specs=[hbm] * 12,
        out_specs=[vmem] * 3,
        scratch_shapes=[
            pltpu.VMEM(deriv.shape, jnp.bfloat16),
            pltpu.VMEM(back.shape, jnp.bfloat16),
            pltpu.VMEM(spread.shape, jnp.bfloat16),
            pltpu.VMEM((3, nodes), f32),
            pltpu.VMEM((3, nodes), f32),
            pltpu.VMEM((3, nodes), f32),
            pltpu.VMEM((1, elements), jnp.int32),
            pltpu.VMEM((13, 128, elements), f32),
            pltpu.VMEM((256, 128), jnp.bfloat16),
            pltpu.VMEM((13, 128, 128), f32),
            pltpu.VMEM((15 * EX * EY, 128), f32),
            pltpu.VMEM((16 * EX * EY, 128), f32),
            pltpu.VMEM((4 * EX * EY, 128), f32),
            pltpu.VMEM((5 * SLOT, 384), f32),
            pltpu.VMEM((384, 384), f32),
            pltpu.VMEM((128, 128), f32),
            pltpu.VMEM((CHUNKS, SROW, 128), f32),
            pltpu.VMEM((2, SROW, 128), f32),
            pltpu.VMEM((2, 8, 128), f32),
            pltpu.VMEM((2, CHUNKS, 4, 128), f32),
            pltpu.VMEM((2, 2, 4, 128), f32),
            pltpu.VMEM((2, 2, 8, 128), f32),
            pltpu.VMEM((2, 2, 4, 128), f32),
            pltpu.VMEM((2, 2, 2, 4, 128), f32),
            pltpu.VMEM((2, SROW, 128), f32),
            pltpu.VMEM((2, 8, 128), f32),
            pltpu.VMEM((2, 2, 8, 128), f32),
            pltpu.VMEM((2, CHUNKS, 4, 128), f32),
            pltpu.VMEM((2, 2, 4, 128), f32),
            pltpu.VMEM((2, 2, 4, 128), f32),
            pltpu.VMEM((2, 2, 2, 4, 128), f32),
            pltpu.VMEM((2 * SROW // 4 + 2 * CHUNKS + 28, 4, 128), f32),
            pltpu.SemaphoreType.DMA((9,)),
            pltpu.SemaphoreType.DMA((1,)),
            pltpu.SemaphoreType.DMA((1,)),
        ],
        compiler_params=pltpu.CompilerParams(
            collective_id=0, has_side_effects=True, vmem_limit_bytes=LIMIT
        ),
    )(
        *fields,
        node_index.reshape(125, 1, elements),
        inv_map.reshape(9, 125, 1, elements),
        *elems,
        jnp.asarray(deriv),
        jnp.asarray(back),
        jnp.asarray(spread, jnp.bfloat16),
    )
    final = pl.pallas_call(
        finish,
        out_shape=[out] * 3,
        in_specs=[vmem] * 3,
        out_specs=[hbm] * 3,
        scratch_shapes=[pltpu.VMEM((3, nodes), f32), pltpu.SemaphoreType.DMA((3,))],
        compiler_params=pltpu.CompilerParams(vmem_limit_bytes=LIMIT),
    )(*[pltpu.with_memory_space_constraint(x, pltpu.VMEM) for x in result])
    return tuple(x.reshape(displ.shape) for x in final)


def solution(mesh):
    field = P(None, "gx", "gy", "gz", None)
    elem = P("gx", "gy", "gz", None, None)
    placed = (field,) * 3 + (elem, P("gx", "gy", "gz", None, None, None)) + (elem,) * 4
    return jax.shard_map(
        body, mesh=mesh, in_specs=placed, out_specs=(field,) * 3, check_vma=False
    )
```
